128 devices in a mesh: gx: 4 (over y), gy: 8 (over x_lo, z), gz: 4 (over x_hi, core).
Axes of the slice: x: 4 (x_hi: 2, x_lo: 2; x = x_hi * 2 + x_lo), y: 4, z: 4, core: 2. Of those that a mesh axis runs over, the one named last changes fastest.
Arguments:
- populations: float32 [19, 32, 128, 512], P(None, 'gx', 'gy', 'gz'), may hold values from 0 to 1, as said below
- solid_fraction: float32 [32, 128, 512], P('gx', 'gy', 'gz'), may hold values from 0 to 1
- intersection: int32 [32, 128, 512], P('gx', 'gy', 'gz'), may hold values from 0 to 256, as said below
- touch: int32 [4, 8, 4, 256], P('gx', 'gy', 'gz'), may hold values from 0 to 3455, as said below
- particles: float32 [4, 8, 4, 6, 128], P('gx', 'gy', 'gz'), may hold values from -8 to 8, as said below
- contacts: int32 [4, 8, 4, 12, 128], P('gx', 'gy', 'gz'), may hold values from 0 to 3456, as said below
- dest_code: int32 [4, 8, 4, 128], P('gx', 'gy', 'gz'), may hold values from 4 to 22, as said below
- dest_slot: int32 [4, 8, 4, 128], P('gx', 'gy', 'gz'), may hold values from 0 to 127, as said below
Outputs:
- populations_next: float32 [19, 32, 128, 512], P(None, 'gx', 'gy', 'gz')
- particles_next: float32 [4, 8, 4, 6, 128], P('gx', 'gy', 'gz')
The draws below stay inside these ranges and needn't reach their ends.
Inputs may be any that keep to these rules, and one draw needn't show every extreme that they name: intersection = 256 marks a cell that no sphere covers; otherwise a touch slot of the cell's block. `touch`: entry o * 128 + s names slot s of the block at offset o of the 27 neighbouring blocks, offsets ordered with x slowest; the entries of one block are distinct and name every slot of the block itself. `contacts`: 3456 marks an empty entry. `dest_code`: a sphere stays (code 13) or moves one block along one axis (codes 4, 10, 12, 14, 16, 22), never out of the mesh; every slot of every block receives exactly one record. `dest_slot`: see dest_code. `populations`: every population is positive. `particles`: positions, in radii from the block centre, lie within the block's half widths; speeds lie within -1.5 to 1.5.
All inputs are finite; a program needn't handle non-finite values.
Results may differ from the reference program's by a relative error of at most 0.000076.
Values sent between devices are 32-bit elements; how exact they have to be, the bound alone decides.
A program may use at most 128 MiB of HBM per device.

```python
import jax
import jax.numpy as jnp
from jax import lax

CX = 8
CY = 16
CZ = 128
P_SIZE = 128
NC = 12
R = 8
K = 256
BX = 4
BY = 8
BZ = 4
NX = 32
NY = 128
NZ = 512


LATTICE = [(0, 0, 0), (1, 0, 0), (-1, 0, 0), (0, 1, 0), (0, -1, 0), (0, 0, 1), (0, 0, -1), (1, 1, 0), (-1, -1, 0), (1, -1, 0), (-1, 1, 0), (1, 0, 1), (-1, 0, -1), (1, 0, -1), (-1, 0, 1), (0, 1, 1), (0, -1, -1), (0, 1, -1), (0, -1, 1)]


WEIGHTS = [1.0 / 3.0] + [1.0 / 18.0] * 6 + [1.0 / 36.0] * 12


CONTACT_STEPS = [(1, 0, 0), (-1, 0, 0), (0, 1, 0), (0, -1, 0), (0, 0, 1), (0, 0, -1), (1, 1, 0), (-1, -1, 0), (1, 0, 1), (-1, 0, -1), (0, 1, 1), (0, -1, -1)]


def equilibrium_drawn(density, velocity):
    square = velocity[0] * velocity[0] + velocity[1] * velocity[1] + velocity[2] * velocity[2]
    result = []
    for vector, weight in zip(LATTICE, WEIGHTS):
        projected = vector[0] * velocity[0] + vector[1] * velocity[1] + vector[2] * velocity[2]
        result.append(weight * density * (1.0 + 3.0 * projected + 4.5 * projected * projected - 1.5 * square))
    return jnp.stack(result)


def draw_populations(key, part):
    subkeys = jax.random.split(key, 3)
    grid_shape = (NX, NY, NZ)
    density = 1.0 + 0.02 * jax.random.truncated_normal(subkeys[0], -3.0, 3.0, grid_shape, jnp.float32)
    velocity = 0.04 * jax.random.truncated_normal(subkeys[1], -2.0, 2.0, (3,) + grid_shape, jnp.float32)
    jitter = 1.0 + 0.3 * (jax.random.uniform(subkeys[2], (19,) + grid_shape, jnp.float32) - 0.5)
    return equilibrium_drawn(density, velocity) * jitter


def draw_intersection(key, part):
    subkeys = jax.random.split(jax.random.fold_in(key, 11), 2)
    grid_shape = (NX, NY, NZ)
    height = lax.broadcasted_iota(jnp.int32, grid_shape, 2)
    draw_height = jax.random.randint(subkeys[0], grid_shape, 0, NZ)
    is_solid = draw_height < (NZ - height) * 3 // 4
    chosen = jax.random.randint(subkeys[1], grid_shape, 0, K)
    return jnp.where(is_solid, chosen, K).astype(jnp.int32)


def slot_tables(key):
    folded = jax.random.fold_in(key, 29)
    block_keys = jax.random.split(folded, BX * BY * BZ)
    slot_of_site = jax.vmap(lambda block_key: jax.random.permutation(block_key, P_SIZE))(block_keys)
    slot_of_site = slot_of_site.reshape(BX, BY, BZ, P_SIZE).astype(jnp.int32)
    site_of_slot = jnp.argsort(slot_of_site, axis=-1).astype(jnp.int32)
    return (slot_of_site, site_of_slot)


def neighbour_entry(slot_of_site, site_x, site_y, site_z, home_x, home_y, home_z):
    layers = P_SIZE // 16
    move_x = (site_x + 4) // 4 - 1
    move_y = (site_y + 4) // 4 - 1
    move_z = (site_z + layers) // layers - 1
    block_x = home_x + move_x
    block_y = home_y + move_y
    block_z = home_z + move_z
    inside = (block_x >= 0) & (block_x < BX) & (block_y >= 0) & (block_y < BY) & (block_z >= 0) & (block_z < BZ)
    flat_block = (jnp.clip(block_x, 0, BX - 1) * BY + jnp.clip(block_y, 0, BY - 1)) * BZ + jnp.clip(block_z, 0, BZ - 1)
    local_site = (site_z - layers * move_z) * 16 + (site_y - 4 * move_y) * 4 + site_x - 4 * move_x
    slot_found = slot_of_site.reshape(-1)[flat_block * P_SIZE + local_site]
    code = 9 * (move_x + 1) + 3 * (move_y + 1) + move_z + 1
    return ((code * P_SIZE + slot_found).astype(jnp.int32), inside)


def draw_particles(key, part):
    slot_of_site, site_of_slot = slot_tables(key)
    subkeys = jax.random.split(jax.random.fold_in(key, 13), 2)
    layers = P_SIZE // 16
    spacing_x = CX / (4.0 * R)
    spacing_y = CY / (4.0 * R)
    spacing_z = CZ / (layers * 1.0 * R)
    site_x = (site_of_slot % 4).astype(jnp.float32)
    site_y = (site_of_slot // 4 % 4).astype(jnp.float32)
    site_z = (site_of_slot // 16).astype(jnp.float32)
    centres = jnp.stack([(site_x + 0.5) * spacing_x - CX / (2.0 * R), (site_y + 0.5) * spacing_y - CY / (2.0 * R), (site_z + 0.5) * spacing_z - CZ / (2.0 * R)], axis=3)
    spacing = jnp.array([spacing_x, spacing_y, spacing_z], jnp.float32)
    jitter = jax.random.uniform(subkeys[0], (BX, BY, BZ, 3, P_SIZE), jnp.float32, -0.3, 0.3) * spacing[:, None]
    places = centres + jitter
    speeds = 0.6 * jax.random.truncated_normal(subkeys[1], -2.5, 2.5, (BX, BY, BZ, 3, P_SIZE), jnp.float32)
    return jnp.concatenate([places, speeds], axis=3)


def draw_contacts(key, part):
    slot_of_site, site_of_slot = slot_tables(key)
    shape_here = (BX, BY, BZ, P_SIZE)
    site_x = site_of_slot % 4
    site_y = site_of_slot // 4 % 4
    site_z = site_of_slot // 16
    home_x = lax.broadcasted_iota(jnp.int32, shape_here, 0)
    home_y = lax.broadcasted_iota(jnp.int32, shape_here, 1)
    home_z = lax.broadcasted_iota(jnp.int32, shape_here, 2)
    listed = []
    for step in CONTACT_STEPS:
        entry, inside = neighbour_entry(slot_of_site, site_x + step[0], site_y + step[1], site_z + step[2], home_x, home_y, home_z)
        listed.append(jnp.where(inside, entry, 27 * P_SIZE))
    stacked = jnp.stack(listed, axis=3)
    empty = jax.random.randint(jax.random.fold_in(key, 17), stacked.shape, 0, 4) == 0
    return jnp.where(empty, 27 * P_SIZE, stacked).astype(jnp.int32)


def draw_touch(key, part):
    slot_of_site, unused = slot_tables(key)
    layers = P_SIZE // 16
    extended = 36 * (layers + 2)
    shape_here = (BX, BY, BZ, extended)
    candidate = lax.broadcasted_iota(jnp.int32, shape_here, 3)
    around_x = candidate % 6 - 1
    around_y = candidate // 6 % 6 - 1
    around_z = candidate // 36 - 1
    home_x = lax.broadcasted_iota(jnp.int32, shape_here, 0)
    home_y = lax.broadcasted_iota(jnp.int32, shape_here, 1)
    home_z = lax.broadcasted_iota(jnp.int32, shape_here, 2)
    entry, inside = neighbour_entry(slot_of_site, around_x, around_y, around_z, home_x, home_y, home_z)
    inner = (around_x >= 0) & (around_x < 4) & (around_y >= 0) & (around_y < 4) & (around_z >= 0) & (around_z < layers)
    tier = jnp.where(inner, 0, jnp.where(inside, 1, 2))
    block_count = BX * BY * BZ
    subkeys = jax.random.split(jax.random.fold_in(key, 31), 2)
    ranks = jax.vmap(lambda block_key: jax.random.permutation(block_key, extended))(jax.random.split(subkeys[0], block_count))
    ranks = ranks.reshape(shape_here).astype(jnp.int32)
    order = jnp.argsort(tier * extended + ranks, axis=-1)[..., :K]
    chosen = jnp.take_along_axis(entry, order, axis=-1)
    shuffle = jax.vmap(lambda block_key: jax.random.permutation(block_key, K))(jax.random.split(subkeys[1], block_count))
    shuffle = shuffle.reshape(BX, BY, BZ, K).astype(jnp.int32)
    return jnp.take_along_axis(chosen, shuffle, axis=-1).astype(jnp.int32)


def migration_plan(key):
    folded = jax.random.fold_in(key, 23)
    subkeys = jax.random.split(folded, 7)
    counts = [BX, BY, BZ]
    shape_here = (BX, BY, BZ, P_SIZE)
    slot_ids = lax.broadcasted_iota(jnp.int32, shape_here, 3)
    moves = []
    for dimension in range(3):
        parity = jax.random.randint(subkeys[dimension], (), 0, 2)
        amount = jax.random.randint(subkeys[3 + dimension], (), max(P_SIZE // 16, 1), P_SIZE // 4 + 1)
        coordinate = lax.broadcasted_iota(jnp.int32, shape_here, dimension)
        first_slot = dimension * (P_SIZE // 4)
        chosen = (slot_ids >= first_slot) & (slot_ids < first_slot + amount)
        upward = ((coordinate - parity) % 2 == 0) & (coordinate + 1 < counts[dimension])
        downward = ((coordinate - parity) % 2 == 1) & (coordinate >= 1)
        moves.append(jnp.where(chosen, upward.astype(jnp.int32) - downward.astype(jnp.int32), 0))
    codes = 13 + 9 * moves[0] + 3 * moves[1] + moves[2]
    block_count = BX * BY * BZ
    perms = jax.vmap(lambda block_key: jax.random.permutation(block_key, P_SIZE))(jax.random.split(subkeys[6], block_count))
    home_x = lax.broadcasted_iota(jnp.int32, shape_here, 0)
    home_y = lax.broadcasted_iota(jnp.int32, shape_here, 1)
    home_z = lax.broadcasted_iota(jnp.int32, shape_here, 2)
    target = ((home_x + moves[0]) * BY + home_y + moves[1]) * BZ + home_z + moves[2]
    slots_new = perms.reshape(-1)[target * P_SIZE + slot_ids]
    return (codes.astype(jnp.int32), slots_new.astype(jnp.int32))


def draw_dest_code(key, part):
    return migration_plan(key)[0]


def draw_dest_slot(key, part):
    return migration_plan(key)[1]


def block_levels(own_key, shape, pieces, smallest, high):
    loudness, own = 1.0, jax.random.fold_in(own_key, 6)
    for position, blocks in pieces:
        steps = jnp.exp(jax.random.uniform(jax.random.fold_in(own, position), (blocks,), jnp.float32, smallest / len(pieces), high / len(pieces)))
        loudness = loudness * jnp.repeat(steps, shape[position] // blocks).reshape([-1 if axis == position else 1 for axis in range(len(shape))])
    return loudness


def setup_inputs(seed: int = 0) -> dict:
    arg_keys = jax.random.split(jax.random.key(seed), 9)
    return {
        "populations": draw_populations(jax.random.fold_in(arg_keys[8], 71), 0),
        "solid_fraction": jnp.clip(1.0 * jax.random.uniform(arg_keys[1], (NX, NY, NZ), jnp.float32) ** block_levels(arg_keys[1], (NX, NY, NZ), ((0, 4), (1, 8), (2, 4)), -0.2, 0.2), 0.0, 1.0),
        "intersection": draw_intersection(jax.random.fold_in(arg_keys[8], 71), 0),
        "touch": draw_touch(jax.random.fold_in(arg_keys[8], 71), 0),
        "particles": draw_particles(jax.random.fold_in(arg_keys[8], 71), 0),
        "contacts": draw_contacts(jax.random.fold_in(arg_keys[8], 71), 0),
        "dest_code": draw_dest_code(jax.random.fold_in(arg_keys[8], 71), 0),
        "dest_slot": draw_dest_slot(jax.random.fold_in(arg_keys[8], 71), 0),
    }


LATTICE = [(0, 0, 0), (1, 0, 0), (-1, 0, 0), (0, 1, 0), (0, -1, 0), (0, 0, 1), (0, 0, -1),
           (1, 1, 0), (-1, -1, 0), (1, -1, 0), (-1, 1, 0), (1, 0, 1), (-1, 0, -1),
           (1, 0, -1), (-1, 0, 1), (0, 1, 1), (0, -1, -1), (0, 1, -1), (0, -1, 1)]
OPPOSITE = [0, 2, 1, 4, 3, 6, 5, 8, 7, 10, 9, 12, 11, 14, 13, 16, 15, 18, 17]
WEIGHTS = [1.0 / 3.0] + [1.0 / 18.0] * 6 + [1.0 / 36.0] * 12
RELAX_TIME = 0.8
SPEED_UNIT = 0.05
FORCE_SCALE = 0.1
CONTACT_GAIN = 1.0
GRAVITY_STEP = 0.1


def equilibrium(density, velocity):
    square = velocity[0] * velocity[0] + velocity[1] * velocity[1] + velocity[2] * velocity[2]
    result = []
    for vector, weight in zip(LATTICE, WEIGHTS):
        projected = vector[0] * velocity[0] + vector[1] * velocity[1] + vector[2] * velocity[2]
        result.append(weight * density * (1.0 + 3.0 * projected + 4.5 * projected * projected - 1.5 * square))
    return jnp.stack(result)


def collide(populations, solid_weight, solid_velocity):
    lattice_table = jnp.array(LATTICE, jnp.float32)
    density = jnp.sum(populations, axis=0)
    momentum = jnp.tensordot(lattice_table.T, populations, axes=1, precision=lax.Precision.HIGHEST)
    velocity = momentum / density
    fluid_eq = equilibrium(density, velocity)
    solid_eq = equilibrium(density, solid_velocity)
    mirrored = jnp.stack([populations[mirror_index] for mirror_index in OPPOSITE])
    fluid_mirror = jnp.stack([fluid_eq[mirror_index] for mirror_index in OPPOSITE])
    exchange_term = mirrored - populations + solid_eq - fluid_mirror
    relaxed = populations - (1.0 - solid_weight) / RELAX_TIME * (populations - fluid_eq) + solid_weight * exchange_term
    cell_force = -jnp.tensordot(lattice_table.T, solid_weight * exchange_term, axes=1, precision=lax.Precision.HIGHEST)
    return relaxed, cell_force


def block_offsets(entries, slots_each, span_x, span_y, span_z, radius):
    block_code = jnp.arange(entries, dtype=jnp.int32) // slots_each
    return jnp.stack([(block_code // 9 - 1).astype(jnp.float32) * (span_x / radius),
                      ((block_code // 3) % 3 - 1).astype(jnp.float32) * (span_y / radius),
                      (block_code % 3 - 1).astype(jnp.float32) * (span_z / radius)])


def reference(populations, solid_fraction, intersection, touch, particles, contacts, dest_code, dest_slot):
    blocks = BX * BY * BZ
    padded = jnp.pad(particles, ((1, 1), (1, 1), (1, 1), (0, 0), (0, 0)))
    neighbourhood = jnp.stack([padded[step_x:step_x + BX, step_y:step_y + BY, step_z:step_z + BZ]
                               for step_x in range(3) for step_y in range(3) for step_z in range(3)], axis=3)
    records_near = jnp.moveaxis(neighbourhood, 4, 3).reshape(blocks, 6, 27 * P_SIZE)
    touch_rows = touch.reshape(blocks, K)
    touch_velocity = jnp.take_along_axis(records_near[:, 3:6, :], jnp.broadcast_to(touch_rows[:, None, :], (blocks, 3, K)), axis=2)
    touch_velocity = jnp.concatenate([touch_velocity, jnp.zeros((blocks, 3, 1), jnp.float32)], axis=2)
    velocity_rows = jnp.transpose(touch_velocity, (0, 2, 1)).reshape(blocks * (K + 1), 3)
    block_x = (jnp.arange(NX, dtype=jnp.int32) // CX)[:, None, None]
    block_y = (jnp.arange(NY, dtype=jnp.int32) // CY)[None, :, None]
    block_z = (jnp.arange(NZ, dtype=jnp.int32) // CZ)[None, None, :]
    slot_rows = ((block_x * BY + block_y) * BZ + block_z) * (K + 1) + intersection
    fraction_term = jnp.where(intersection < K, solid_fraction * (RELAX_TIME - 0.5) / ((1.0 - solid_fraction) + (RELAX_TIME - 0.5)), jnp.float32(0.0))

    def slab_step(start):
        slab_pop = lax.dynamic_slice_in_dim(populations, start, CX, 1)
        slab_rows = lax.dynamic_slice_in_dim(slot_rows, start, CX, 0)
        slab_weight = lax.dynamic_slice_in_dim(fraction_term, start, CX, 0)
        solid_velocity = SPEED_UNIT * jnp.moveaxis(velocity_rows[slab_rows], -1, 0)
        return collide(slab_pop, slab_weight, solid_velocity)

    relaxed, cell_force = lax.map(slab_step, jnp.arange(BX, dtype=jnp.int32) * CX)
    relaxed = jnp.moveaxis(relaxed, 0, 1).reshape(19, NX, NY, NZ)
    cell_force = jnp.moveaxis(cell_force, 0, 1).reshape(3, NX, NY, NZ)

    coord_x = jnp.arange(NX, dtype=jnp.int32)[:, None, None]
    coord_y = jnp.arange(NY, dtype=jnp.int32)[None, :, None]
    coord_z = jnp.arange(NZ, dtype=jnp.int32)[None, None, :]
    passed = []
    for direction, vector in enumerate(LATTICE):
        rolled = jnp.roll(relaxed[direction], vector, axis=(0, 1, 2))
        inside = ((coord_x - vector[0] >= 0) & (coord_x - vector[0] < NX) & (coord_y - vector[1] >= 0)
                  & (coord_y - vector[1] < NY) & (coord_z - vector[2] >= 0) & (coord_z - vector[2] < NZ))
        passed.append(jnp.where(inside, rolled, relaxed[OPPOSITE[direction]]))
    populations_next = jnp.stack(passed)

    touch_force = jax.ops.segment_sum(cell_force.reshape(3, -1).T, slot_rows.reshape(-1), num_segments=blocks * (K + 1))
    touch_force = touch_force.reshape(blocks, K + 1, 3)[:, :K, :]
    owner_x = lax.broadcasted_iota(jnp.int32, (BX, BY, BZ, K), 0).reshape(blocks, K)
    owner_y = lax.broadcasted_iota(jnp.int32, (BX, BY, BZ, K), 1).reshape(blocks, K)
    owner_z = lax.broadcasted_iota(jnp.int32, (BX, BY, BZ, K), 2).reshape(blocks, K)
    touch_code = touch_rows // P_SIZE
    owner_rows = (((owner_x + touch_code // 9) * (BY + 2) + owner_y + (touch_code // 3) % 3) * (BZ + 2)
                  + owner_z + touch_code % 3) * P_SIZE + touch_rows % P_SIZE
    hydro = jax.ops.segment_sum(touch_force.reshape(-1, 3), owner_rows.reshape(-1), num_segments=(BX + 2) * (BY + 2) * (BZ + 2) * P_SIZE)
    hydro = hydro.reshape(BX + 2, BY + 2, BZ + 2, P_SIZE, 3)[1:-1, 1:-1, 1:-1]
    hydro = jnp.moveaxis(hydro, -1, 3).reshape(blocks, 3, P_SIZE)

    offsets = block_offsets(27 * P_SIZE + 1, P_SIZE, CX, CY, CZ, R)
    partner_table = jnp.concatenate([records_near[:, 0:3, :], jnp.zeros((blocks, 3, 1), jnp.float32)], axis=2) + offsets[None]
    contact_rows = contacts.reshape(blocks, NC, P_SIZE)
    partner = jax.vmap(lambda table_block, rows_block: jnp.take(table_block, rows_block, axis=1))(partner_table, contact_rows)
    own_records = particles.reshape(blocks, 6, P_SIZE)
    separation = own_records[:, 0:3, None, :] - partner
    valid = (contact_rows < 27 * P_SIZE).astype(jnp.float32)
    square = jnp.sum(separation * separation, axis=1)
    soften = 1.0 + 0.25 * square
    strength = CONTACT_GAIN * valid / (soften * soften)
    contact_force = jnp.sum(separation * strength[:, None], axis=2)
    gravity = jnp.array([0.0, 0.0, GRAVITY_STEP], jnp.float32)
    velocity_new = own_records[:, 3:6] + FORCE_SCALE * hydro + contact_force - gravity[None, :, None]
    position_new = own_records[:, 0:3] + velocity_new * (SPEED_UNIT / R)

    dest_codes = dest_code.reshape(blocks, P_SIZE)
    move_x = dest_codes // 9 - 1
    move_y = (dest_codes // 3) % 3 - 1
    move_z = dest_codes % 3 - 1
    shifted = position_new - jnp.stack([move_x.astype(jnp.float32) * (CX / R), move_y.astype(jnp.float32) * (CY / R),
                                        move_z.astype(jnp.float32) * (CZ / R)], axis=1)
    record = jnp.concatenate([shifted, velocity_new], axis=1)
    home_x = owner_x[:, 0:1]
    home_y = owner_y[:, 0:1]
    home_z = owner_z[:, 0:1]
    target = (((home_x + move_x) * BY + home_y + move_y) * BZ + home_z + move_z) * P_SIZE + dest_slot.reshape(blocks, P_SIZE)
    arrived = jax.ops.segment_sum(jnp.transpose(record, (0, 2, 1)).reshape(-1, 6), target.reshape(-1), num_segments=blocks * P_SIZE)
    arrived = jnp.moveaxis(arrived.reshape(BX, BY, BZ, P_SIZE, 6), -1, 3)
    return populations_next, arrived
```

```python
import jax
import jax.numpy as jnp
from jax import lax
from jax.experimental import pallas as pl
from jax.experimental.pallas import tpu as pltpu
from jax.sharding import PartitionSpec as P

LATTICE = [
    (0, 0, 0),
    (1, 0, 0),
    (-1, 0, 0),
    (0, 1, 0),
    (0, -1, 0),
    (0, 0, 1),
    (0, 0, -1),
    (1, 1, 0),
    (-1, -1, 0),
    (1, -1, 0),
    (-1, 1, 0),
    (1, 0, 1),
    (-1, 0, -1),
    (1, 0, -1),
    (-1, 0, 1),
    (0, 1, 1),
    (0, -1, -1),
    (0, 1, -1),
    (0, -1, 1),
]
OPPOSITE = [0, 2, 1, 4, 3, 6, 5, 8, 7, 10, 9, 12, 11, 14, 13, 16, 15, 18, 17]
WEIGHTS = [1.0 / 3.0] + [1.0 / 18.0] * 6 + [1.0 / 36.0] * 12
PAIRS = [(i, i + 1) for i in range(1, 19, 2)]
RELAX_TIME = 0.8
SPEED_UNIT = 0.05
FORCE_SCALE = 0.1
CONTACT_GAIN = 1.0
GRAVITY_STEP = 0.1
R = 8.0
CX, CY, CZ, SLOTS, TOUCHES, CANDIDATES = 8, 16, 128, 128, 256, 12
SPANS = (CX / R, CY / R, CZ / R)
AXES = ("gx", "gy", "gz")
MESH = pl.DeviceIdType.MESH

X_UP, X_DOWN = [1, 7, 9, 11, 13], [2, 8, 10, 12, 14]
Y_MOVERS = [[3, 7, 10, 15, 17], [4, 9, 8, 18, 16]]
Z_MOVERS = [[5, 11, 14, 15, 18], [6, 13, 12, 17, 16]]
PLACE = {d: n for n, d in enumerate(X_UP + X_DOWN + [0, 3, 4, 5, 6, 15, 16, 17, 18])}
MOVE_CODES = [4, 10, 12, 13, 14, 16, 22]
PAD = 8


def offset_of(code):
    return (code // 9 - 1, code // 3 % 3 - 1, code % 3 - 1)


def lane_gather(table, index):
    return jnp.take_along_axis(table, index, axis=1, mode="promise_in_bounds")


def dot_lanes(a, b):
    return lax.dot_general(a, b, (((1,), (1,)), ((), ())), preferred_element_type=jnp.float32)


def kernel(
    sizes,
    pop,
    frac,
    inter,
    touch,
    part,
    cont,
    dcode,
    dslot,
    out_pop,
    out_part,
    f_v,
    frac_v,
    int_v,
    touch_v,
    cont_v,
    dcode_v,
    dslot_v,
    nb,
    mac,
    split,
    inv_v,
    inv2_v,
    cs,
    cr,
    rel,
    ys,
    yr,
    ye,
    zm,
    zs,
    zr,
    ze,
    rec,
    ds,
    dr,
    in_sem,
    pop_sem,
    a_send,
    a_recv,
    b_send,
    b_recv,
    c_send,
    c_recv,
    d_send,
    d_recv,
):
    here = [lax.axis_index(axis) for axis in AXES]

    def device(offset):
        return tuple(
            here[n] if offset[n] == 0 else lax.rem(here[n] + offset[n] + sizes[n], sizes[n])
            for n in range(3)
        )

    def exists(offset):
        ok = None
        for n in range(3):
            if isinstance(offset[n], int) and offset[n] == 0:
                continue
            there = here[n] + offset[n]
            test = (there >= 0) & (there < sizes[n])
            ok = test if ok is None else ok & test
        return ok

    others = [code for code in range(27) if code != 13]

    barrier = pltpu.get_barrier_semaphore()
    for code in others:
        pl.semaphore_signal(
            barrier, inc=1, device_id=device(offset_of(code)), device_id_type=MESH
        )

    small = [
        (part.at[0, 0, 0], nb.at[13, pl.ds(0, 6)]),
        (touch.at[0, 0], touch_v),
        (dcode.at[0, 0], dcode_v),
        (dslot.at[0, 0], dslot_v),
        (frac, frac_v),
        (inter, int_v),
        (cont.at[0, 0, 0], cont_v),
    ]
    loads = [pltpu.make_async_copy(s, d, in_sem.at[n]) for n, (s, d) in enumerate(small)]
    for load in loads:
        load.start()

    def pop_load(x):
        return pltpu.make_async_copy(pop.at[:, x], f_v.at[:, x], pop_sem.at[x])

    for x in range(CX):
        pop_load(x).start()

    lane = lax.broadcasted_iota(jnp.int32, (8, 128), 1)
    sub = lax.broadcasted_iota(jnp.int32, (8, 128), 0)

    loads[1].wait()
    loads[2].wait()
    loads[3].wait()
    entry = touch_v[0:1, :]
    wide = lax.broadcasted_iota(jnp.int32, (112, TOUCHES), 1)
    row = lax.broadcasted_iota(jnp.int32, (112, TOUCHES), 0)
    named = jnp.where((entry >> 7) == (row >> 2), wide + 1, 0).astype(jnp.float32)
    slot_row = lax.broadcasted_iota(jnp.int32, (SLOTS, TOUCHES), 0)
    placed = jnp.where((entry & 127) == slot_row, 1.0, 0.0)
    inverse = dot_lanes(named.astype(jnp.bfloat16), placed.astype(jnp.bfloat16))
    inv_v[...] = (inverse.astype(jnp.int32) - 1).reshape(14, 8, 128)
    code_row = jnp.broadcast_to(dcode_v[0:1, :], (8, 128))
    moved = jnp.concatenate(
        [jnp.where(code_row == code, lane + 1, 0).astype(jnp.float32) for code in MOVE_CODES]
        + [jnp.zeros((8, 128), jnp.float32)],
        axis=0,
    )
    tall = lax.broadcasted_iota(jnp.int32, (SLOTS, SLOTS), 0)
    landing = jnp.where(dslot_v[0:1, :] == tall, 1.0, 0.0)
    inverse2 = dot_lanes(moved.astype(jnp.bfloat16), landing.astype(jnp.bfloat16))
    inv2_v[...] = (inverse2.astype(jnp.int32) - 1).reshape(8, 8, 128)

    loads[0].wait()
    pl.semaphore_wait(barrier, 26)

    def send_a(code):
        return pltpu.make_async_remote_copy(
            src_ref=nb.at[13],
            dst_ref=nb.at[26 - code],
            send_sem=a_send.at[code],
            recv_sem=a_recv.at[26 - code],
            device_id=device(offset_of(code)),
            device_id_type=MESH,
        )

    for code in others:
        send_a(code).start()

    loads[4].wait()
    loads[5].wait()

    def moments(x, carry):
        pop_load(x).wait()
        for half in range(2):
            rows = pl.ds(8 * half, 8)
            f = [f_v[d, x, rows, :] for d in range(19)]
            rho = f[0]
            momentum = [None, None, None]
            for d in range(1, 19):
                rho = rho + f[d]
            for n in range(3):
                for d in range(1, 19):
                    if LATTICE[d][n] == 1:
                        momentum[n] = f[d] if momentum[n] is None else momentum[n] + f[d]
                for d in range(1, 19):
                    if LATTICE[d][n] == -1:
                        momentum[n] = momentum[n] - f[d]
            eps = frac_v[x, rows, :]
            weight = jnp.where(
                int_v[x, rows, :] < TOUCHES,
                eps * (RELAX_TIME - 0.5) / (1.0 - eps + (RELAX_TIME - 0.5)),
                0.0,
            )
            scale = 1.0 / rho
            mac[0, x, rows, :] = rho
            mac[1, x, rows, :] = weight
            for n in range(3):
                mac[2 + n, x, rows, :] = momentum[n] * scale
            for n, term in enumerate(momentum + [rho]):
                term = term * weight
                high = term.astype(jnp.bfloat16).astype(jnp.float32)
                start = 8 * (CY * x + 8 * half)
                split[pl.ds(start + n, 8, stride=8), :] = high
                split[pl.ds(start + 4 + n, 8, stride=8), :] = term - high
        return carry

    lax.fori_loop(0, CX, moments, 0)

    low_row = lax.broadcasted_iota(jnp.int32, (32, 128), 0)

    def add_slab(x, total):
        left, right = [], []
        for y in range(CY):
            slots = int_v[x, pl.ds(y, 1), :]
            tile = split[pl.ds(pl.multiple_of(8 * (CY * x + y), 8), 8), :]
            upper = jnp.broadcast_to(slots >> 5, (8, 128))
            picked = [jnp.where(upper == a, tile, 0.0) for a in range(8)]
            left.append(jnp.concatenate(picked, axis=0).astype(jnp.bfloat16))
            lower = jnp.broadcast_to(slots & 31, (32, 128))
            right.append(jnp.where(lower == low_row, 1.0, 0.0).astype(jnp.bfloat16))
        return total + dot_lanes(
            jnp.concatenate(left, axis=1), jnp.concatenate(right, axis=1)
        )

    total = lax.fori_loop(0, CX, add_slab, jnp.zeros((64, 32), jnp.float32))
    tables = []
    for h in range(2):
        table = jnp.concatenate(
            [total[8 * a : 8 * a + 8, :] for a in range(4 * h, 4 * h + 4)], axis=1
        )
        tables.append(table + pltpu.roll(table, 4, 0))

    for q in range(14):
        source = inv_v[q]
        index = source & 127
        picked = jnp.where(
            source < 128, lane_gather(tables[0], index), lane_gather(tables[1], index)
        )
        picked = jnp.where(source >= 0, picked, 0.0)
        cs[2 * q] = picked[0:4, :]
        cs[2 * q + 1] = picked[4:8, :]

    def send_c(code):
        return pltpu.make_async_remote_copy(
            src_ref=cs.at[code],
            dst_ref=cr.at[26 - code],
            send_sem=c_send.at[code],
            recv_sem=c_recv.at[26 - code],
            device_id=device(offset_of(code)),
            device_id_type=MESH,
        )

    for code in others:
        send_c(code).start()

    def relax(x, carry):
        for half in range(2):
            rows = pl.ds(8 * half, 8)
            dest = pl.ds(PAD + 8 * half, 8)
            rho = mac[0, x, rows, :]
            weight = mac[1, x, rows, :]
            u = [mac[2 + n, x, rows, :] for n in range(3)]
            alpha = (1.0 - weight) * (1.0 / RELAX_TIME)
            keep = 1.0 - alpha - weight
            even = (alpha - weight) * rho
            odd = 3.0 * (alpha + weight) * rho
            base = even * (1.0 - 1.5 * (u[0] * u[0] + u[1] * u[1] + u[2] * u[2]))
            even = 4.5 * even
            rel[PLACE[0], x + 1, dest, :] = (1.0 - alpha) * f_v[0, x, rows, :] + WEIGHTS[0] * base
            for i, j in PAIRS:
                along = None
                for n in range(3):
                    if LATTICE[i][n] == 1:
                        along = u[n] if along is None else along + u[n]
                    elif LATTICE[i][n] == -1:
                        along = -u[n] if along is None else along - u[n]
                symmetric = WEIGHTS[i] * (base + even * along * along)
                skew = WEIGHTS[i] * (odd * along)
                fi, fj = f_v[i, x, rows, :], f_v[j, x, rows, :]
                rel[PLACE[i], x + 1, dest, :] = keep * fi + weight * fj + (symmetric + skew)
                rel[PLACE[j], x + 1, dest, :] = keep * fj + weight * fi + (symmetric - skew)
        return carry

    lax.fori_loop(0, CX, relax, 0)

    for code in others:
        send_a(code).wait()

    def mask_records(code, carry):
        ok = exists((code // 9 - 1, code // 3 % 3 - 1, code % 3 - 1))
        nb[code] = jnp.where(ok, nb[code], 0.0)
        return carry

    lax.fori_loop(0, 27, mask_records, 0)

    touch_code = [jnp.broadcast_to(touch_v[0:1, pl.ds(128 * h, 128)] >> 7, (8, 128)) for h in range(2)]
    touch_slot = [jnp.broadcast_to(touch_v[0:1, pl.ds(128 * h, 128)] & 127, (8, 128)) for h in range(2)]

    def find_velocity(code, found):
        tile = nb[code]
        return tuple(
            jnp.where(touch_code[h] == code, lane_gather(tile, touch_slot[h]), found[h])
            for h in range(2)
        )

    zero = jnp.zeros((8, 128), jnp.float32)
    found = lax.fori_loop(0, 27, find_velocity, (zero, zero))
    speed = [
        [jnp.broadcast_to(SPEED_UNIT * found[h][3 + n : 4 + n, :], (8, 128)) for n in range(3)]
        for h in range(2)
    ]

    def solid(x, carry):
        for half in range(2):
            rows = pl.ds(8 * half, 8)
            dest = pl.ds(PAD + 8 * half, 8)
            slots = int_v[x, rows, :]
            index = slots & 127
            first = slots < 128
            v = [
                jnp.where(first, lane_gather(speed[0][n], index), lane_gather(speed[1][n], index))
                for n in range(3)
            ]
            mass = mac[0, x, rows, :] * mac[1, x, rows, :]
            base = mass * (1.0 - 1.5 * (v[0] * v[0] + v[1] * v[1] + v[2] * v[2]))
            even = 4.5 * mass
            odd = 3.0 * mass
            relaxed = {}
            relaxed[0] = rel[PLACE[0], x + 1, dest, :] + WEIGHTS[0] * base
            for i, j in PAIRS:
                along = None
                for n in range(3):
                    if LATTICE[i][n] == 1:
                        along = v[n] if along is None else along + v[n]
                    elif LATTICE[i][n] == -1:
                        along = -v[n] if along is None else along - v[n]
                symmetric = WEIGHTS[i] * (base + even * along * along)
                skew = WEIGHTS[i] * (odd * along)
                relaxed[i] = rel[PLACE[i], x + 1, dest, :] + (symmetric + skew)
                relaxed[j] = rel[PLACE[j], x + 1, dest, :] + (symmetric - skew)
            for d in range(19):
                rel[PLACE[d], x + 1, dest, :] = relaxed[d]
            packed = zero
            for side in range(2):
                edge = 127 if side == 0 else 0
                for n, d in enumerate(Z_MOVERS[side]):
                    packed = jnp.where(
                        lane == 8 * side + n, relaxed[d][:, edge : edge + 1], packed
                    )
            zm[pl.ds(pl.multiple_of(CY * x + 8 * half, 8), 8), :] = packed
            side = 1 - half
            edge = 7 if side == 0 else 0
            for n, d in enumerate(Y_MOVERS[side]):
                target = lax.rem(x + LATTICE[d][0] + CX, CX)
                ys[side, n, pl.ds(target, 1), :] = relaxed[d][edge : edge + 1, :]
        return carry

    lax.fori_loop(0, CX, solid, 0)

    across = jnp.transpose(zm[...])
    for side in range(2):
        tile = across[8 * side : 8 * side + 8, :]
        up_y = jnp.where((lane & 15) == 0, pltpu.roll(tile, 128 - 15, 1), pltpu.roll(tile, 1, 1))
        down_y = jnp.where((lane & 15) == 15, pltpu.roll(tile, 15, 1), pltpu.roll(tile, 127, 1))
        tile = jnp.where(sub == 1, pltpu.roll(tile, 16, 1), tile)
        tile = jnp.where(sub == 2, pltpu.roll(tile, 112, 1), tile)
        tile = jnp.where(sub == 3, up_y, tile)
        zs[side] = jnp.where(sub == 4, down_y, tile)

    body_rows = pl.ds(PAD, CY)
    moves = [
        (rel.at[pl.ds(0, 5), CX, body_rows], rel.at[pl.ds(0, 5), 0, body_rows], (1, 0, 0)),
        (rel.at[pl.ds(5, 5), 1, body_rows], rel.at[pl.ds(5, 5), CX + 1, body_rows], (-1, 0, 0)),
    ]
    for side in range(2):
        step = 1 - 2 * side
        moves.append((ys.at[side], yr.at[side], (0, step, 0)))
        moves.append((ys.at[side, 1], ye.at[side, 0], (1, step, 0)))
        moves.append((ys.at[side, 2], ye.at[side, 1], (-1, step, 0)))
        moves.append((zs.at[side], zr.at[side], (0, 0, step)))
        moves.append((zs.at[side], ze.at[side, 0], (1, 0, step)))
        moves.append((zs.at[side], ze.at[side, 1], (-1, 0, step)))
        moves.append((zs.at[side], ze.at[side, 2], (0, 1, step)))
        moves.append((zs.at[side], ze.at[side, 3], (0, -1, step)))
    b_copies = [
        pltpu.make_async_remote_copy(
            src_ref=source,
            dst_ref=target,
            send_sem=b_send.at[n],
            recv_sem=b_recv.at[n],
            device_id=device(offset),
            device_id_type=MESH,
        )
        for n, (source, target, offset) in enumerate(moves)
    ]
    for copy in b_copies:
        copy.start()

    loads[6].wait()
    listed = [
        cont_v[0:8, :],
        jnp.concatenate([cont_v[8:12, :], jnp.full((4, 128), 27 * SLOTS, jnp.int32)], axis=0),
    ]
    listed_code = [entries >> 7 for entries in listed]
    listed_slot = [entries & 127 for entries in listed]

    def find_partner(code, partner):
        shifts = (code // 9 - 1, code // 3 % 3 - 1, code % 3 - 1)
        result = []
        for n in range(3):
            line = nb[code, pl.ds(n, 1), :] + shifts[n].astype(jnp.float32) * SPANS[n]
            line = jnp.broadcast_to(line, (8, 128))
            for h in range(2):
                result.append(
                    jnp.where(
                        listed_code[h] == code,
                        lane_gather(line, listed_slot[h]),
                        partner[2 * n + h],
                    )
                )
        return tuple(result)

    partner = lax.fori_loop(0, 27, find_partner, (zero,) * 6)
    force = [None, None, None]
    for h in range(2):
        apart = [nb[13, n : n + 1, :] - partner[2 * n + h] for n in range(3)]
        square = apart[0] * apart[0] + apart[1] * apart[1] + apart[2] * apart[2]
        soften = 1.0 + 0.25 * square
        strength = jnp.where(listed_code[h] < 27, CONTACT_GAIN / (soften * soften), 0.0)
        for n in range(3):
            term = jnp.sum(apart[n] * strength, axis=0, keepdims=True)
            force[n] = term if h == 0 else force[n] + term

    for code in others:
        send_c(code).wait()
    hydro = cs[13]
    for code in others:
        hydro = hydro + jnp.where(exists(offset_of(code)), cr[code], 0.0)
    rec[6:8, :] = jnp.zeros((2, 128), jnp.float32)
    for n in range(3):
        speed_old = nb[13, 3 + n : 4 + n, :]
        pulled = hydro[n : n + 1, :] - (SPEED_UNIT * speed_old) * hydro[3:4, :]
        speed_new = speed_old + FORCE_SCALE * pulled + force[n]
        if n == 2:
            speed_new = speed_new - GRAVITY_STEP
        rec[3 + n : 4 + n, :] = speed_new
        rec[n : n + 1, :] = nb[13, n : n + 1, :] + speed_new * (SPEED_UNIT / R)

    record = rec[...]
    for n, code in enumerate(MOVE_CODES):
        shift = zero
        for axis, step in enumerate(offset_of(code)):
            if step != 0:
                shift = jnp.where(sub == axis, step * SPANS[axis], shift)
        source = inv2_v[n]
        picked = lane_gather(record - shift, source & 127)
        ds[n] = jnp.where(source >= 0, picked, 0.0)
    d_copies = [
        pltpu.make_async_remote_copy(
            src_ref=ds.at[n],
            dst_ref=dr.at[6 - n],
            send_sem=d_send.at[n],
            recv_sem=d_recv.at[6 - n],
            device_id=device(offset_of(code)),
            device_id_type=MESH,
        )
        for n, code in enumerate(MOVE_CODES)
        if code != 13
    ]
    for copy in d_copies:
        copy.start()

    for copy in b_copies:
        copy.wait()
    for side in range(2):
        at = PAD - 1 if side == 0 else PAD + CY
        for n, d in enumerate(Y_MOVERS[side]):
            tile = yr[side, n]
            if n == 1:
                tile = jnp.where(sub == 0, ye[side, 0], tile)
            if n == 2:
                tile = jnp.where(sub == CX - 1, ye[side, 1], tile)
            for x in range(CX):
                rel[PLACE[d], x + 1 - LATTICE[d][0], at : at + 1, :] = tile[x : x + 1, :]
    columns = []
    for side in range(2):
        tile = zr[side]
        tile = jnp.where((sub == 1) & (lane < CY), ze[side, 0], tile)
        tile = jnp.where((sub == 2) & (lane >= 128 - CY), ze[side, 1], tile)
        tile = jnp.where((sub == 3) & ((lane & 15) == 0), ze[side, 2], tile)
        tile = jnp.where((sub == 4) & ((lane & 15) == 15), ze[side, 3], tile)
        columns.append(tile)
    zm[...] = jnp.transpose(
        jnp.concatenate(columns + [jnp.zeros((112, 128), jnp.float32)], axis=0)
    )

    low_wall = [here[n] == 0 for n in range(3)]
    high_wall = [here[n] == sizes[n] - 1 for n in range(3)]

    def stream(x, carry):
        for half in range(2):
            rows = pl.ds(8 * half, 8)
            beside = zm[pl.ds(pl.multiple_of(CY * x + 8 * half, 8), 8), :]
            walls = {
                (0, 1): low_wall[0] & (x == 0),
                (0, -1): high_wall[0] & (x == CX - 1),
                (2, 1): low_wall[2] & (lane == 0),
                (2, -1): high_wall[2] & (lane == 127),
            }
            if half == 0:
                walls[(1, 1)] = low_wall[1] & (sub == 0)
            else:
                walls[(1, -1)] = high_wall[1] & (sub == 7)
            for d in range(19):
                vector = LATTICE[d]
                value = rel[
                    PLACE[d], x + 1 - vector[0], pl.ds(PAD + 8 * half - vector[1], 8), :
                ]
                if vector[2] != 0:
                    side = 0 if vector[2] == 1 else 1
                    column = 8 * side + Z_MOVERS[side].index(d)
                    edge = 0 if side == 0 else 127
                    value = jnp.where(
                        lane == edge,
                        beside[:, column : column + 1],
                        pltpu.roll(value, vector[2] % 128, 1),
                    )
                blocked = None
                for axis in range(3):
                    wall = walls.get((axis, vector[axis]))
                    if vector[axis] != 0 and wall is not None:
                        blocked = wall if blocked is None else blocked | wall
                if blocked is not None:
                    back = rel[PLACE[OPPOSITE[d]], x + 1, pl.ds(PAD + 8 * half, 8), :]
                    value = jnp.where(blocked, back, value)
                out_pop[d, x, rows, :] = value
        return carry

    lax.fori_loop(0, CX, stream, 0)

    for copy in d_copies:
        copy.wait()
    arrived = ds[3]
    for n in range(7):
        if n != 3:
            arrived = arrived + dr[n]
    out_part[0, 0, 0] = arrived[0:6, :]


def body(sizes, *args):
    f32, i32 = jnp.float32, jnp.int32
    vmem = pltpu.VMEM
    sems = pltpu.SemaphoreType.DMA
    return pl.pallas_call(
        lambda *refs: kernel(sizes, *refs),
        out_shape=(
            jax.ShapeDtypeStruct((19, CX, CY, CZ), f32),
            jax.ShapeDtypeStruct((1, 1, 1, 6, SLOTS), f32),
        ),
        in_specs=[pl.BlockSpec(memory_space=pl.ANY)] * 8,
        out_specs=(
            pl.BlockSpec(memory_space=vmem),
            pl.BlockSpec(memory_space=vmem),
        ),
        scratch_shapes=[
            vmem((19, CX, CY, CZ), f32),
            vmem((CX, CY, CZ), f32),
            vmem((CX, CY, CZ), i32),
            vmem((1, TOUCHES), i32),
            vmem((CANDIDATES, SLOTS), i32),
            vmem((1, SLOTS), i32),
            vmem((1, SLOTS), i32),
            vmem((27, 8, 128), f32),
            vmem((5, CX, CY, CZ), f32),
            vmem((8 * CX * CY, CZ), f32),
            vmem((14, 8, 128), i32),
            vmem((8, 8, 128), i32),
            vmem((28, 4, 128), f32),
            vmem((27, 4, 128), f32),
            vmem((19, CX + 2, CY + 2 * PAD, CZ), f32),
            vmem((2, 5, CX, CZ), f32),
            vmem((2, 5, CX, CZ), f32),
            vmem((2, 2, CX, CZ), f32),
            vmem((CX * CY, 128), f32),
            vmem((2, 8, 128), f32),
            vmem((2, 8, 128), f32),
            vmem((2, 4, 8, 128), f32),
            vmem((8, 128), f32),
            vmem((7, 8, 128), f32),
            vmem((7, 8, 128), f32),
            sems((7,)),
            sems((CX,)),
            sems((27,)),
            sems((27,)),
            sems((18,)),
            sems((18,)),
            sems((27,)),
            sems((27,)),
            sems((7,)),
            sems((7,)),
        ],
        compiler_params=pltpu.CompilerParams(collective_id=0, has_side_effects=True),
    )(*args)


def solution(mesh):
    sizes = tuple(mesh.shape[axis] for axis in AXES)
    cells, blocks = P(*AXES), P(*AXES, None)
    records = P(*AXES, None, None)
    fields = P(None, *AXES)
    return jax.shard_map(
        lambda *args: body(sizes, *args),
        mesh=mesh,
        in_specs=(fields, cells, cells, blocks, records, records, blocks, blocks),
        out_specs=(fields, records),
        check_vma=False,
    )
```

```python
import jax
import jax.numpy as jnp
from jax import lax
from jax.experimental import pallas as pl
from jax.experimental.pallas import tpu as pltpu
from jax.sharding import PartitionSpec as P

LATTICE = [
    (0, 0, 0),
    (1, 0, 0),
    (-1, 0, 0),
    (0, 1, 0),
    (0, -1, 0),
    (0, 0, 1),
    (0, 0, -1),
    (1, 1, 0),
    (-1, -1, 0),
    (1, -1, 0),
    (-1, 1, 0),
    (1, 0, 1),
    (-1, 0, -1),
    (1, 0, -1),
    (-1, 0, 1),
    (0, 1, 1),
    (0, -1, -1),
    (0, 1, -1),
    (0, -1, 1),
]
OPPOSITE = [0, 2, 1, 4, 3, 6, 5, 8, 7, 10, 9, 12, 11, 14, 13, 16, 15, 18, 17]
WEIGHTS = [1.0 / 3.0] + [1.0 / 18.0] * 6 + [1.0 / 36.0] * 12
PAIRS = [(i, i + 1) for i in range(1, 19, 2)]
RELAX_TIME = 0.8
SPEED_UNIT = 0.05
FORCE_SCALE = 0.1
CONTACT_GAIN = 1.0
GRAVITY_STEP = 0.1
R = 8.0
CX, CY, CZ, SLOTS, TOUCHES, CANDIDATES = 8, 16, 128, 128, 256, 12
SPANS = (CX / R, CY / R, CZ / R)
AXES = ("gx", "gy", "gz")
MESH = pl.DeviceIdType.MESH

X_UP, X_DOWN = [1, 7, 9, 11, 13], [2, 8, 10, 12, 14]
Y_MOVERS = [[3, 7, 10, 15, 17], [4, 9, 8, 18, 16]]
Z_MOVERS = [[5, 11, 14, 15, 18], [6, 13, 12, 17, 16]]
PLACE = {d: n for n, d in enumerate(X_UP + X_DOWN + [0, 3, 4, 5, 6, 15, 16, 17, 18])}
MOVE_CODES = [4, 10, 12, 13, 14, 16, 22]
PAD = 8
STRIDE = CY + 2 * PAD


def offset_of(code):
    return (code // 9 - 1, code // 3 % 3 - 1, code % 3 - 1)


def projected(velocity, d):
    along = None
    for n in range(3):
        if LATTICE[d][n] == 1:
            along = velocity[n] if along is None else along + velocity[n]
        elif LATTICE[d][n] == -1:
            along = -velocity[n] if along is None else along - velocity[n]
    return along


def lane_gather(table, index):
    return jnp.take_along_axis(table, index, axis=1, mode="promise_in_bounds")


def dot_lanes(a, b):
    return lax.dot_general(a, b, (((1,), (1,)), ((), ())), preferred_element_type=jnp.float32)


def kernel(
    sizes,
    pop,
    frac,
    inter,
    touch,
    part,
    cont,
    dcode,
    dslot,
    rel_out,
    col_out,
    out_part,
    f_v,
    frac_v,
    int_v,
    touch_v,
    cont_v,
    dcode_v,
    dslot_v,
    nb,
    mac,
    split,
    inv_v,
    inv2_v,
    cs,
    cr,
    zc,
    xs,
    xr,
    ys,
    yr,
    ye,
    zm,
    zs,
    zr,
    ze,
    rec,
    ds,
    dr,
    in_sem,
    pop_sem,
    a_send,
    a_recv,
    b_send,
    b_recv,
    c_send,
    c_recv,
    d_send,
    d_recv,
):
    rel = rel_out
    here = [lax.axis_index(axis) for axis in AXES]

    def device(offset):
        return tuple(
            here[n] if offset[n] == 0 else lax.rem(here[n] + offset[n] + sizes[n], sizes[n])
            for n in range(3)
        )

    def exists(offset):
        ok = None
        for n in range(3):
            if offset[n] != 0:
                test = here[n] > 0 if offset[n] < 0 else here[n] < sizes[n] - 1
                ok = test if ok is None else ok & test
        return ok

    others = [code for code in range(27) if code != 13]
    others.sort(key=lambda code: -sum(abs(step) for step in offset_of(code)))
    ok = {code: exists(offset_of(code)) for code in others}
    around = [
        1 + (here[n] > 0).astype(jnp.int32) + (here[n] < sizes[n] - 1).astype(jnp.int32)
        for n in range(3)
    ]

    def start_all(make):
        for code in others:
            pl.when(ok[code])(lambda code=code: make(code).start())

    def wait_all(make):
        for code in others:

            @pl.when(ok[code])
            def _(code=code):
                make(26 - code).wait_recv()
                make(code).wait_send()

    barrier = pltpu.get_barrier_semaphore()
    for code in others:

        @pl.when(ok[code])
        def _(code=code):
            pl.semaphore_signal(
                barrier, inc=1, device_id=device(offset_of(code)), device_id_type=MESH
            )

    small = [
        (part.at[0, 0, :, 0], nb.at[13, pl.ds(0, 6)]),
        (touch.at[0, 0], touch_v),
        (dcode.at[0, 0], dcode_v),
        (dslot.at[0, 0], dslot_v),
        (frac, frac_v),
        (inter, int_v),
        (cont.at[0, 0, :, 0], cont_v),
    ]
    loads = [pltpu.make_async_copy(s, d, in_sem.at[n]) for n, (s, d) in enumerate(small)]
    for load in loads:
        load.start()

    def pop_load(x):
        return pltpu.make_async_copy(
            pop.at[:, pl.ds(CY * x, CY)], f_v.at[:, pl.ds(CY * x, CY)], pop_sem.at[x]
        )

    for x in range(CX):
        pop_load(x).start()

    lane = lax.broadcasted_iota(jnp.int32, (8, 128), 1)
    sub = lax.broadcasted_iota(jnp.int32, (8, 128), 0)

    loads[0].wait()
    pl.semaphore_wait(barrier, around[0] * around[1] * around[2] - 1)

    def send_a(code):
        return pltpu.make_async_remote_copy(
            src_ref=nb.at[13],
            dst_ref=nb.at[26 - code],
            send_sem=a_send.at[code],
            recv_sem=a_recv.at[26 - code],
            device_id=device(offset_of(code)),
            device_id_type=MESH,
        )

    start_all(send_a)

    loads[1].wait()
    loads[2].wait()
    loads[3].wait()
    entry = touch_v[0:1, :]
    wide = lax.broadcasted_iota(jnp.int32, (112, TOUCHES), 1)
    row = lax.broadcasted_iota(jnp.int32, (112, TOUCHES), 0)
    named = jnp.where((entry >> 7) == (row >> 2), wide + 1, 0).astype(jnp.float32)
    slot_row = lax.broadcasted_iota(jnp.int32, (SLOTS, TOUCHES), 0)
    placed = jnp.where((entry & 127) == slot_row, 1.0, 0.0)
    inverse = dot_lanes(named.astype(jnp.bfloat16), placed.astype(jnp.bfloat16))
    inv_v[...] = (inverse.astype(jnp.int32) - 1).reshape(14, 8, 128)
    code_row = jnp.broadcast_to(dcode_v[0:1, :], (8, 128))
    moved = jnp.concatenate(
        [jnp.where(code_row == code, lane + 1, 0).astype(jnp.float32) for code in MOVE_CODES]
        + [jnp.zeros((8, 128), jnp.float32)],
        axis=0,
    )
    tall = lax.broadcasted_iota(jnp.int32, (SLOTS, SLOTS), 0)
    landing = jnp.where(dslot_v[0:1, :] == tall, 1.0, 0.0)
    inverse2 = dot_lanes(moved.astype(jnp.bfloat16), landing.astype(jnp.bfloat16))
    inv2_v[...] = (inverse2.astype(jnp.int32) - 1).reshape(8, 8, 128)

    loads[4].wait()
    loads[5].wait()

    def moments(x, carry):
        pop_load(x).wait()
        for half in range(2):
            start = pl.multiple_of(CY * x + 8 * half, 8)
            rows = pl.ds(start, 8)
            f = [f_v[d, rows, :] for d in range(19)]
            rho = f[0]
            momentum = [None, None, None]
            for d in range(1, 19):
                rho = rho + f[d]
            for n in range(3):
                for d in range(1, 19):
                    if LATTICE[d][n] == 1:
                        momentum[n] = f[d] if momentum[n] is None else momentum[n] + f[d]
                for d in range(1, 19):
                    if LATTICE[d][n] == -1:
                        momentum[n] = momentum[n] - f[d]
            eps = frac_v[rows, :]
            weight = jnp.where(
                int_v[rows, :] < TOUCHES,
                eps * (RELAX_TIME - 0.5) / (1.0 - eps + (RELAX_TIME - 0.5)),
                0.0,
            )
            scale = 1.0 / rho
            mac[0, rows, :] = rho
            mac[1, rows, :] = weight
            for n in range(3):
                mac[2 + n, rows, :] = momentum[n] * scale
            for n, term in enumerate(momentum + [rho]):
                term = term * weight
                if n == 3:
                    mac[5, rows, :] = term
                high = term.astype(jnp.bfloat16).astype(jnp.float32)
                split[pl.ds(8 * start + n, 8, stride=8), :] = high
                split[pl.ds(8 * start + 4 + n, 8, stride=8), :] = term - high
        return carry

    lax.fori_loop(0, CX, moments, 0, unroll=2)

    low_row = lax.broadcasted_iota(jnp.int32, (32, 128), 0)

    def add_slab(x, total):
        left, right = [], []
        for y in range(CY):
            slots = int_v[pl.ds(CY * x + y, 1), :]
            tile = split[pl.ds(pl.multiple_of(8 * (CY * x + y), 8), 8), :]
            upper = jnp.broadcast_to(slots >> 5, (8, 128))
            picked = [jnp.where(upper == a, tile, 0.0) for a in range(8)]
            left.append(jnp.concatenate(picked, axis=0).astype(jnp.bfloat16))
            lower = jnp.broadcast_to(slots & 31, (32, 128))
            right.append(jnp.where(lower == low_row, 1.0, 0.0).astype(jnp.bfloat16))
        return total + dot_lanes(
            jnp.concatenate(left, axis=1), jnp.concatenate(right, axis=1)
        )

    total = lax.fori_loop(0, CX, add_slab, jnp.zeros((64, 32), jnp.float32), unroll=4)
    tables = []
    for h in range(2):
        table = jnp.concatenate(
            [total[8 * a : 8 * a + 8, :] for a in range(4 * h, 4 * h + 4)], axis=1
        )
        tables.append(table + pltpu.roll(table, 4, 0))

    for q in range(14):
        source = inv_v[q]
        index = source & 127
        picked = jnp.where(
            source < 128, lane_gather(tables[0], index), lane_gather(tables[1], index)
        )
        picked = jnp.where(source >= 0, picked, 0.0)
        cs[2 * q] = picked[0:4, :]
        cs[2 * q + 1] = picked[4:8, :]

    def send_c(code):
        return pltpu.make_async_remote_copy(
            src_ref=cs.at[code],
            dst_ref=cr.at[26 - code],
            send_sem=c_send.at[code],
            recv_sem=c_recv.at[26 - code],
            device_id=device(offset_of(code)),
            device_id_type=MESH,
        )

    start_all(send_c)

    def cell_rows(x, half):
        cells = pl.ds(pl.multiple_of(CY * x + 8 * half, 8), 8)
        return cells, pl.ds(pl.multiple_of(STRIDE * (x + 1) + PAD + 8 * half, 8), 8)

    def relax(x, carry):
        for half in range(2):
            rows, dest = cell_rows(x, half)
            rho = mac[0, rows, :]
            weight = mac[1, rows, :]
            u = [mac[2 + n, rows, :] for n in range(3)]
            alpha = (1.0 - weight) * (1.0 / RELAX_TIME)
            keep = 1.0 - alpha - weight
            even = (alpha - weight) * rho
            odd = 3.0 * (alpha + weight) * rho
            base = even * (1.0 - 1.5 * (u[0] * u[0] + u[1] * u[1] + u[2] * u[2]))
            even = 4.5 * even
            rel[PLACE[0], dest, :] = (1.0 - alpha) * f_v[0, rows, :] + WEIGHTS[0] * base
            for i, j in PAIRS:
                along = projected(u, i)
                symmetric = WEIGHTS[i] * (base + even * along * along)
                skew = WEIGHTS[i] * (odd * along)
                fi, fj = f_v[i, rows, :], f_v[j, rows, :]
                rel[PLACE[i], dest, :] = keep * fi + weight * fj + (symmetric + skew)
                rel[PLACE[j], dest, :] = keep * fj + weight * fi + (symmetric - skew)
        return carry

    lax.fori_loop(0, CX, relax, 0, unroll=2)

    def pack_ends(x, carry):
        for half in range(2):
            rows, dest = cell_rows(x, half)
            packed = jnp.zeros((8, 128), jnp.float32)
            for side in range(2):
                edge = 127 if side == 0 else 0
                values = [rel[PLACE[d], dest, :] for d in Z_MOVERS[side]]
                values += [mac[5, rows, :], int_v[rows, :].astype(jnp.float32)]
                for n, value in enumerate(values):
                    packed = jnp.where(lane == 8 * side + n, value[:, edge : edge + 1], packed)
            zm[rows, :] = packed
        return carry

    lax.fori_loop(0, CX, pack_ends, 0, unroll=CX)
    zc[...] = jnp.transpose(zm[...])[0:16, :]

    wait_all(send_a)

    for code in others:
        nb[code] = jnp.where(ok[code], nb[code], 0.0)

    touch_code = [jnp.broadcast_to(touch_v[0:1, pl.ds(128 * h, 128)] >> 7, (8, 128)) for h in range(2)]
    touch_slot = [jnp.broadcast_to(touch_v[0:1, pl.ds(128 * h, 128)] & 127, (8, 128)) for h in range(2)]

    def find_velocity(code, found):
        tile = nb[code]
        return tuple(
            jnp.where(touch_code[h] == code, lane_gather(tile, touch_slot[h]), found[h])
            for h in range(2)
        )

    zero = jnp.zeros((8, 128), jnp.float32)
    found = lax.fori_loop(0, 27, find_velocity, (zero, zero), unroll=27)
    speed = [
        [jnp.broadcast_to(SPEED_UNIT * found[h][3 + n : 4 + n, :], (8, 128)) for n in range(3)]
        for h in range(2)
    ]

    def solid_part(slots, mass):
        index = slots & 127
        first = slots < 128
        v = [
            jnp.where(first, lane_gather(speed[0][n], index), lane_gather(speed[1][n], index))
            for n in range(3)
        ]
        base = mass * (1.0 - 1.5 * (v[0] * v[0] + v[1] * v[1] + v[2] * v[2]))
        return v, base, 4.5 * mass, 3.0 * mass

    def solid_term(parts, d):
        v, base, even, odd = parts
        along = projected(v, d)
        return WEIGHTS[d] * (base + along * (even * along + odd))

    for side in range(2):
        x = CX - 1 if side == 0 else 0
        for half in range(2):
            rows, dest = cell_rows(x, half)
            parts = solid_part(int_v[rows, :], mac[5, rows, :])
            for n, d in enumerate((X_UP, X_DOWN)[side]):
                value = rel[PLACE[d], dest, :] + solid_term(parts, d)
                xs[side, n, pl.ds(8 * half, 8), :] = value
    for side in range(2):
        y = CY - 1 if side == 0 else 0
        rows = pl.ds(y, CX, stride=CY)
        dest = pl.ds(STRIDE + PAD + y, CX, stride=STRIDE)
        parts = solid_part(int_v[rows, :], mac[5, rows, :])
        for n, d in enumerate(Y_MOVERS[side]):
            value = rel[PLACE[d], dest, :] + solid_term(parts, d)
            if LATTICE[d][0] != 0:
                value = pltpu.roll(value, LATTICE[d][0] % CX, 0)
            ys[side, n] = value
    for side in range(2):
        slots = jnp.broadcast_to(zc[8 * side + 6 : 8 * side + 7, :].astype(jnp.int32), (8, 128))
        mass = jnp.broadcast_to(zc[8 * side + 5 : 8 * side + 6, :], (8, 128))
        v, base, even, odd = solid_part(slots, mass)
        along = zero
        share = jnp.full((8, 128), 1.0 / 36.0, jnp.float32)
        for n, d in enumerate(Z_MOVERS[side]):
            along = jnp.where(sub == n, projected(v, d), along)
        share = jnp.where(sub == 0, 1.0 / 18.0, share)
        tile = zc[8 * side : 8 * side + 8, :] + share * (base + along * (even * along + odd))
        up_y = jnp.where((lane & 15) == 0, pltpu.roll(tile, 128 - 15, 1), pltpu.roll(tile, 1, 1))
        down_y = jnp.where((lane & 15) == 15, pltpu.roll(tile, 15, 1), pltpu.roll(tile, 127, 1))
        moved_z = jnp.where(sub == 1, pltpu.roll(tile, 16, 1), tile)
        moved_z = jnp.where(sub == 2, pltpu.roll(tile, 112, 1), moved_z)
        moved_z = jnp.where(sub == 3, up_y, moved_z)
        zs[side] = jnp.where(sub == 4, down_y, moved_z)

    moves = []
    for side in range(2):
        step = 1 - 2 * side
        moves.append((xs.at[side], xr.at[side], (step, 0, 0)))
        moves.append((ys.at[side], yr.at[side], (0, step, 0)))
        moves.append((ys.at[side, 1], ye.at[side, 0], (1, step, 0)))
        moves.append((ys.at[side, 2], ye.at[side, 1], (-1, step, 0)))
        moves.append((zs.at[side], zr.at[side], (0, 0, step)))
        moves.append((zs.at[side], ze.at[side, 0], (1, 0, step)))
        moves.append((zs.at[side], ze.at[side, 1], (-1, 0, step)))
        moves.append((zs.at[side], ze.at[side, 2], (0, 1, step)))
        moves.append((zs.at[side], ze.at[side, 3], (0, -1, step)))
    def send_b(n):
        source, target, offset = moves[n]
        return pltpu.make_async_remote_copy(
            src_ref=source,
            dst_ref=target,
            send_sem=b_send.at[n],
            recv_sem=b_recv.at[n],
            device_id=device(offset),
            device_id_type=MESH,
        )

    def code_of(offset):
        return 9 * (offset[0] + 1) + 3 * (offset[1] + 1) + offset[2] + 1

    for n in range(len(moves)):
        pl.when(ok[code_of(moves[n][2])])(lambda n=n: send_b(n).start())

    def solid(x, carry):
        for half in range(2):
            rows, dest = cell_rows(x, half)
            v, base, even, odd = solid_part(int_v[rows, :], mac[5, rows, :])
            rel[PLACE[0], dest, :] = rel[PLACE[0], dest, :] + WEIGHTS[0] * base
            for i, j in PAIRS:
                along = projected(v, i)
                symmetric = WEIGHTS[i] * (base + even * along * along)
                skew = WEIGHTS[i] * (odd * along)
                rel[PLACE[i], dest, :] = rel[PLACE[i], dest, :] + (symmetric + skew)
                rel[PLACE[j], dest, :] = rel[PLACE[j], dest, :] + (symmetric - skew)
        return carry

    lax.fori_loop(0, CX, solid, 0, unroll=CX)

    loads[6].wait()
    listed = [
        cont_v[0:8, :],
        jnp.concatenate([cont_v[8:12, :], jnp.full((4, 128), 27 * SLOTS, jnp.int32)], axis=0),
    ]
    listed_code = [entries >> 7 for entries in listed]
    listed_slot = [entries & 127 for entries in listed]

    def find_partner(code, partner):
        shifts = (code // 9 - 1, code // 3 % 3 - 1, code % 3 - 1)
        result = []
        for n in range(3):
            line = nb[code, pl.ds(n, 1), :] + shifts[n].astype(jnp.float32) * SPANS[n]
            line = jnp.broadcast_to(line, (8, 128))
            for h in range(2):
                result.append(
                    jnp.where(
                        listed_code[h] == code,
                        lane_gather(line, listed_slot[h]),
                        partner[2 * n + h],
                    )
                )
        return tuple(result)

    partner = lax.fori_loop(0, 27, find_partner, (zero,) * 6, unroll=27)
    force = [None, None, None]
    for h in range(2):
        apart = [nb[13, n : n + 1, :] - partner[2 * n + h] for n in range(3)]
        square = apart[0] * apart[0] + apart[1] * apart[1] + apart[2] * apart[2]
        soften = 1.0 + 0.25 * square
        strength = jnp.where(listed_code[h] < 27, CONTACT_GAIN / (soften * soften), 0.0)
        for n in range(3):
            term = jnp.sum(apart[n] * strength, axis=0, keepdims=True)
            force[n] = term if h == 0 else force[n] + term

    wait_all(send_c)
    hydro = cs[13]
    for code in others:
        hydro = hydro + jnp.where(ok[code], cr[code], 0.0)
    rec[6:8, :] = jnp.zeros((2, 128), jnp.float32)
    for n in range(3):
        speed_old = nb[13, 3 + n : 4 + n, :]
        pulled = hydro[n : n + 1, :] - (SPEED_UNIT * speed_old) * hydro[3:4, :]
        speed_new = speed_old + FORCE_SCALE * pulled + force[n]
        if n == 2:
            speed_new = speed_new - GRAVITY_STEP
        rec[3 + n : 4 + n, :] = speed_new
        rec[n : n + 1, :] = nb[13, n : n + 1, :] + speed_new * (SPEED_UNIT / R)

    record = rec[...]
    for n, code in enumerate(MOVE_CODES):
        shift = zero
        for axis, step in enumerate(offset_of(code)):
            if step != 0:
                shift = jnp.where(sub == axis, step * SPANS[axis], shift)
        source = inv2_v[n]
        picked = lane_gather(record - shift, source & 127)
        ds[n] = jnp.where(source >= 0, picked, 0.0)
    def send_d(n):
        return pltpu.make_async_remote_copy(
            src_ref=ds.at[n],
            dst_ref=dr.at[6 - n],
            send_sem=d_send.at[n],
            recv_sem=d_recv.at[6 - n],
            device_id=device(offset_of(MOVE_CODES[n])),
            device_id_type=MESH,
        )

    movers = [n for n in range(7) if MOVE_CODES[n] != 13]
    for n in movers:
        pl.when(ok[MOVE_CODES[n]])(lambda n=n: send_d(n).start())

    for n in movers:

        @pl.when(ok[MOVE_CODES[n]])
        def _(n=n):
            send_d(6 - n).wait_recv()
            send_d(n).wait_send()

    arrived = ds[3]
    for n in movers:
        arrived = arrived + jnp.where(ok[MOVE_CODES[n]], dr[n], 0.0)
    out_part[0, 0, :, 0, :] = arrived[0:6, :]

    for n in range(len(moves)):
        there = moves[n][2]

        @pl.when(ok[26 - code_of(there)])
        def _(n=n):
            send_b(n).wait_recv()

        @pl.when(ok[code_of(there)])
        def _(n=n):
            send_b(n).wait_send()

    for side in range(2):
        x = -1 if side == 0 else CX
        for n, d in enumerate((X_UP, X_DOWN)[side]):
            rel[PLACE[d], pl.ds(STRIDE * (x + 1) + PAD, CY), :] = xr[side, n]
    for side in range(2):
        y = -1 if side == 0 else CY
        for n, d in enumerate(Y_MOVERS[side]):
            tile = yr[side, n]
            if n == 1:
                tile = jnp.where(sub == 0, ye[side, 0], tile)
            if n == 2:
                tile = jnp.where(sub == CX - 1, ye[side, 1], tile)
            start = STRIDE * (1 - LATTICE[d][0]) + PAD + y
            rel[PLACE[d], pl.ds(start, CX, stride=STRIDE), :] = tile
    columns = []
    for side in range(2):
        tile = zr[side]
        tile = jnp.where((sub == 1) & (lane < CY), ze[side, 0], tile)
        tile = jnp.where((sub == 2) & (lane >= 128 - CY), ze[side, 1], tile)
        tile = jnp.where((sub == 3) & ((lane & 15) == 0), ze[side, 2], tile)
        tile = jnp.where((sub == 4) & ((lane & 15) == 15), ze[side, 3], tile)
        columns.append(tile)
    col_out[...] = jnp.transpose(
        jnp.concatenate(columns + [jnp.zeros((112, 128), jnp.float32)], axis=0)
    )


def stream_kernel(sizes, rel, columns, records, out_pop, out_part, out_v, out_sem, part_sem):
    here = [lax.axis_index(axis) for axis in AXES]
    keep_records = pltpu.make_async_copy(records, out_part, part_sem.at[0])
    keep_records.start()
    lane = lax.broadcasted_iota(jnp.int32, (8, 128), 1)
    sub = lax.broadcasted_iota(jnp.int32, (8, 128), 0)
    low_wall = [here[n] == 0 for n in range(3)]
    high_wall = [here[n] == sizes[n] - 1 for n in range(3)]
    order = sorted(range(19), key=lambda d: LATTICE[d][2] != 0)

    def put(d):
        return pltpu.make_async_copy(out_v.at[d], out_pop.at[d], out_sem.at[d])

    for d in order:
        vector = LATTICE[d]
        for x in range(CX):
            for half in range(2):
                cells = pl.ds(CY * x + 8 * half, 8)
                walls = {
                    (0, 1): low_wall[0] if x == 0 else None,
                    (0, -1): high_wall[0] if x == CX - 1 else None,
                    (1, 1): low_wall[1] & (sub == 0) if half == 0 else None,
                    (1, -1): high_wall[1] & (sub == 7) if half == 1 else None,
                    (2, 1): low_wall[2] & (lane == 0),
                    (2, -1): high_wall[2] & (lane == 127),
                }
                start = STRIDE * (x + 1 - vector[0]) + PAD + 8 * half - vector[1]
                value = rel[PLACE[d], pl.ds(start, 8), :]
                if vector[2] != 0:
                    side = 0 if vector[2] == 1 else 1
                    column = 8 * side + Z_MOVERS[side].index(d)
                    value = jnp.where(
                        lane == (0 if side == 0 else 127),
                        columns[cells, column : column + 1],
                        pltpu.roll(value, vector[2] % 128, 1),
                    )
                blocked = None
                for axis in range(3):
                    wall = walls.get((axis, vector[axis]))
                    if wall is not None:
                        blocked = wall if blocked is None else blocked | wall
                if blocked is not None:
                    back = rel[PLACE[OPPOSITE[d]], pl.ds(STRIDE * (x + 1) + PAD + 8 * half, 8), :]
                    value = jnp.where(blocked, back, value)
                out_v[d, cells, :] = value
        put(d).start()
    for d in order:
        put(d).wait()
    keep_records.wait()


def body(sizes, pop, frac, inter, touch, part, cont, dcode, dslot):
    f32, i32 = jnp.float32, jnp.int32
    cells = CX * CY
    part, cont = (jnp.transpose(a, (0, 1, 3, 2, 4)) for a in (part, cont))
    args = (
        pop.reshape(19, cells, CZ),
        frac.reshape(cells, CZ),
        inter.reshape(cells, CZ),
        touch,
        part,
        cont,
        dcode,
        dslot,
    )
    vmem = pltpu.VMEM
    sems = pltpu.SemaphoreType.DMA
    in_vmem = pl.BlockSpec(memory_space=vmem)
    in_any = pl.BlockSpec(memory_space=pl.ANY)
    relaxed, columns, records = pl.pallas_call(
        lambda *refs: kernel(sizes, *refs),
        out_shape=(
            vmem((19, STRIDE * (CX + 2), CZ), f32),
            vmem((cells, 128), f32),
            vmem((1, 1, 6, 1, SLOTS), f32),
        ),
        in_specs=[in_any] * 8,
        out_specs=(in_vmem,) * 3,
        scratch_shapes=[
            vmem((19, cells, CZ), f32),
            vmem((cells, CZ), f32),
            vmem((cells, CZ), i32),
            vmem((1, TOUCHES), i32),
            vmem((CANDIDATES, SLOTS), i32),
            vmem((1, SLOTS), i32),
            vmem((1, SLOTS), i32),
            vmem((27, 8, 128), f32),
            vmem((6, cells, CZ), f32),
            vmem((8 * cells, CZ), f32),
            vmem((14, 8, 128), i32),
            vmem((8, 8, 128), i32),
            vmem((28, 4, 128), f32),
            vmem((27, 4, 128), f32),
            vmem((16, 128), f32),
            vmem((2, 5, CY, CZ), f32),
            vmem((2, 5, CY, CZ), f32),
            vmem((2, 5, CX, CZ), f32),
            vmem((2, 5, CX, CZ), f32),
            vmem((2, 2, CX, CZ), f32),
            vmem((cells, 128), f32),
            vmem((2, 8, 128), f32),
            vmem((2, 8, 128), f32),
            vmem((2, 4, 8, 128), f32),
            vmem((8, 128), f32),
            vmem((7, 8, 128), f32),
            vmem((7, 8, 128), f32),
            sems((7,)),
            sems((CX,)),
            sems((27,)),
            sems((27,)),
            sems((18,)),
            sems((18,)),
            sems((27,)),
            sems((27,)),
            sems((7,)),
            sems((7,)),
        ],
        compiler_params=pltpu.CompilerParams(collective_id=0, has_side_effects=True),
    )(*args)
    populations, records = pl.pallas_call(
        lambda *refs: stream_kernel(sizes, *refs),
        out_shape=(
            jax.ShapeDtypeStruct((19, cells, CZ), f32),
            jax.ShapeDtypeStruct((1, 1, 6, 1, SLOTS), f32),
        ),
        in_specs=[in_vmem] * 3,
        out_specs=(in_any,) * 2,
        scratch_shapes=[vmem((19, cells, CZ), f32), sems((19,)), sems((1,))],
    )(*(pltpu.with_memory_space_constraint(a, vmem) for a in (relaxed, columns, records)))
    return populations.reshape(19, CX, CY, CZ), jnp.transpose(records, (0, 1, 3, 2, 4))


def solution(mesh):
    sizes = tuple(mesh.shape[axis] for axis in AXES)
    cells, blocks = P(*AXES), P(*AXES, None)
    records = P(*AXES, None, None)
    fields = P(None, *AXES)
    return jax.shard_map(
        lambda *args: body(sizes, *args),
        mesh=mesh,
        in_specs=(fields, cells, cells, blocks, records, records, blocks, blocks),
        out_specs=(fields, records),
        check_vma=False,
    )
```

```python
import jax
import jax.numpy as jnp
from jax import lax
from jax.experimental import pallas as pl
from jax.experimental.pallas import tpu as pltpu
from jax.sharding import PartitionSpec as P

LATTICE = [
    (0, 0, 0),
    (1, 0, 0),
    (-1, 0, 0),
    (0, 1, 0),
    (0, -1, 0),
    (0, 0, 1),
    (0, 0, -1),
    (1, 1, 0),
    (-1, -1, 0),
    (1, -1, 0),
    (-1, 1, 0),
    (1, 0, 1),
    (-1, 0, -1),
    (1, 0, -1),
    (-1, 0, 1),
    (0, 1, 1),
    (0, -1, -1),
    (0, 1, -1),
    (0, -1, 1),
]
OPPOSITE = [0, 2, 1, 4, 3, 6, 5, 8, 7, 10, 9, 12, 11, 14, 13, 16, 15, 18, 17]
WEIGHTS = [1.0 / 3.0] + [1.0 / 18.0] * 6 + [1.0 / 36.0] * 12
PAIRS = [(i, i + 1) for i in range(1, 19, 2)]
RELAX_TIME = 0.8
SPEED_UNIT = 0.05
FORCE_SCALE = 0.1
CONTACT_GAIN = 1.0
GRAVITY_STEP = 0.1
R = 8.0
CX, CY, CZ, SLOTS, TOUCHES, CANDIDATES = 8, 16, 128, 128, 256, 12
SPANS = (CX / R, CY / R, CZ / R)
AXES = ("gx", "gy", "gz")
MESH = pl.DeviceIdType.MESH

X_UP, X_DOWN = [1, 7, 9, 11, 13], [2, 8, 10, 12, 14]
Y_MOVERS = [[3, 7, 10, 15, 17], [4, 9, 8, 18, 16]]
Z_MOVERS = [[5, 11, 14, 15, 18], [6, 13, 12, 17, 16]]
PLACE = {d: n for n, d in enumerate(X_UP + X_DOWN + [0, 3, 4, 5, 6, 15, 16, 17, 18])}
MOVE_CODES = [4, 10, 12, 13, 14, 16, 22]
PAD = 8
STRIDE = CY + 2 * PAD


def offset_of(code):
    return (code // 9 - 1, code // 3 % 3 - 1, code % 3 - 1)


def projected(velocity, d):
    along = None
    for n in range(3):
        if LATTICE[d][n] == 1:
            along = velocity[n] if along is None else along + velocity[n]
        elif LATTICE[d][n] == -1:
            along = -velocity[n] if along is None else along - velocity[n]
    return along


def lane_gather(table, index):
    return jnp.take_along_axis(table, index, axis=1, mode="promise_in_bounds")


def dot_lanes(a, b):
    return lax.dot_general(a, b, (((1,), (1,)), ((), ())), preferred_element_type=jnp.float32)


def kernel(
    sizes,
    pop,
    frac,
    inter,
    touch,
    part,
    cont,
    dcode,
    dslot,
    rel_out,
    col_out,
    out_part,
    f_v,
    frac_v,
    int_v,
    touch_v,
    cont_v,
    dcode_v,
    dslot_v,
    nb,
    mac,
    split,
    inv_v,
    inv2_v,
    cs,
    cr,
    zc,
    xs,
    xr,
    ys,
    yr,
    ye,
    zm,
    zs,
    zr,
    ze,
    rec,
    ds,
    dr,
    in_sem,
    a_send,
    a_recv,
    b_send,
    b_recv,
    c_send,
    c_recv,
    d_send,
    d_recv,
):
    rel = rel_out
    here = [lax.axis_index(axis) for axis in AXES]

    def device(offset):
        return tuple(
            here[n] if offset[n] == 0 else lax.rem(here[n] + offset[n] + sizes[n], sizes[n])
            for n in range(3)
        )

    def exists(offset):
        ok = None
        for n in range(3):
            if offset[n] != 0:
                test = here[n] > 0 if offset[n] < 0 else here[n] < sizes[n] - 1
                ok = test if ok is None else ok & test
        return ok

    others = [code for code in range(27) if code != 13]
    others.sort(key=lambda code: -sum(abs(step) for step in offset_of(code)))
    ok = {code: exists(offset_of(code)) for code in others}
    def start_all(make):
        for code in others:
            pl.when(ok[code])(lambda code=code: make(code).start())

    count = [
        (here[n] > 0).astype(jnp.int32) + (here[n] < sizes[n] - 1).astype(jnp.int32)
        for n in range(3)
    ]

    neighbours = (count[0] + 1) * (count[1] + 1) * (count[2] + 1) - 1

    def wait_rows(sem, rows):
        pltpu.make_async_copy(split.at[pl.ds(0, rows)], split.at[pl.ds(0, rows)], sem).wait()

    def wait_all(sem, rows):
        for n in sorted({a * b * c - 1 for a in (2, 3) for b in (2, 3) for c in (2, 3)}):
            pl.when(neighbours == n)(lambda n=n: wait_rows(sem, rows * n))

    def wait_sides(sem, rows_of):
        for a in (1, 2):
            for b in (1, 2):
                for c in (1, 2):
                    here_now = (count[0] == a) & (count[1] == b) & (count[2] == c)
                    pl.when(here_now)(lambda a=a, b=b, c=c: wait_rows(sem, rows_of(a, b, c)))

    barrier = pltpu.get_barrier_semaphore()
    for code in others:

        @pl.when(ok[code])
        def _(code=code):
            pl.semaphore_signal(
                barrier, inc=1, device_id=device(offset_of(code)), device_id_type=MESH
            )

    own_load = pltpu.make_async_copy(part.at[0, 0, :, 0], nb.at[13, pl.ds(0, 6)], in_sem.at[0])
    own_load.start()
    for source, target in (
        (touch.at[0, 0], touch_v),
        (dcode.at[0, 0], dcode_v),
        (dslot.at[0, 0], dslot_v),
        (cont.at[0, 0, :, 0], cont_v),
    ):
        pltpu.make_async_copy(source, target, in_sem.at[1]).start()
    for source, target in ((frac, frac_v), (inter, int_v)):
        pltpu.make_async_copy(source, target, in_sem.at[2]).start()

    def pop_load(x):
        return pltpu.make_async_copy(
            pop.at[:, pl.ds(64 * x, 64)], f_v.at[:, pl.ds(64 * x, 64)], in_sem.at[3 + x]
        )

    for x in range(2):
        pop_load(x).start()

    lane = lax.broadcasted_iota(jnp.int32, (8, 128), 1)
    sub = lax.broadcasted_iota(jnp.int32, (8, 128), 0)

    def send_a(code):
        return pltpu.make_async_remote_copy(
            src_ref=nb.at[13],
            dst_ref=nb.at[26 - code],
            send_sem=a_send,
            recv_sem=a_recv,
            device_id=device(offset_of(code)),
            device_id_type=MESH,
        )

    def send_c(code):
        return pltpu.make_async_remote_copy(
            src_ref=cs.at[code],
            dst_ref=cr.at[26 - code],
            send_sem=c_send,
            recv_sem=c_recv,
            device_id=device(offset_of(code)),
            device_id_type=MESH,
        )

    def partial_sums():
        wait_rows(in_sem.at[1], 4 + CANDIDATES)
        entry = touch_v[0:1, :]
        wide = lax.broadcasted_iota(jnp.int32, (112, TOUCHES), 1)
        row = lax.broadcasted_iota(jnp.int32, (112, TOUCHES), 0)
        named = jnp.where((entry >> 7) == (row >> 2), wide + 1, 0).astype(jnp.float32)
        slot_row = lax.broadcasted_iota(jnp.int32, (SLOTS, TOUCHES), 0)
        placed = jnp.where((entry & 127) == slot_row, 1.0, 0.0)
        inverse = dot_lanes(named.astype(jnp.bfloat16), placed.astype(jnp.bfloat16))
        inv_v[...] = (inverse.astype(jnp.int32) - 1).reshape(14, 8, 128)
        code_row = jnp.broadcast_to(dcode_v[0:1, :], (8, 128))
        moved = jnp.concatenate(
            [jnp.where(code_row == code, lane + 1, 0).astype(jnp.float32) for code in MOVE_CODES]
            + [jnp.zeros((8, 128), jnp.float32)],
            axis=0,
        )
        tall = lax.broadcasted_iota(jnp.int32, (SLOTS, SLOTS), 0)
        landing = jnp.where(dslot_v[0:1, :] == tall, 1.0, 0.0)
        inverse2 = dot_lanes(moved.astype(jnp.bfloat16), landing.astype(jnp.bfloat16))
        inv2_v[...] = (inverse2.astype(jnp.int32) - 1).reshape(8, 8, 128)

        wait_rows(in_sem.at[2], 2 * CX * CY)

        def moments(x, carry):
            for half in range(2):
                start = pl.multiple_of(CY * x + 8 * half, 8)
                rows = pl.ds(start, 8)
                f = [f_v[d, rows, :] for d in range(19)]
                rho = f[0]
                momentum = [None, None, None]
                for d in range(1, 19):
                    rho = rho + f[d]
                for n in range(3):
                    for d in range(1, 19):
                        if LATTICE[d][n] == 1:
                            momentum[n] = f[d] if momentum[n] is None else momentum[n] + f[d]
                    for d in range(1, 19):
                        if LATTICE[d][n] == -1:
                            momentum[n] = momentum[n] - f[d]
                eps = frac_v[rows, :]
                weight = jnp.where(
                    int_v[rows, :] < TOUCHES,
                    eps * (RELAX_TIME - 0.5) / (1.0 - eps + (RELAX_TIME - 0.5)),
                    0.0,
                )
                scale = 1.0 / rho
                mac[0, rows, :] = rho
                mac[1, rows, :] = weight
                for n in range(3):
                    mac[2 + n, rows, :] = momentum[n] * scale
                for n, term in enumerate(momentum + [rho]):
                    term = term * weight
                    if n == 3:
                        mac[5, rows, :] = term
                    high = term.astype(jnp.bfloat16).astype(jnp.float32)
                    split[pl.ds(8 * start + n, 8, stride=8), :] = high
                    split[pl.ds(8 * start + 4 + n, 8, stride=8), :] = term - high
            return carry

        for part_x in range(2):
            pop_load(part_x).wait()
            lax.fori_loop(4 * part_x, 4 * part_x + 4, moments, 0, unroll=2)

        low_row = lax.broadcasted_iota(jnp.int32, (32, 128), 0)

        def add_slab(x, total):
            left, right = [], []
            for y in range(CY):
                slots = int_v[pl.ds(CY * x + y, 1), :]
                tile = split[pl.ds(pl.multiple_of(8 * (CY * x + y), 8), 8), :]
                upper = jnp.broadcast_to(slots >> 5, (8, 128))
                picked = [jnp.where(upper == a, tile, 0.0) for a in range(8)]
                left.append(jnp.concatenate(picked, axis=0).astype(jnp.bfloat16))
                lower = jnp.broadcast_to(slots & 31, (32, 128))
                right.append(jnp.where(lower == low_row, 1.0, 0.0).astype(jnp.bfloat16))
            return total + dot_lanes(
                jnp.concatenate(left, axis=1), jnp.concatenate(right, axis=1)
            )

        total = lax.fori_loop(0, CX, add_slab, jnp.zeros((64, 32), jnp.float32), unroll=4)
        tables = []
        for h in range(2):
            table = jnp.concatenate(
                [total[8 * a : 8 * a + 8, :] for a in range(4 * h, 4 * h + 4)], axis=1
            )
            tables.append(table + pltpu.roll(table, 4, 0))

        for q in range(14):
            source = inv_v[q]
            index = source & 127
            picked = jnp.where(
                source < 128, lane_gather(tables[0], index), lane_gather(tables[1], index)
            )
            picked = jnp.where(source >= 0, picked, 0.0)
            cs[2 * q] = picked[0:4, :]
            cs[2 * q + 1] = picked[4:8, :]


    early = (here[2] == 1) | (here[1] == 4) | ((here[0] < 3) & (lax.rem(here[1], 4) < 3))
    pl.when(early)(partial_sums)

    own_load.wait()
    pl.semaphore_wait(barrier, neighbours)
    start_all(send_a)
    pl.when(jnp.logical_not(early))(partial_sums)

    start_all(send_c)

    def cell_rows(x, half):
        cells = pl.ds(pl.multiple_of(CY * x + 8 * half, 8), 8)
        return cells, pl.ds(pl.multiple_of(STRIDE * (x + 1) + PAD + 8 * half, 8), 8)

    def relax(x, carry):
        for half in range(2):
            rows, dest = cell_rows(x, half)
            rho = mac[0, rows, :]
            weight = mac[1, rows, :]
            u = [mac[2 + n, rows, :] for n in range(3)]
            alpha = (1.0 - weight) * (1.0 / RELAX_TIME)
            keep = 1.0 - alpha - weight
            even = (alpha - weight) * rho
            odd = 3.0 * (alpha + weight) * rho
            base = even * (1.0 - 1.5 * (u[0] * u[0] + u[1] * u[1] + u[2] * u[2]))
            even = 4.5 * even
            rel[PLACE[0], dest, :] = (1.0 - alpha) * f_v[0, rows, :] + WEIGHTS[0] * base
            for i, j in PAIRS:
                along = projected(u, i)
                symmetric = WEIGHTS[i] * (base + even * along * along)
                skew = WEIGHTS[i] * (odd * along)
                fi, fj = f_v[i, rows, :], f_v[j, rows, :]
                rel[PLACE[i], dest, :] = keep * fi + weight * fj + (symmetric + skew)
                rel[PLACE[j], dest, :] = keep * fj + weight * fi + (symmetric - skew)
        return carry

    lax.fori_loop(0, CX, relax, 0, unroll=2)

    def pack_ends(x, carry):
        for half in range(2):
            rows, dest = cell_rows(x, half)
            packed = jnp.zeros((8, 128), jnp.float32)
            for side in range(2):
                edge = 127 if side == 0 else 0
                values = [rel[PLACE[d], dest, :] for d in Z_MOVERS[side]]
                values += [mac[5, rows, :], int_v[rows, :].astype(jnp.float32)]
                for n, value in enumerate(values):
                    packed = jnp.where(lane == 8 * side + n, value[:, edge : edge + 1], packed)
            zm[rows, :] = packed
        return carry

    lax.fori_loop(0, CX, pack_ends, 0, unroll=CX)
    zc[...] = jnp.transpose(zm[...])[0:16, :]

    wait_all(a_recv, 8)

    for code in others:
        nb[code] = jnp.where(ok[code], nb[code], 0.0)

    touch_code = [jnp.broadcast_to(touch_v[0:1, pl.ds(128 * h, 128)] >> 7, (8, 128)) for h in range(2)]
    touch_slot = [jnp.broadcast_to(touch_v[0:1, pl.ds(128 * h, 128)] & 127, (8, 128)) for h in range(2)]

    def find_velocity(code, found):
        tile = nb[code]
        return tuple(
            jnp.where(touch_code[h] == code, lane_gather(tile, touch_slot[h]), found[h])
            for h in range(2)
        )

    zero = jnp.zeros((8, 128), jnp.float32)
    found = lax.fori_loop(0, 27, find_velocity, (zero, zero), unroll=27)
    speed = [
        [jnp.broadcast_to(SPEED_UNIT * found[h][3 + n : 4 + n, :], (8, 128)) for n in range(3)]
        for h in range(2)
    ]

    def solid_part(slots, mass):
        index = slots & 127
        first = slots < 128
        v = [
            jnp.where(first, lane_gather(speed[0][n], index), lane_gather(speed[1][n], index))
            for n in range(3)
        ]
        base = mass * (1.0 - 1.5 * (v[0] * v[0] + v[1] * v[1] + v[2] * v[2]))
        return v, base, 4.5 * mass, 3.0 * mass

    def solid_term(parts, d):
        v, base, even, odd = parts
        along = projected(v, d)
        return WEIGHTS[d] * (base + along * (even * along + odd))

    for side in range(2):
        x = CX - 1 if side == 0 else 0
        for half in range(2):
            rows, dest = cell_rows(x, half)
            parts = solid_part(int_v[rows, :], mac[5, rows, :])
            for n, d in enumerate((X_UP, X_DOWN)[side]):
                value = rel[PLACE[d], dest, :] + solid_term(parts, d)
                xs[side, n, pl.ds(8 * half, 8), :] = value
    for side in range(2):
        y = CY - 1 if side == 0 else 0
        rows = pl.ds(y, CX, stride=CY)
        dest = pl.ds(STRIDE + PAD + y, CX, stride=STRIDE)
        parts = solid_part(int_v[rows, :], mac[5, rows, :])
        for n, d in enumerate(Y_MOVERS[side]):
            value = rel[PLACE[d], dest, :] + solid_term(parts, d)
            if LATTICE[d][0] != 0:
                value = pltpu.roll(value, LATTICE[d][0] % CX, 0)
            ys[side, n] = value
    for side in range(2):
        slots = jnp.broadcast_to(zc[8 * side + 6 : 8 * side + 7, :].astype(jnp.int32), (8, 128))
        mass = jnp.broadcast_to(zc[8 * side + 5 : 8 * side + 6, :], (8, 128))
        v, base, even, odd = solid_part(slots, mass)
        along = zero
        share = jnp.full((8, 128), 1.0 / 36.0, jnp.float32)
        for n, d in enumerate(Z_MOVERS[side]):
            along = jnp.where(sub == n, projected(v, d), along)
        share = jnp.where(sub == 0, 1.0 / 18.0, share)
        tile = zc[8 * side : 8 * side + 8, :] + share * (base + along * (even * along + odd))
        up_y = jnp.where((lane & 15) == 0, pltpu.roll(tile, 128 - 15, 1), pltpu.roll(tile, 1, 1))
        down_y = jnp.where((lane & 15) == 15, pltpu.roll(tile, 15, 1), pltpu.roll(tile, 127, 1))
        moved_z = jnp.where(sub == 1, pltpu.roll(tile, 16, 1), tile)
        moved_z = jnp.where(sub == 2, pltpu.roll(tile, 112, 1), moved_z)
        moved_z = jnp.where(sub == 3, up_y, moved_z)
        zs[side] = jnp.where(sub == 4, down_y, moved_z)

    moves = []
    for side in range(2):
        step = 1 - 2 * side
        moves.append((xs.at[side], xr.at[side], (step, 0, 0)))
        moves.append((ys.at[side], yr.at[side], (0, step, 0)))
        moves.append((ys.at[side, 1], ye.at[side, 0], (1, step, 0)))
        moves.append((ys.at[side, 2], ye.at[side, 1], (-1, step, 0)))
        moves.append((zs.at[side], zr.at[side], (0, 0, step)))
        moves.append((zs.at[side], ze.at[side, 0], (1, 0, step)))
        moves.append((zs.at[side], ze.at[side, 1], (-1, 0, step)))
        moves.append((zs.at[side], ze.at[side, 2], (0, 1, step)))
        moves.append((zs.at[side], ze.at[side, 3], (0, -1, step)))
    def send_b(n):
        source, target, offset = moves[n]
        return pltpu.make_async_remote_copy(
            src_ref=source,
            dst_ref=target,
            send_sem=b_send,
            recv_sem=b_recv,
            device_id=device(offset),
            device_id_type=MESH,
        )

    def code_of(offset):
        return 9 * (offset[0] + 1) + 3 * (offset[1] + 1) + offset[2] + 1

    for n in range(len(moves)):
        pl.when(ok[code_of(moves[n][2])])(lambda n=n: send_b(n).start())

    listed = [
        cont_v[0:8, :],
        jnp.concatenate([cont_v[8:12, :], jnp.full((4, 128), 27 * SLOTS, jnp.int32)], axis=0),
    ]
    listed_code = [entries >> 7 for entries in listed]
    listed_slot = [entries & 127 for entries in listed]

    def find_partner(code, partner):
        shifts = (code // 9 - 1, code // 3 % 3 - 1, code % 3 - 1)
        result = []
        for n in range(3):
            line = nb[code, pl.ds(n, 1), :] + shifts[n].astype(jnp.float32) * SPANS[n]
            line = jnp.broadcast_to(line, (8, 128))
            for h in range(2):
                result.append(
                    jnp.where(
                        listed_code[h] == code,
                        lane_gather(line, listed_slot[h]),
                        partner[2 * n + h],
                    )
                )
        return tuple(result)

    partner = lax.fori_loop(0, 27, find_partner, (zero,) * 6, unroll=27)
    force = [None, None, None]
    for h in range(2):
        apart = [nb[13, n : n + 1, :] - partner[2 * n + h] for n in range(3)]
        square = apart[0] * apart[0] + apart[1] * apart[1] + apart[2] * apart[2]
        soften = 1.0 + 0.25 * square
        strength = jnp.where(listed_code[h] < 27, CONTACT_GAIN / (soften * soften), 0.0)
        for n in range(3):
            term = jnp.sum(apart[n] * strength, axis=0, keepdims=True)
            force[n] = term if h == 0 else force[n] + term

    wait_all(c_recv, 4)
    hydro = cs[13]
    for code in others:
        hydro = hydro + jnp.where(ok[code], cr[code], 0.0)
    rec[6:8, :] = jnp.zeros((2, 128), jnp.float32)
    for n in range(3):
        speed_old = nb[13, 3 + n : 4 + n, :]
        pulled = hydro[n : n + 1, :] - (SPEED_UNIT * speed_old) * hydro[3:4, :]
        speed_new = speed_old + FORCE_SCALE * pulled + force[n]
        if n == 2:
            speed_new = speed_new - GRAVITY_STEP
        rec[3 + n : 4 + n, :] = speed_new
        rec[n : n + 1, :] = nb[13, n : n + 1, :] + speed_new * (SPEED_UNIT / R)

    record = rec[...]
    for n, code in enumerate(MOVE_CODES):
        shift = zero
        for axis, step in enumerate(offset_of(code)):
            if step != 0:
                shift = jnp.where(sub == axis, step * SPANS[axis], shift)
        source = inv2_v[n]
        picked = lane_gather(record - shift, source & 127)
        ds[n] = jnp.where(source >= 0, picked, 0.0)
    def send_d(n):
        return pltpu.make_async_remote_copy(
            src_ref=ds.at[n],
            dst_ref=dr.at[6 - n],
            send_sem=d_send,
            recv_sem=d_recv,
            device_id=device(offset_of(MOVE_CODES[n])),
            device_id_type=MESH,
        )

    movers = [n for n in range(7) if MOVE_CODES[n] != 13]
    for n in movers:
        pl.when(ok[MOVE_CODES[n]])(lambda n=n: send_d(n).start())

    def solid(x, carry):
        for half in range(2):
            rows, dest = cell_rows(x, half)
            v, base, even, odd = solid_part(int_v[rows, :], mac[5, rows, :])
            rel[PLACE[0], dest, :] = rel[PLACE[0], dest, :] + WEIGHTS[0] * base
            for i, j in PAIRS:
                along = projected(v, i)
                symmetric = WEIGHTS[i] * (base + even * along * along)
                skew = WEIGHTS[i] * (odd * along)
                rel[PLACE[i], dest, :] = rel[PLACE[i], dest, :] + (symmetric + skew)
                rel[PLACE[j], dest, :] = rel[PLACE[j], dest, :] + (symmetric - skew)
        return carry

    lax.fori_loop(0, CX, solid, 0, unroll=CX)

    def side_rows(a, b, c):
        return 8 * (10 * a + 5 * b + c + a * b + a * c + b * c)

    wait_sides(b_recv, side_rows)
    wait_sides(d_recv, lambda a, b, c: 8 * (a + b + c))
    arrived = ds[3]
    for n in movers:
        arrived = arrived + jnp.where(ok[MOVE_CODES[n]], dr[n], 0.0)
    out_part[0, 0, :, 0, :] = arrived[0:6, :]

    wait_all(a_send, 8)
    wait_all(c_send, 4)
    wait_sides(b_send, side_rows)
    wait_sides(d_send, lambda a, b, c: 8 * (a + b + c))

    for side in range(2):
        x = -1 if side == 0 else CX
        for n, d in enumerate((X_UP, X_DOWN)[side]):
            rel[PLACE[d], pl.ds(STRIDE * (x + 1) + PAD, CY), :] = xr[side, n]
    for side in range(2):
        y = -1 if side == 0 else CY
        for n, d in enumerate(Y_MOVERS[side]):
            tile = yr[side, n]
            if n == 1:
                tile = jnp.where(sub == 0, ye[side, 0], tile)
            if n == 2:
                tile = jnp.where(sub == CX - 1, ye[side, 1], tile)
            start = STRIDE * (1 - LATTICE[d][0]) + PAD + y
            rel[PLACE[d], pl.ds(start, CX, stride=STRIDE), :] = tile
    columns = []
    for side in range(2):
        tile = zr[side]
        tile = jnp.where((sub == 1) & (lane < CY), ze[side, 0], tile)
        tile = jnp.where((sub == 2) & (lane >= 128 - CY), ze[side, 1], tile)
        tile = jnp.where((sub == 3) & ((lane & 15) == 0), ze[side, 2], tile)
        tile = jnp.where((sub == 4) & ((lane & 15) == 15), ze[side, 3], tile)
        columns.append(tile)
    col_out[...] = jnp.transpose(
        jnp.concatenate(columns + [jnp.zeros((112, 128), jnp.float32)], axis=0)
    )


def stream_kernel(sizes, rel, columns, records, out_pop, out_part, out_v, out_sem, part_sem):
    here = [lax.axis_index(axis) for axis in AXES]
    keep_records = pltpu.make_async_copy(records, out_part, part_sem)
    keep_records.start()
    lane = lax.broadcasted_iota(jnp.int32, (8, 128), 1)
    sub = lax.broadcasted_iota(jnp.int32, (8, 128), 0)
    low_wall = [here[n] == 0 for n in range(3)]
    high_wall = [here[n] == sizes[n] - 1 for n in range(3)]
    order = sorted(range(19), key=lambda d: LATTICE[d][2] != 0)

    def put(d):
        return pltpu.make_async_copy(out_v.at[d], out_pop.at[d], out_sem)

    for d in order:
        vector = LATTICE[d]
        for x in range(CX):
            for half in range(2):
                cells = pl.ds(CY * x + 8 * half, 8)
                walls = {
                    (0, 1): low_wall[0] if x == 0 else None,
                    (0, -1): high_wall[0] if x == CX - 1 else None,
                    (1, 1): low_wall[1] & (sub == 0) if half == 0 else None,
                    (1, -1): high_wall[1] & (sub == 7) if half == 1 else None,
                    (2, 1): low_wall[2] & (lane == 0),
                    (2, -1): high_wall[2] & (lane == 127),
                }
                start = STRIDE * (x + 1 - vector[0]) + PAD + 8 * half - vector[1]
                value = rel[PLACE[d], pl.ds(start, 8), :]
                if vector[2] != 0:
                    side = 0 if vector[2] == 1 else 1
                    column = 8 * side + Z_MOVERS[side].index(d)
                    value = jnp.where(
                        lane == (0 if side == 0 else 127),
                        columns[cells, column : column + 1],
                        pltpu.roll(value, vector[2] % 128, 1),
                    )
                blocked = None
                for axis in range(3):
                    wall = walls.get((axis, vector[axis]))
                    if wall is not None:
                        blocked = wall if blocked is None else blocked | wall
                if blocked is not None:
                    back = rel[PLACE[OPPOSITE[d]], pl.ds(STRIDE * (x + 1) + PAD + 8 * half, 8), :]
                    value = jnp.where(blocked, back, value)
                out_v[d, cells, :] = value
        put(d).start()
    pltpu.make_async_copy(out_v, out_pop, out_sem).wait()
    keep_records.wait()


def body(sizes, pop, frac, inter, touch, part, cont, dcode, dslot):
    f32, i32 = jnp.float32, jnp.int32
    cells = CX * CY
    part, cont = (jnp.transpose(a, (0, 1, 3, 2, 4)) for a in (part, cont))
    args = (
        pop.reshape(19, cells, CZ),
        frac.reshape(cells, CZ),
        inter.reshape(cells, CZ),
        touch,
        part,
        cont,
        dcode,
        dslot,
    )
    vmem = pltpu.VMEM
    sems = pltpu.SemaphoreType.DMA
    in_vmem = pl.BlockSpec(memory_space=vmem)
    in_any = pl.BlockSpec(memory_space=pl.ANY)
    relaxed, columns, records = pl.pallas_call(
        lambda *refs: kernel(sizes, *refs),
        out_shape=(
            vmem((19, STRIDE * (CX + 2), CZ), f32),
            vmem((cells, 128), f32),
            vmem((1, 1, 6, 1, SLOTS), f32),
        ),
        in_specs=[in_any] * 8,
        out_specs=(in_vmem,) * 3,
        scratch_shapes=[
            vmem((19, cells, CZ), f32),
            vmem((cells, CZ), f32),
            vmem((cells, CZ), i32),
            vmem((1, TOUCHES), i32),
            vmem((CANDIDATES, SLOTS), i32),
            vmem((1, SLOTS), i32),
            vmem((1, SLOTS), i32),
            vmem((27, 8, 128), f32),
            vmem((6, cells, CZ), f32),
            vmem((8 * cells, CZ), f32),
            vmem((14, 8, 128), i32),
            vmem((8, 8, 128), i32),
            vmem((28, 4, 128), f32),
            vmem((27, 4, 128), f32),
            vmem((16, 128), f32),
            vmem((2, 5, CY, CZ), f32),
            vmem((2, 5, CY, CZ), f32),
            vmem((2, 5, CX, CZ), f32),
            vmem((2, 5, CX, CZ), f32),
            vmem((2, 2, CX, CZ), f32),
            vmem((cells, 128), f32),
            vmem((2, 8, 128), f32),
            vmem((2, 8, 128), f32),
            vmem((2, 4, 8, 128), f32),
            vmem((8, 128), f32),
            vmem((7, 8, 128), f32),
            vmem((7, 8, 128), f32),
            sems((5,)),
            sems,
            sems,
            sems,
            sems,
            sems,
            sems,
            sems,
            sems,
        ],
        compiler_params=pltpu.CompilerParams(collective_id=0, has_side_effects=True),
    )(*args)
    populations, records = pl.pallas_call(
        lambda *refs: stream_kernel(sizes, *refs),
        out_shape=(
            jax.ShapeDtypeStruct((19, cells, CZ), f32),
            jax.ShapeDtypeStruct((1, 1, 6, 1, SLOTS), f32),
        ),
        in_specs=[in_vmem] * 3,
        out_specs=(in_any,) * 2,
        scratch_shapes=[vmem((19, cells, CZ), f32), sems, sems],
    )(*(pltpu.with_memory_space_constraint(a, vmem) for a in (relaxed, columns, records)))
    return populations.reshape(19, CX, CY, CZ), jnp.transpose(records, (0, 1, 3, 2, 4))


def solution(mesh):
    sizes = tuple(mesh.shape[axis] for axis in AXES)
    cells, blocks = P(*AXES), P(*AXES, None)
    records = P(*AXES, None, None)
    fields = P(None, *AXES)
    return jax.shard_map(
        lambda *args: body(sizes, *args),
        mesh=mesh,
        in_specs=(fields, cells, cells, blocks, records, records, blocks, blocks),
        out_specs=(fields, records),
        check_vma=False,
    )
```

```python
import jax
import jax.numpy as jnp
from jax import lax
from jax.experimental import pallas as pl
from jax.experimental.pallas import tpu as pltpu
from jax.sharding import PartitionSpec as P

LATTICE = [
    (0, 0, 0),
    (1, 0, 0),
    (-1, 0, 0),
    (0, 1, 0),
    (0, -1, 0),
    (0, 0, 1),
    (0, 0, -1),
    (1, 1, 0),
    (-1, -1, 0),
    (1, -1, 0),
    (-1, 1, 0),
    (1, 0, 1),
    (-1, 0, -1),
    (1, 0, -1),
    (-1, 0, 1),
    (0, 1, 1),
    (0, -1, -1),
    (0, 1, -1),
    (0, -1, 1),
]
OPPOSITE = [0, 2, 1, 4, 3, 6, 5, 8, 7, 10, 9, 12, 11, 14, 13, 16, 15, 18, 17]
WEIGHTS = [1.0 / 3.0] + [1.0 / 18.0] * 6 + [1.0 / 36.0] * 12
PAIRS = [(i, i + 1) for i in range(1, 19, 2)]
RELAX_TIME = 0.8
SPEED_UNIT = 0.05
FORCE_SCALE = 0.1
CONTACT_GAIN = 1.0
GRAVITY_STEP = 0.1
R = 8.0
CX, CY, CZ, SLOTS, TOUCHES, CANDIDATES = 8, 16, 128, 128, 256, 12
SPANS = (CX / R, CY / R, CZ / R)
AXES = ("gx", "gy", "gz")
MESH = pl.DeviceIdType.MESH

X_UP, X_DOWN = [1, 7, 9, 11, 13], [2, 8, 10, 12, 14]
Y_MOVERS = [[3, 7, 10, 15, 17], [4, 9, 8, 18, 16]]
Z_MOVERS = [[5, 11, 14, 15, 18], [6, 13, 12, 17, 16]]
PLACE = {d: n for n, d in enumerate(X_UP + X_DOWN + [0, 3, 4, 5, 6, 15, 16, 17, 18])}
MOVE_CODES = [4, 10, 12, 13, 14, 16, 22]
PAD = 8
STRIDE = CY + 2 * PAD


def offset_of(code):
    return (code // 9 - 1, code // 3 % 3 - 1, code % 3 - 1)


def projected(velocity, d):
    along = None
    for n in range(3):
        if LATTICE[d][n] == 1:
            along = velocity[n] if along is None else along + velocity[n]
        elif LATTICE[d][n] == -1:
            along = -velocity[n] if along is None else along - velocity[n]
    return along


def lane_gather(table, index):
    return jnp.take_along_axis(table, index, axis=1, mode="promise_in_bounds")


def dot_lanes(a, b):
    return lax.dot_general(a, b, (((1,), (1,)), ((), ())), preferred_element_type=jnp.float32)


def kernel(
    sizes,
    pop,
    frac,
    inter,
    touch,
    part,
    cont,
    dcode,
    dslot,
    rel_out,
    col_out,
    out_part,
    f_v,
    frac_v,
    int_v,
    touch_v,
    cont_v,
    dcode_v,
    dslot_v,
    nb,
    mac,
    split,
    inv_v,
    inv2_v,
    cs,
    cr,
    zc,
    xs,
    xr,
    ys,
    yr,
    ye,
    zm,
    zs,
    zr,
    ze,
    rec,
    ds,
    dr,
    in_sem,
    a_recv,
    b_recv,
    c_recv,
    d_recv,
    sent,
):
    rel = rel_out
    here = [lax.axis_index(axis) for axis in AXES]

    def device(offset):
        return tuple(
            here[n] if offset[n] == 0 else lax.rem(here[n] + offset[n] + sizes[n], sizes[n])
            for n in range(3)
        )

    def exists(offset):
        ok = None
        for n in range(3):
            if offset[n] != 0:
                test = here[n] > 0 if offset[n] < 0 else here[n] < sizes[n] - 1
                ok = test if ok is None else ok & test
        return ok

    others = [code for code in range(27) if code != 13]
    others.sort(key=lambda code: -sum(abs(step) for step in offset_of(code)))
    ok = {code: exists(offset_of(code)) for code in others}
    def start_all(make):
        for code in others:
            pl.when(ok[code])(lambda code=code: make(code).start())

    count = [
        (here[n] > 0).astype(jnp.int32) + (here[n] < sizes[n] - 1).astype(jnp.int32)
        for n in range(3)
    ]

    neighbours = (count[0] + 1) * (count[1] + 1) * (count[2] + 1) - 1

    def wait_rows(sem, rows):
        pltpu.make_async_copy(split.at[pl.ds(0, rows)], split.at[pl.ds(0, rows)], sem).wait()

    def wait_all(sem, rows):
        for n in sorted({a * b * c - 1 for a in (2, 3) for b in (2, 3) for c in (2, 3)}):
            pl.when(neighbours == n)(lambda n=n: wait_rows(sem, rows * n))

    def wait_sides(sem, rows_of):
        for a in (1, 2):
            for b in (1, 2):
                for c in (1, 2):
                    here_now = (count[0] == a) & (count[1] == b) & (count[2] == c)
                    pl.when(here_now)(lambda a=a, b=b, c=c: wait_rows(sem, rows_of(a, b, c)))

    barrier = pltpu.get_barrier_semaphore()
    for code in others:

        @pl.when(ok[code])
        def _(code=code):
            pl.semaphore_signal(
                barrier, inc=1, device_id=device(offset_of(code)), device_id_type=MESH
            )

    own_load = pltpu.make_async_copy(part.at[0, 0, :, 0], nb.at[13, pl.ds(0, 6)], in_sem.at[0])
    own_load.start()
    for source, target in (
        (touch.at[0, 0], touch_v),
        (dcode.at[0, 0], dcode_v),
        (dslot.at[0, 0], dslot_v),
        (cont.at[0, 0, :, 0], cont_v),
        (frac, frac_v),
        (inter, int_v),
    ):
        pltpu.make_async_copy(source, target, in_sem.at[1]).start()
    pop_load = pltpu.make_async_copy(pop, f_v, in_sem.at[2])
    pop_load.start()

    lane = lax.broadcasted_iota(jnp.int32, (8, 128), 1)
    sub = lax.broadcasted_iota(jnp.int32, (8, 128), 0)

    def send_a(code):
        return pltpu.make_async_remote_copy(
            src_ref=nb.at[13],
            dst_ref=nb.at[26 - code],
            send_sem=sent,
            recv_sem=a_recv.at[int(0 not in offset_of(code))],
            device_id=device(offset_of(code)),
            device_id_type=MESH,
        )

    def send_c(code):
        return pltpu.make_async_remote_copy(
            src_ref=cs.at[code],
            dst_ref=cr.at[26 - code],
            send_sem=sent,
            recv_sem=c_recv,
            device_id=device(offset_of(code)),
            device_id_type=MESH,
        )

    def partial_sums():
        wait_rows(in_sem.at[1], 4 + CANDIDATES + 2 * CX * CY)
        entry = touch_v[0:1, :]
        wide = lax.broadcasted_iota(jnp.int32, (112, TOUCHES), 1)
        row = lax.broadcasted_iota(jnp.int32, (112, TOUCHES), 0)
        named = jnp.where((entry >> 7) == (row >> 2), wide + 1, 0).astype(jnp.float32)
        slot_row = lax.broadcasted_iota(jnp.int32, (SLOTS, TOUCHES), 0)
        placed = jnp.where((entry & 127) == slot_row, 1.0, 0.0)
        inverse = dot_lanes(named.astype(jnp.bfloat16), placed.astype(jnp.bfloat16))
        inv_v[...] = (inverse.astype(jnp.int32) - 1).reshape(14, 8, 128)
        code_row = jnp.broadcast_to(dcode_v[0:1, :], (8, 128))
        moved = jnp.concatenate(
            [jnp.where(code_row == code, lane + 1, 0).astype(jnp.float32) for code in MOVE_CODES]
            + [jnp.zeros((8, 128), jnp.float32)],
            axis=0,
        )
        tall = lax.broadcasted_iota(jnp.int32, (SLOTS, SLOTS), 0)
        landing = jnp.where(dslot_v[0:1, :] == tall, 1.0, 0.0)
        inverse2 = dot_lanes(moved.astype(jnp.bfloat16), landing.astype(jnp.bfloat16))
        inv2_v[...] = (inverse2.astype(jnp.int32) - 1).reshape(8, 8, 128)

        pop_load.wait()

        def moments(x, carry):
            for half in range(2):
                start = pl.multiple_of(CY * x + 8 * half, 8)
                rows = pl.ds(start, 8)
                f = [f_v[d, rows, :] for d in range(19)]
                rho = f[0]
                momentum = [None, None, None]
                for d in range(1, 19):
                    rho = rho + f[d]
                for n in range(3):
                    for d in range(1, 19):
                        if LATTICE[d][n] == 1:
                            momentum[n] = f[d] if momentum[n] is None else momentum[n] + f[d]
                    for d in range(1, 19):
                        if LATTICE[d][n] == -1:
                            momentum[n] = momentum[n] - f[d]
                eps = frac_v[rows, :]
                weight = jnp.where(
                    int_v[rows, :] < TOUCHES,
                    eps * (RELAX_TIME - 0.5) / (1.0 - eps + (RELAX_TIME - 0.5)),
                    0.0,
                )
                scale = 1.0 / rho
                mac[0, rows, :] = rho
                mac[1, rows, :] = weight
                for n in range(3):
                    mac[2 + n, rows, :] = momentum[n] * scale
                for n, term in enumerate(momentum + [rho]):
                    term = term * weight
                    if n == 3:
                        mac[5, rows, :] = term
                    high = term.astype(jnp.bfloat16).astype(jnp.float32)
                    split[pl.ds(8 * start + n, 8, stride=8), :] = high
                    split[pl.ds(8 * start + 4 + n, 8, stride=8), :] = term - high
            return carry

        lax.fori_loop(0, CX, moments, 0, unroll=2)

        low_row = lax.broadcasted_iota(jnp.int32, (32, 128), 0)

        def add_slab(x, total):
            left, right = [], []
            for y in range(CY):
                slots = int_v[pl.ds(CY * x + y, 1), :]
                tile = split[pl.ds(pl.multiple_of(8 * (CY * x + y), 8), 8), :]
                upper = jnp.broadcast_to(slots >> 5, (8, 128))
                picked = [jnp.where(upper == a, tile, 0.0) for a in range(8)]
                left.append(jnp.concatenate(picked, axis=0).astype(jnp.bfloat16))
                lower = jnp.broadcast_to(slots & 31, (32, 128))
                right.append(jnp.where(lower == low_row, 1.0, 0.0).astype(jnp.bfloat16))
            return total + dot_lanes(
                jnp.concatenate(left, axis=1), jnp.concatenate(right, axis=1)
            )

        total = lax.fori_loop(0, CX, add_slab, jnp.zeros((64, 32), jnp.float32), unroll=4)
        tables = []
        for h in range(2):
            table = jnp.concatenate(
                [total[8 * a : 8 * a + 8, :] for a in range(4 * h, 4 * h + 4)], axis=1
            )
            tables.append(table + pltpu.roll(table, 4, 0))

        for q in range(14):
            source = inv_v[q]
            index = source & 127
            picked = jnp.where(
                source < 128, lane_gather(tables[0], index), lane_gather(tables[1], index)
            )
            picked = jnp.where(source >= 0, picked, 0.0)
            cs[2 * q] = picked[0:4, :]
            cs[2 * q + 1] = picked[4:8, :]


    early = (here[2] == 1) | (here[1] == 4) | ((here[0] < 3) & (lax.rem(here[1], 4) < 3))
    pl.when(early)(partial_sums)

    own_load.wait()
    pl.semaphore_wait(barrier, neighbours)
    start_all(send_a)
    pl.when(jnp.logical_not(early))(partial_sums)

    start_all(send_c)

    def cell_rows(x, half):
        cells = pl.ds(pl.multiple_of(CY * x + 8 * half, 8), 8)
        return cells, pl.ds(pl.multiple_of(STRIDE * (x + 1) + PAD + 8 * half, 8), 8)

    def relax(x, carry):
        for half in range(2):
            rows, dest = cell_rows(x, half)
            rho = mac[0, rows, :]
            weight = mac[1, rows, :]
            u = [mac[2 + n, rows, :] for n in range(3)]
            alpha = (1.0 - weight) * (1.0 / RELAX_TIME)
            keep = 1.0 - alpha - weight
            even = (alpha - weight) * rho
            odd = 3.0 * (alpha + weight) * rho
            base = even * (1.0 - 1.5 * (u[0] * u[0] + u[1] * u[1] + u[2] * u[2]))
            even = 4.5 * even
            rel[PLACE[0], dest, :] = (1.0 - alpha) * f_v[0, rows, :] + WEIGHTS[0] * base
            for i, j in PAIRS:
                along = projected(u, i)
                symmetric = WEIGHTS[i] * (base + even * along * along)
                skew = WEIGHTS[i] * (odd * along)
                fi, fj = f_v[i, rows, :], f_v[j, rows, :]
                rel[PLACE[i], dest, :] = keep * fi + weight * fj + (symmetric + skew)
                rel[PLACE[j], dest, :] = keep * fj + weight * fi + (symmetric - skew)
        return carry

    lax.fori_loop(0, CX, relax, 0, unroll=2)

    def pack_ends(x, carry):
        for half in range(2):
            rows, dest = cell_rows(x, half)
            packed = jnp.zeros((8, 128), jnp.float32)
            for side in range(2):
                edge = 127 if side == 0 else 0
                values = [rel[PLACE[d], dest, :] for d in Z_MOVERS[side]]
                values += [mac[5, rows, :], int_v[rows, :].astype(jnp.float32)]
                for n, value in enumerate(values):
                    packed = jnp.where(lane == 8 * side + n, value[:, edge : edge + 1], packed)
            zm[rows, :] = packed
        return carry

    lax.fori_loop(0, CX, pack_ends, 0, unroll=CX)
    across = jnp.transpose(zm[...])

    def at_target(tile):
        up_y = jnp.where((lane & 15) == 0, pltpu.roll(tile, 128 - 15, 1), pltpu.roll(tile, 1, 1))
        down_y = jnp.where((lane & 15) == 15, pltpu.roll(tile, 15, 1), pltpu.roll(tile, 127, 1))
        moved_z = jnp.where(sub == 1, pltpu.roll(tile, 16, 1), tile)
        moved_z = jnp.where(sub == 2, pltpu.roll(tile, 112, 1), moved_z)
        moved_z = jnp.where(sub == 3, up_y, moved_z)
        return jnp.where(sub == 4, down_y, moved_z)

    for side in range(2):
        zc[side, 0] = at_target(across[8 * side : 8 * side + 8, :])
        for n in range(2):
            line = across[8 * side + 5 + n : 8 * side + 6 + n, :]
            zc[side, 1 + n] = at_target(jnp.broadcast_to(line, (8, 128)))

    touch_code, touch_slot = (
        [jnp.broadcast_to(part_of[:, 128 * h : 128 * h + 128], (8, 128)) for h in range(2)]
        for part_of in (touch_v[0:1, :] >> 7, touch_v[0:1, :] & 127)
    )
    zero = jnp.zeros((8, 128), jnp.float32)
    found = [zero, zero]

    def find_velocity(code):
        tile = nb[code]
        if code != 13:
            tile = jnp.where(ok[code], tile, 0.0)
            nb[code] = tile
        for h in range(2):
            found[h] = jnp.where(
                touch_code[h] == code, lane_gather(tile, touch_slot[h]), found[h]
            )

    corners = [code for code in others if 0 not in offset_of(code)]
    wait_sides(a_recv.at[0], lambda a, b, c: 8 * ((a + 1) * (b + 1) * (c + 1) - 1 - a * b * c))
    find_velocity(13)
    for code in others:
        if code not in corners:
            find_velocity(code)
    wait_sides(a_recv.at[1], lambda a, b, c: 8 * a * b * c)
    for code in corners:
        find_velocity(code)
    speed = [
        [jnp.broadcast_to(SPEED_UNIT * found[h][3 + n : 4 + n, :], (8, 128)) for n in range(3)]
        for h in range(2)
    ]

    def solid_part(slots, mass):
        index = slots & 127
        first = slots < 128
        v = [
            jnp.where(first, lane_gather(speed[0][n], index), lane_gather(speed[1][n], index))
            for n in range(3)
        ]
        base = mass * (1.0 - 1.5 * (v[0] * v[0] + v[1] * v[1] + v[2] * v[2]))
        return v, base, 4.5 * mass, 3.0 * mass

    def solid_term(parts, d):
        v, base, even, odd = parts
        along = projected(v, d)
        return WEIGHTS[d] * (base + along * (even * along + odd))

    def send_b(move):
        source, target, offset = move
        return pltpu.make_async_remote_copy(
            src_ref=source,
            dst_ref=target,
            send_sem=sent,
            recv_sem=b_recv.at[abs(offset[2])],
            device_id=device(offset),
            device_id_type=MESH,
        )

    def code_of(offset):
        return 9 * (offset[0] + 1) + 3 * (offset[1] + 1) + offset[2] + 1

    def start_b(moves):
        for move in moves:
            pl.when(ok[code_of(move[2])])(lambda move=move: send_b(move).start())

    signs = [[jnp.zeros((8, 128), jnp.float32) for n in range(3)] for side in range(2)]
    for side in range(2):
        for n, d in enumerate(Z_MOVERS[side]):
            for axis in range(3):
                if LATTICE[d][axis] != 0:
                    signs[side][axis] = jnp.where(
                        sub == n, float(LATTICE[d][axis]), signs[side][axis]
                    )
    share = jnp.where(sub == 0, 1.0 / 18.0, 1.0 / 36.0)
    for side in range(2):
        v, base, even, odd = solid_part(zc[side, 2].astype(jnp.int32), zc[side, 1])
        along = signs[side][0] * v[0] + signs[side][1] * v[1] + signs[side][2] * v[2]
        zs[side] = zc[side, 0] + share * (base + along * (even * along + odd))
    moves = []
    for n, (step_x, step_y) in ((3, (0, -1)), (2, (0, 1)), (0, (1, 0)), (1, (-1, 0))):
        for side in (1, 0):
            moves.append((zs.at[side], ze.at[side, n], (step_x, step_y, 1 - 2 * side)))
    start_b(moves)
    for side in range(2):
        x = CX - 1 if side == 0 else 0
        for half in range(2):
            rows, dest = cell_rows(x, half)
            parts = solid_part(int_v[rows, :], mac[5, rows, :])
            for n, d in enumerate((X_UP, X_DOWN)[side]):
                value = rel[PLACE[d], dest, :] + solid_term(parts, d)
                xs[side, n, pl.ds(8 * half, 8), :] = value
    for side in range(2):
        y = CY - 1 if side == 0 else 0
        rows = pl.ds(y, CX, stride=CY)
        dest = pl.ds(STRIDE + PAD + y, CX, stride=STRIDE)
        parts = solid_part(int_v[rows, :], mac[5, rows, :])
        for n, d in enumerate(Y_MOVERS[side]):
            value = rel[PLACE[d], dest, :] + solid_term(parts, d)
            if LATTICE[d][0] != 0:
                value = pltpu.roll(value, LATTICE[d][0] % CX, 0)
            ys[side, n] = value
    start_b([(xs.at[side], xr.at[side], (1 - 2 * side, 0, 0)) for side in (1, 0)])
    moves = []
    for side in (1, 0):
        step = 1 - 2 * side
        moves.append((ys.at[side, 1], ye.at[side, 0], (1, step, 0)))
        moves.append((ys.at[side, 2], ye.at[side, 1], (-1, step, 0)))
    for side in (1, 0):
        moves.append((ys.at[side], yr.at[side], (0, 1 - 2 * side, 0)))
    start_b(moves)
    start_b([(zs.at[side], zr.at[side], (0, 0, 1 - 2 * side)) for side in (1, 0)])

    listed = [
        cont_v[0:8, :],
        jnp.concatenate([cont_v[8:12, :], jnp.full((4, 128), 27 * SLOTS, jnp.int32)], axis=0),
    ]
    listed_code = [entries >> 7 for entries in listed]
    listed_slot = [entries & 127 for entries in listed]

    def find_partner(code, partner):
        shifts = (code // 9 - 1, code // 3 % 3 - 1, code % 3 - 1)
        result = []
        for n in range(3):
            line = nb[code, pl.ds(n, 1), :] + shifts[n].astype(jnp.float32) * SPANS[n]
            line = jnp.broadcast_to(line, (8, 128))
            for h in range(2):
                result.append(
                    jnp.where(
                        listed_code[h] == code,
                        lane_gather(line, listed_slot[h]),
                        partner[2 * n + h],
                    )
                )
        return tuple(result)

    partner = lax.fori_loop(0, 27, find_partner, (zero,) * 6, unroll=27)
    force = [None, None, None]
    for h in range(2):
        apart = [nb[13, n : n + 1, :] - partner[2 * n + h] for n in range(3)]
        square = apart[0] * apart[0] + apart[1] * apart[1] + apart[2] * apart[2]
        soften = 1.0 + 0.25 * square
        strength = jnp.where(listed_code[h] < 27, CONTACT_GAIN / (soften * soften), 0.0)
        for n in range(3):
            term = jnp.sum(apart[n] * strength, axis=0, keepdims=True)
            force[n] = term if h == 0 else force[n] + term

    wait_all(c_recv, 4)
    hydro = cs[13]
    for code in others:
        hydro = hydro + jnp.where(ok[code], cr[code], 0.0)
    rec[6:8, :] = jnp.zeros((2, 128), jnp.float32)
    for n in range(3):
        speed_old = nb[13, 3 + n : 4 + n, :]
        pulled = hydro[n : n + 1, :] - (SPEED_UNIT * speed_old) * hydro[3:4, :]
        speed_new = speed_old + FORCE_SCALE * pulled + force[n]
        if n == 2:
            speed_new = speed_new - GRAVITY_STEP
        rec[3 + n : 4 + n, :] = speed_new
        rec[n : n + 1, :] = nb[13, n : n + 1, :] + speed_new * (SPEED_UNIT / R)

    record = rec[...]
    for n, code in enumerate(MOVE_CODES):
        shift = zero
        for axis, step in enumerate(offset_of(code)):
            if step != 0:
                shift = jnp.where(sub == axis, step * SPANS[axis], shift)
        source = inv2_v[n]
        picked = lane_gather(record - shift, source & 127)
        ds[n] = jnp.where(source >= 0, picked, 0.0)
    def send_d(n):
        return pltpu.make_async_remote_copy(
            src_ref=ds.at[n],
            dst_ref=dr.at[6 - n],
            send_sem=sent,
            recv_sem=d_recv,
            device_id=device(offset_of(MOVE_CODES[n])),
            device_id_type=MESH,
        )

    movers = [n for n in range(7) if MOVE_CODES[n] != 13]
    for n in movers:
        pl.when(ok[MOVE_CODES[n]])(lambda n=n: send_d(n).start())

    def solid(x, carry):
        for half in range(2):
            rows, dest = cell_rows(x, half)
            v, base, even, odd = solid_part(int_v[rows, :], mac[5, rows, :])
            rel[PLACE[0], dest, :] = rel[PLACE[0], dest, :] + WEIGHTS[0] * base
            for i, j in PAIRS:
                along = projected(v, i)
                symmetric = WEIGHTS[i] * (base + even * along * along)
                skew = WEIGHTS[i] * (odd * along)
                rel[PLACE[i], dest, :] = rel[PLACE[i], dest, :] + (symmetric + skew)
                rel[PLACE[j], dest, :] = rel[PLACE[j], dest, :] + (symmetric - skew)
        return carry

    lax.fori_loop(0, CX, solid, 0, unroll=CX)

    def near_rows(a, b):
        return 8 * (10 * a + 5 * b + a * b)

    def far_rows(a, b, c):
        return 8 * c * (1 + a + b)

    wait_sides(b_recv.at[0], lambda a, b, c: near_rows(a, b))
    for side in range(2):
        x = -1 if side == 0 else CX
        for n, d in enumerate((X_UP, X_DOWN)[side]):
            rel[PLACE[d], pl.ds(STRIDE * (x + 1) + PAD, CY), :] = xr[side, n]
    for side in range(2):
        y = -1 if side == 0 else CY
        for n, d in enumerate(Y_MOVERS[side]):
            tile = yr[side, n]
            if n == 1:
                tile = jnp.where(sub == 0, ye[side, 0], tile)
            if n == 2:
                tile = jnp.where(sub == CX - 1, ye[side, 1], tile)
            start = STRIDE * (1 - LATTICE[d][0]) + PAD + y
            rel[PLACE[d], pl.ds(start, CX, stride=STRIDE), :] = tile
    wait_sides(d_recv, lambda a, b, c: 8 * (a + b + c))
    arrived = ds[3]
    for n in movers:
        arrived = arrived + jnp.where(ok[MOVE_CODES[n]], dr[n], 0.0)
    out_part[0, 0, :, 0, :] = arrived[0:6, :]

    wait_sides(b_recv.at[1], far_rows)
    for side in range(2):
        tile = zr[side]
        tile = jnp.where((sub == 1) & (lane < CY), ze[side, 0], tile)
        tile = jnp.where((sub == 2) & (lane >= 128 - CY), ze[side, 1], tile)
        tile = jnp.where((sub == 3) & ((lane & 15) == 0), ze[side, 2], tile)
        tile = jnp.where((sub == 4) & ((lane & 15) == 15), ze[side, 3], tile)
        col_out[8 * side : 8 * side + 8, :] = tile
    wait_sides(
        sent,
        lambda a, b, c: 12 * ((a + 1) * (b + 1) * (c + 1) - 1)
        + near_rows(a, b)
        + far_rows(a, b, c)
        + 8 * (a + b + c),
    )


def stream_kernel(sizes, rel, ends, records, out_pop, out_part, out_v, out_sem, part_sem):
    here = [lax.axis_index(axis) for axis in AXES]
    keep_records = pltpu.make_async_copy(records, out_part, part_sem)
    keep_records.start()
    lane = lax.broadcasted_iota(jnp.int32, (8, 128), 1)
    sub = lax.broadcasted_iota(jnp.int32, (8, 128), 0)
    low_wall = [here[n] == 0 for n in range(3)]
    high_wall = [here[n] == sizes[n] - 1 for n in range(3)]
    order = sorted(range(19), key=lambda d: LATTICE[d][2] != 0)

    def put(d):
        return pltpu.make_async_copy(out_v.at[d], out_pop.at[d], out_sem)

    for d in order:
        vector = LATTICE[d]
        if d == order[4]:
            columns = jnp.transpose(
                jnp.concatenate([ends[...], jnp.zeros((112, 128), jnp.float32)], axis=0)
            )
        for x in range(CX):
            for half in range(2):
                cells = pl.ds(CY * x + 8 * half, 8)
                walls = {
                    (0, 1): low_wall[0] if x == 0 else None,
                    (0, -1): high_wall[0] if x == CX - 1 else None,
                    (1, 1): low_wall[1] & (sub == 0) if half == 0 else None,
                    (1, -1): high_wall[1] & (sub == 7) if half == 1 else None,
                    (2, 1): low_wall[2] & (lane == 0),
                    (2, -1): high_wall[2] & (lane == 127),
                }
                start = STRIDE * (x + 1 - vector[0]) + PAD + 8 * half - vector[1]
                value = rel[PLACE[d], pl.ds(start, 8), :]
                if vector[2] != 0:
                    side = 0 if vector[2] == 1 else 1
                    column = 8 * side + Z_MOVERS[side].index(d)
                    value = jnp.where(
                        lane == (0 if side == 0 else 127),
                        columns[CY * x + 8 * half : CY * x + 8 * half + 8, column : column + 1],
                        pltpu.roll(value, vector[2] % 128, 1),
                    )
                blocked = None
                for axis in range(3):
                    wall = walls.get((axis, vector[axis]))
                    if wall is not None:
                        blocked = wall if blocked is None else blocked | wall
                if blocked is not None:
                    back = rel[PLACE[OPPOSITE[d]], pl.ds(STRIDE * (x + 1) + PAD + 8 * half, 8), :]
                    value = jnp.where(blocked, back, value)
                out_v[d, cells, :] = value
        put(d).start()
    pltpu.make_async_copy(out_v, out_pop, out_sem).wait()
    keep_records.wait()


def body(sizes, pop, frac, inter, touch, part, cont, dcode, dslot):
    f32, i32 = jnp.float32, jnp.int32
    cells = CX * CY
    part, cont = (jnp.transpose(a, (0, 1, 3, 2, 4)) for a in (part, cont))
    args = (
        pop.reshape(19, cells, CZ),
        frac.reshape(cells, CZ),
        inter.reshape(cells, CZ),
        touch,
        part,
        cont,
        dcode,
        dslot,
    )
    vmem = pltpu.VMEM
    sems = pltpu.SemaphoreType.DMA
    in_vmem = pl.BlockSpec(memory_space=vmem)
    in_any = pl.BlockSpec(memory_space=pl.ANY)
    relaxed, columns, records = pl.pallas_call(
        lambda *refs: kernel(sizes, *refs),
        out_shape=(
            vmem((19, STRIDE * (CX + 2), CZ), f32),
            vmem((16, 128), f32),
            vmem((1, 1, 6, 1, SLOTS), f32),
        ),
        in_specs=[in_any] * 8,
        out_specs=(in_vmem,) * 3,
        scratch_shapes=[
            vmem((19, cells, CZ), f32),
            vmem((cells, CZ), f32),
            vmem((cells, CZ), i32),
            vmem((1, TOUCHES), i32),
            vmem((CANDIDATES, SLOTS), i32),
            vmem((1, SLOTS), i32),
            vmem((1, SLOTS), i32),
            vmem((27, 8, 128), f32),
            vmem((6, cells, CZ), f32),
            vmem((8 * cells, CZ), f32),
            vmem((14, 8, 128), i32),
            vmem((8, 8, 128), i32),
            vmem((28, 4, 128), f32),
            vmem((27, 4, 128), f32),
            vmem((2, 3, 8, 128), f32),
            vmem((2, 5, CY, CZ), f32),
            vmem((2, 5, CY, CZ), f32),
            vmem((2, 5, CX, CZ), f32),
            vmem((2, 5, CX, CZ), f32),
            vmem((2, 2, CX, CZ), f32),
            vmem((cells, 128), f32),
            vmem((2, 8, 128), f32),
            vmem((2, 8, 128), f32),
            vmem((2, 4, 8, 128), f32),
            vmem((8, 128), f32),
            vmem((7, 8, 128), f32),
            vmem((7, 8, 128), f32),
            sems((3,)),
            sems((2,)),
            sems((2,)),
            sems,
            sems,
            sems,
        ],
        compiler_params=pltpu.CompilerParams(collective_id=0, has_side_effects=True),
    )(*args)
    populations, records = pl.pallas_call(
        lambda *refs: stream_kernel(sizes, *refs),
        out_shape=(
            jax.ShapeDtypeStruct((19, cells, CZ), f32),
            jax.ShapeDtypeStruct((1, 1, 6, 1, SLOTS), f32),
        ),
        in_specs=[in_vmem] * 3,
        out_specs=(in_any,) * 2,
        scratch_shapes=[vmem((19, cells, CZ), f32), sems, sems],
    )(*(pltpu.with_memory_space_constraint(a, vmem) for a in (relaxed, columns, records)))
    return populations.reshape(19, CX, CY, CZ), jnp.transpose(records, (0, 1, 3, 2, 4))


def solution(mesh):
    sizes = tuple(mesh.shape[axis] for axis in AXES)
    cells, blocks = P(*AXES), P(*AXES, None)
    records = P(*AXES, None, None)
    fields = P(None, *AXES)
    return jax.shard_map(
        lambda *args: body(sizes, *args),
        mesh=mesh,
        in_specs=(fields, cells, cells, blocks, records, records, blocks, blocks),
        out_specs=(fields, records),
        check_vma=False,
    )
```

```python
import jax
import jax.numpy as jnp
from jax import lax
from jax.experimental import pallas as pl
from jax.experimental.pallas import tpu as pltpu
from jax.sharding import PartitionSpec as P

LATTICE = [
    (0, 0, 0),
    (1, 0, 0),
    (-1, 0, 0),
    (0, 1, 0),
    (0, -1, 0),
    (0, 0, 1),
    (0, 0, -1),
    (1, 1, 0),
    (-1, -1, 0),
    (1, -1, 0),
    (-1, 1, 0),
    (1, 0, 1),
    (-1, 0, -1),
    (1, 0, -1),
    (-1, 0, 1),
    (0, 1, 1),
    (0, -1, -1),
    (0, 1, -1),
    (0, -1, 1),
]
OPPOSITE = [0, 2, 1, 4, 3, 6, 5, 8, 7, 10, 9, 12, 11, 14, 13, 16, 15, 18, 17]
WEIGHTS = [1.0 / 3.0] + [1.0 / 18.0] * 6 + [1.0 / 36.0] * 12
PAIRS = [(i, i + 1) for i in range(1, 19, 2)]
RELAX_TIME = 0.8
SPEED_UNIT = 0.05
FORCE_SCALE = 0.1
CONTACT_GAIN = 1.0
GRAVITY_STEP = 0.1
R = 8.0
CX, CY, CZ, SLOTS, TOUCHES, CANDIDATES = 8, 16, 128, 128, 256, 12
SPANS = (CX / R, CY / R, CZ / R)
AXES = ("gx", "gy", "gz")
MESH = pl.DeviceIdType.MESH

X_UP, X_DOWN = [1, 7, 9, 11, 13], [2, 8, 10, 12, 14]
Y_MOVERS = [[3, 7, 10, 15, 17], [4, 9, 8, 18, 16]]
Z_MOVERS = [[5, 11, 14, 15, 18], [6, 13, 12, 17, 16]]
PLACE = {d: n for n, d in enumerate(X_UP + X_DOWN + [0, 3, 4, 5, 6, 15, 16, 17, 18])}
MOVE_CODES = [4, 10, 12, 13, 14, 16, 22]
PAD = 8
STRIDE = CY + 2 * PAD


def offset_of(code):
    return (code // 9 - 1, code // 3 % 3 - 1, code % 3 - 1)


def projected(velocity, d):
    along = None
    for n in range(3):
        if LATTICE[d][n] == 1:
            along = velocity[n] if along is None else along + velocity[n]
        elif LATTICE[d][n] == -1:
            along = -velocity[n] if along is None else along - velocity[n]
    return along


def lane_gather(table, index):
    return jnp.take_along_axis(table, index, axis=1, mode="promise_in_bounds")


def dot_lanes(a, b):
    return lax.dot_general(a, b, (((1,), (1,)), ((), ())), preferred_element_type=jnp.float32)


def kernel(
    sizes,
    pop,
    frac,
    inter,
    touch,
    part,
    cont,
    dcode,
    dslot,
    rel_out,
    col_out,
    out_part,
    f_v,
    frac_v,
    int_v,
    touch_v,
    cont_v,
    dcode_v,
    dslot_v,
    nb,
    mac,
    split,
    inv_v,
    inv2_v,
    cs,
    cr,
    zc,
    xs,
    xr,
    ys,
    yr,
    ye,
    zm,
    zs,
    zr,
    ze,
    rec,
    ds,
    dr,
    in_sem,
    a_recv,
    b_recv,
    c_recv,
    d_recv,
    sent,
):
    rel = rel_out
    here = [lax.axis_index(axis) for axis in AXES]

    def device(offset):
        return tuple(
            here[n] if offset[n] == 0 else lax.rem(here[n] + offset[n] + sizes[n], sizes[n])
            for n in range(3)
        )

    def exists(offset):
        ok = None
        for n in range(3):
            if offset[n] != 0:
                test = here[n] > 0 if offset[n] < 0 else here[n] < sizes[n] - 1
                ok = test if ok is None else ok & test
        return ok

    others = [code for code in range(27) if code != 13]
    others.sort(key=lambda code: -sum(abs(step) for step in offset_of(code)))
    ok = {code: exists(offset_of(code)) for code in others}
    def start_all(make):
        for code in others:
            pl.when(ok[code])(lambda code=code: make(code).start())

    count = [
        (here[n] > 0).astype(jnp.int32) + (here[n] < sizes[n] - 1).astype(jnp.int32)
        for n in range(3)
    ]

    neighbours = (count[0] + 1) * (count[1] + 1) * (count[2] + 1) - 1

    def wait_rows(sem, rows):
        pltpu.make_async_copy(split.at[pl.ds(0, rows)], split.at[pl.ds(0, rows)], sem).wait()

    def wait_all(sem, rows):
        for n in sorted({a * b * c - 1 for a in (2, 3) for b in (2, 3) for c in (2, 3)}):
            pl.when(neighbours == n)(lambda n=n: wait_rows(sem, rows * n))

    def wait_sides(sem, rows_of):
        for a in (1, 2):
            for b in (1, 2):
                for c in (1, 2):
                    here_now = (count[0] == a) & (count[1] == b) & (count[2] == c)
                    pl.when(here_now)(lambda a=a, b=b, c=c: wait_rows(sem, rows_of(a, b, c)))

    barrier = pltpu.get_barrier_semaphore()
    for code in others:

        @pl.when(ok[code])
        def _(code=code):
            pl.semaphore_signal(
                barrier, inc=1, device_id=device(offset_of(code)), device_id_type=MESH
            )

    own_load = pltpu.make_async_copy(part.at[0, 0, :, 0], nb.at[13, pl.ds(0, 6)], in_sem.at[0])
    own_load.start()
    for source, target in (
        (touch.at[0, 0], touch_v),
        (dcode.at[0, 0], dcode_v),
        (dslot.at[0, 0], dslot_v),
        (cont.at[0, 0, :, 0], cont_v),
        (frac, frac_v),
        (inter, int_v),
    ):
        pltpu.make_async_copy(source, target, in_sem.at[1]).start()
    def pop_load(n):
        rows = pl.ds(64 * n, 64)
        return pltpu.make_async_copy(pop.at[:, rows], f_v.at[:, rows], in_sem.at[2 + n])

    for n in range(2):
        pop_load(n).start()

    lane = lax.broadcasted_iota(jnp.int32, (8, 128), 1)
    sub = lax.broadcasted_iota(jnp.int32, (8, 128), 0)

    def send_a(code):
        return pltpu.make_async_remote_copy(
            src_ref=nb.at[13],
            dst_ref=nb.at[26 - code],
            send_sem=sent,
            recv_sem=a_recv.at[int(0 not in offset_of(code))],
            device_id=device(offset_of(code)),
            device_id_type=MESH,
        )

    def send_c(code):
        return pltpu.make_async_remote_copy(
            src_ref=cs.at[code],
            dst_ref=cr.at[26 - code],
            send_sem=sent,
            recv_sem=c_recv,
            device_id=device(offset_of(code)),
            device_id_type=MESH,
        )

    def partial_sums():
        wait_rows(in_sem.at[1], 4 + CANDIDATES + 2 * CX * CY)
        entry = touch_v[0:1, :]
        wide = lax.broadcasted_iota(jnp.int32, (112, TOUCHES), 1)
        row = lax.broadcasted_iota(jnp.int32, (112, TOUCHES), 0)
        named = jnp.where((entry >> 7) == (row >> 2), wide + 1, 0).astype(jnp.float32)
        slot_row = lax.broadcasted_iota(jnp.int32, (SLOTS, TOUCHES), 0)
        placed = jnp.where((entry & 127) == slot_row, 1.0, 0.0)
        inverse = dot_lanes(named.astype(jnp.bfloat16), placed.astype(jnp.bfloat16))
        inv_v[...] = (inverse.astype(jnp.int32) - 1).reshape(14, 8, 128)
        code_row = jnp.broadcast_to(dcode_v[0:1, :], (8, 128))
        moved = jnp.concatenate(
            [jnp.where(code_row == code, lane + 1, 0).astype(jnp.float32) for code in MOVE_CODES]
            + [jnp.zeros((8, 128), jnp.float32)],
            axis=0,
        )
        tall = lax.broadcasted_iota(jnp.int32, (SLOTS, SLOTS), 0)
        landing = jnp.where(dslot_v[0:1, :] == tall, 1.0, 0.0)
        inverse2 = dot_lanes(moved.astype(jnp.bfloat16), landing.astype(jnp.bfloat16))
        inv2_v[...] = (inverse2.astype(jnp.int32) - 1).reshape(8, 8, 128)


        def moments(x, carry):
            for half in range(2):
                start = pl.multiple_of(CY * x + 8 * half, 8)
                rows = pl.ds(start, 8)
                f = [f_v[d, rows, :] for d in range(19)]
                rho = f[0]
                momentum = [None, None, None]
                for d in range(1, 19):
                    rho = rho + f[d]
                for n in range(3):
                    for d in range(1, 19):
                        if LATTICE[d][n] == 1:
                            momentum[n] = f[d] if momentum[n] is None else momentum[n] + f[d]
                    for d in range(1, 19):
                        if LATTICE[d][n] == -1:
                            momentum[n] = momentum[n] - f[d]
                eps = frac_v[rows, :]
                weight = jnp.where(
                    int_v[rows, :] < TOUCHES,
                    eps * (RELAX_TIME - 0.5) / (1.0 - eps + (RELAX_TIME - 0.5)),
                    0.0,
                )
                scale = 1.0 / rho
                mac[0, rows, :] = rho
                mac[1, rows, :] = weight
                for n in range(3):
                    mac[2 + n, rows, :] = momentum[n] * scale
                for n, term in enumerate(momentum + [rho]):
                    term = term * weight
                    if n == 3:
                        mac[5, rows, :] = term
                    high = term.astype(jnp.bfloat16).astype(jnp.float32)
                    split[pl.ds(8 * start + n, 8, stride=8), :] = high
                    split[pl.ds(8 * start + 4 + n, 8, stride=8), :] = term - high
            return carry

        for n in range(2):
            pop_load(n).wait()
            lax.fori_loop(4 * n, 4 * n + 4, moments, 0, unroll=2)

        low_row = lax.broadcasted_iota(jnp.int32, (32, 128), 0)

        def add_slab(x, total):
            left, right = [], []
            for y in range(CY):
                slots = int_v[pl.ds(CY * x + y, 1), :]
                tile = split[pl.ds(pl.multiple_of(8 * (CY * x + y), 8), 8), :]
                upper = jnp.broadcast_to(slots >> 5, (8, 128))
                picked = [jnp.where(upper == a, tile, 0.0) for a in range(8)]
                left.append(jnp.concatenate(picked, axis=0).astype(jnp.bfloat16))
                lower = jnp.broadcast_to(slots & 31, (32, 128))
                right.append(jnp.where(lower == low_row, 1.0, 0.0).astype(jnp.bfloat16))
            return total + dot_lanes(
                jnp.concatenate(left, axis=1), jnp.concatenate(right, axis=1)
            )

        total = lax.fori_loop(0, CX, add_slab, jnp.zeros((64, 32), jnp.float32), unroll=8)
        tables = []
        for h in range(2):
            table = jnp.concatenate(
                [total[8 * a : 8 * a + 8, :] for a in range(4 * h, 4 * h + 4)], axis=1
            )
            tables.append(table + pltpu.roll(table, 4, 0))

        for q in range(14):
            source = inv_v[q]
            index = source & 127
            picked = jnp.where(
                source < 128, lane_gather(tables[0], index), lane_gather(tables[1], index)
            )
            picked = jnp.where(source >= 0, picked, 0.0)
            cs[2 * q] = picked[0:4, :]
            cs[2 * q + 1] = picked[4:8, :]


    early = (here[2] == 1) | (here[1] == 4) | ((here[0] < 2) & (lax.rem(here[1], 4) < 2))
    pl.when(early)(partial_sums)

    own_load.wait()
    pl.semaphore_wait(barrier, neighbours)
    start_all(send_a)
    pl.when(jnp.logical_not(early))(partial_sums)

    start_all(send_c)

    def cell_rows(x, half):
        cells = pl.ds(pl.multiple_of(CY * x + 8 * half, 8), 8)
        return cells, pl.ds(pl.multiple_of(STRIDE * (x + 1) + PAD + 8 * half, 8), 8)

    def relax(x, carry):
        for half in range(2):
            rows, dest = cell_rows(x, half)
            rho = mac[0, rows, :]
            weight = mac[1, rows, :]
            u = [mac[2 + n, rows, :] for n in range(3)]
            alpha = (1.0 - weight) * (1.0 / RELAX_TIME)
            keep = 1.0 - alpha - weight
            even = (alpha - weight) * rho
            odd = 3.0 * (alpha + weight) * rho
            base = even * (1.0 - 1.5 * (u[0] * u[0] + u[1] * u[1] + u[2] * u[2]))
            even = 4.5 * even
            rel[PLACE[0], dest, :] = (1.0 - alpha) * f_v[0, rows, :] + WEIGHTS[0] * base
            for i, j in PAIRS:
                along = projected(u, i)
                symmetric = WEIGHTS[i] * (base + even * along * along)
                skew = WEIGHTS[i] * (odd * along)
                fi, fj = f_v[i, rows, :], f_v[j, rows, :]
                rel[PLACE[i], dest, :] = keep * fi + weight * fj + (symmetric + skew)
                rel[PLACE[j], dest, :] = keep * fj + weight * fi + (symmetric - skew)
        return carry

    lax.fori_loop(0, CX, relax, 0, unroll=2)

    def pack_ends(x, carry):
        for half in range(2):
            rows, dest = cell_rows(x, half)
            packed = jnp.zeros((8, 128), jnp.float32)
            for side in range(2):
                edge = 127 if side == 0 else 0
                values = [rel[PLACE[d], dest, :] for d in Z_MOVERS[side]]
                values += [mac[5, rows, :], int_v[rows, :].astype(jnp.float32)]
                for n, value in enumerate(values):
                    packed = jnp.where(lane == 8 * side + n, value[:, edge : edge + 1], packed)
            zm[rows, :] = packed
        return carry

    lax.fori_loop(0, CX, pack_ends, 0, unroll=CX)
    across = jnp.transpose(zm[...])

    def at_target(tile):
        up_y = jnp.where((lane & 15) == 0, pltpu.roll(tile, 128 - 15, 1), pltpu.roll(tile, 1, 1))
        down_y = jnp.where((lane & 15) == 15, pltpu.roll(tile, 15, 1), pltpu.roll(tile, 127, 1))
        moved_z = jnp.where(sub == 1, pltpu.roll(tile, 16, 1), tile)
        moved_z = jnp.where(sub == 2, pltpu.roll(tile, 112, 1), moved_z)
        moved_z = jnp.where(sub == 3, up_y, moved_z)
        return jnp.where(sub == 4, down_y, moved_z)

    for side in range(2):
        zc[side, 0] = at_target(across[8 * side : 8 * side + 8, :])
        for n in range(2):
            line = across[8 * side + 5 + n : 8 * side + 6 + n, :]
            zc[side, 1 + n] = at_target(jnp.broadcast_to(line, (8, 128)))

    touch_code, touch_slot = (
        [jnp.broadcast_to(part_of[:, 128 * h : 128 * h + 128], (8, 128)) for h in range(2)]
        for part_of in (touch_v[0:1, :] >> 7, touch_v[0:1, :] & 127)
    )
    zero = jnp.zeros((8, 128), jnp.float32)
    found = [zero, zero]

    def find_velocity(code):
        tile = nb[code]
        if code != 13:
            tile = jnp.where(ok[code], tile, 0.0)
            nb[code] = tile
        for h in range(2):
            found[h] = jnp.where(
                touch_code[h] == code, lane_gather(tile, touch_slot[h]), found[h]
            )

    corners = [code for code in others if 0 not in offset_of(code)]
    wait_sides(a_recv.at[0], lambda a, b, c: 8 * ((a + 1) * (b + 1) * (c + 1) - 1 - a * b * c))
    find_velocity(13)
    for code in others:
        if code not in corners:
            find_velocity(code)
    wait_sides(a_recv.at[1], lambda a, b, c: 8 * a * b * c)
    for code in corners:
        find_velocity(code)
    speed = [
        [jnp.broadcast_to(SPEED_UNIT * found[h][3 + n : 4 + n, :], (8, 128)) for n in range(3)]
        for h in range(2)
    ]

    def solid_part(slots, mass):
        index = slots & 127
        first = slots < 128
        v = [
            jnp.where(first, lane_gather(speed[0][n], index), lane_gather(speed[1][n], index))
            for n in range(3)
        ]
        base = mass * (1.0 - 1.5 * (v[0] * v[0] + v[1] * v[1] + v[2] * v[2]))
        return v, base, 4.5 * mass, 3.0 * mass

    def solid_term(parts, d):
        v, base, even, odd = parts
        along = projected(v, d)
        return WEIGHTS[d] * (base + along * (even * along + odd))

    def send_b(move):
        source, target, offset = move
        return pltpu.make_async_remote_copy(
            src_ref=source,
            dst_ref=target,
            send_sem=sent,
            recv_sem=b_recv.at[abs(offset[2])],
            device_id=device(offset),
            device_id_type=MESH,
        )

    def code_of(offset):
        return 9 * (offset[0] + 1) + 3 * (offset[1] + 1) + offset[2] + 1

    def start_b(moves):
        for move in moves:
            pl.when(ok[code_of(move[2])])(lambda move=move: send_b(move).start())

    signs = [[jnp.zeros((8, 128), jnp.float32) for n in range(3)] for side in range(2)]
    for side in range(2):
        for n, d in enumerate(Z_MOVERS[side]):
            for axis in range(3):
                if LATTICE[d][axis] != 0:
                    signs[side][axis] = jnp.where(
                        sub == n, float(LATTICE[d][axis]), signs[side][axis]
                    )
    share = jnp.where(sub == 0, 1.0 / 18.0, 1.0 / 36.0)
    for side in range(2):
        v, base, even, odd = solid_part(zc[side, 2].astype(jnp.int32), zc[side, 1])
        along = signs[side][0] * v[0] + signs[side][1] * v[1] + signs[side][2] * v[2]
        zs[side] = zc[side, 0] + share * (base + along * (even * along + odd))
    moves = []
    for n, (step_x, step_y) in ((3, (0, -1)), (2, (0, 1)), (0, (1, 0)), (1, (-1, 0))):
        for side in (1, 0):
            moves.append((zs.at[side], ze.at[side, n], (step_x, step_y, 1 - 2 * side)))
    start_b(moves)
    for side in range(2):
        x = CX - 1 if side == 0 else 0
        for half in range(2):
            rows, dest = cell_rows(x, half)
            parts = solid_part(int_v[rows, :], mac[5, rows, :])
            for n, d in enumerate((X_UP, X_DOWN)[side]):
                value = rel[PLACE[d], dest, :] + solid_term(parts, d)
                xs[side, n, pl.ds(8 * half, 8), :] = value
    for side in range(2):
        y = CY - 1 if side == 0 else 0
        rows = pl.ds(y, CX, stride=CY)
        dest = pl.ds(STRIDE + PAD + y, CX, stride=STRIDE)
        parts = solid_part(int_v[rows, :], mac[5, rows, :])
        for n, d in enumerate(Y_MOVERS[side]):
            value = rel[PLACE[d], dest, :] + solid_term(parts, d)
            if LATTICE[d][0] != 0:
                value = pltpu.roll(value, LATTICE[d][0] % CX, 0)
            ys[side, n] = value
    moves = []
    for side in (1, 0):
        step = 1 - 2 * side
        moves.append((ys.at[side, 1], ye.at[side, 0], (1, step, 0)))
        moves.append((ys.at[side, 2], ye.at[side, 1], (-1, step, 0)))
    for side in (1, 0):
        moves.append((ys.at[side], yr.at[side], (0, 1 - 2 * side, 0)))
    for side in (1, 0):
        moves.append((xs.at[side], xr.at[side], (1 - 2 * side, 0, 0)))
    for side in (1, 0):
        moves.append((zs.at[side], zr.at[side], (0, 0, 1 - 2 * side)))
    start_b(moves)

    listed = [
        cont_v[0:8, :],
        jnp.concatenate([cont_v[8:12, :], jnp.full((4, 128), 27 * SLOTS, jnp.int32)], axis=0),
    ]
    listed_code = [entries >> 7 for entries in listed]
    listed_slot = [entries & 127 for entries in listed]

    def find_partner(code, partner):
        shifts = (code // 9 - 1, code // 3 % 3 - 1, code % 3 - 1)
        result = []
        for n in range(3):
            line = nb[code, pl.ds(n, 1), :] + shifts[n].astype(jnp.float32) * SPANS[n]
            line = jnp.broadcast_to(line, (8, 128))
            for h in range(2):
                result.append(
                    jnp.where(
                        listed_code[h] == code,
                        lane_gather(line, listed_slot[h]),
                        partner[2 * n + h],
                    )
                )
        return tuple(result)

    partner = lax.fori_loop(0, 27, find_partner, (zero,) * 6, unroll=27)
    force = [None, None, None]
    for h in range(2):
        apart = [nb[13, n : n + 1, :] - partner[2 * n + h] for n in range(3)]
        square = apart[0] * apart[0] + apart[1] * apart[1] + apart[2] * apart[2]
        soften = 1.0 + 0.25 * square
        strength = jnp.where(listed_code[h] < 27, CONTACT_GAIN / (soften * soften), 0.0)
        for n in range(3):
            term = jnp.sum(apart[n] * strength, axis=0, keepdims=True)
            force[n] = term if h == 0 else force[n] + term

    wait_all(c_recv, 4)
    hydro = cs[13]
    for code in others:
        hydro = hydro + jnp.where(ok[code], cr[code], 0.0)
    rec[6:8, :] = jnp.zeros((2, 128), jnp.float32)
    for n in range(3):
        speed_old = nb[13, 3 + n : 4 + n, :]
        pulled = hydro[n : n + 1, :] - (SPEED_UNIT * speed_old) * hydro[3:4, :]
        speed_new = speed_old + FORCE_SCALE * pulled + force[n]
        if n == 2:
            speed_new = speed_new - GRAVITY_STEP
        rec[3 + n : 4 + n, :] = speed_new
        rec[n : n + 1, :] = nb[13, n : n + 1, :] + speed_new * (SPEED_UNIT / R)

    record = rec[...]
    for n, code in enumerate(MOVE_CODES):
        shift = zero
        for axis, step in enumerate(offset_of(code)):
            if step != 0:
                shift = jnp.where(sub == axis, step * SPANS[axis], shift)
        source = inv2_v[n]
        picked = lane_gather(record - shift, source & 127)
        ds[n] = jnp.where(source >= 0, picked, 0.0)
    def send_d(n):
        return pltpu.make_async_remote_copy(
            src_ref=ds.at[n],
            dst_ref=dr.at[6 - n],
            send_sem=sent,
            recv_sem=d_recv,
            device_id=device(offset_of(MOVE_CODES[n])),
            device_id_type=MESH,
        )

    movers = [n for n in range(7) if MOVE_CODES[n] != 13]
    for n in movers:
        pl.when(ok[MOVE_CODES[n]])(lambda n=n: send_d(n).start())

    def solid(x, carry):
        for half in range(2):
            rows, dest = cell_rows(x, half)
            v, base, even, odd = solid_part(int_v[rows, :], mac[5, rows, :])
            rel[PLACE[0], dest, :] = rel[PLACE[0], dest, :] + WEIGHTS[0] * base
            for i, j in PAIRS:
                along = projected(v, i)
                symmetric = WEIGHTS[i] * (base + even * along * along)
                skew = WEIGHTS[i] * (odd * along)
                rel[PLACE[i], dest, :] = rel[PLACE[i], dest, :] + (symmetric + skew)
                rel[PLACE[j], dest, :] = rel[PLACE[j], dest, :] + (symmetric - skew)
        return carry

    lax.fori_loop(0, CX, solid, 0, unroll=CX)

    def near_rows(a, b):
        return 8 * (10 * a + 5 * b + a * b)

    def far_rows(a, b, c):
        return 8 * c * (1 + a + b)

    wait_sides(b_recv.at[0], lambda a, b, c: near_rows(a, b))
    for side in range(2):
        x = -1 if side == 0 else CX
        for n, d in enumerate((X_UP, X_DOWN)[side]):
            rel[PLACE[d], pl.ds(STRIDE * (x + 1) + PAD, CY), :] = xr[side, n]
    for side in range(2):
        y = -1 if side == 0 else CY
        for n, d in enumerate(Y_MOVERS[side]):
            tile = yr[side, n]
            if n == 1:
                tile = jnp.where(sub == 0, ye[side, 0], tile)
            if n == 2:
                tile = jnp.where(sub == CX - 1, ye[side, 1], tile)
            start = STRIDE * (1 - LATTICE[d][0]) + PAD + y
            rel[PLACE[d], pl.ds(start, CX, stride=STRIDE), :] = tile
    wait_sides(d_recv, lambda a, b, c: 8 * (a + b + c))
    arrived = ds[3]
    for n in movers:
        arrived = arrived + jnp.where(ok[MOVE_CODES[n]], dr[n], 0.0)
    out_part[0, 0, :, 0, :] = arrived[0:6, :]

    wait_sides(b_recv.at[1], far_rows)
    for side in range(2):
        tile = zr[side]
        tile = jnp.where((sub == 1) & (lane < CY), ze[side, 0], tile)
        tile = jnp.where((sub == 2) & (lane >= 128 - CY), ze[side, 1], tile)
        tile = jnp.where((sub == 3) & ((lane & 15) == 0), ze[side, 2], tile)
        tile = jnp.where((sub == 4) & ((lane & 15) == 15), ze[side, 3], tile)
        col_out[8 * side : 8 * side + 8, :] = tile
    wait_sides(
        sent,
        lambda a, b, c: 12 * ((a + 1) * (b + 1) * (c + 1) - 1)
        + near_rows(a, b)
        + far_rows(a, b, c)
        + 8 * (a + b + c),
    )


def stream_kernel(sizes, rel, ends, records, out_pop, out_part, out_v, out_sem, part_sem):
    here = [lax.axis_index(axis) for axis in AXES]
    keep_records = pltpu.make_async_copy(records, out_part, part_sem)
    keep_records.start()
    lane = lax.broadcasted_iota(jnp.int32, (8, 128), 1)
    sub = lax.broadcasted_iota(jnp.int32, (8, 128), 0)
    low_wall = [here[n] == 0 for n in range(3)]
    high_wall = [here[n] == sizes[n] - 1 for n in range(3)]
    order = sorted(range(19), key=lambda d: LATTICE[d][2] != 0)

    def put(d):
        return pltpu.make_async_copy(out_v.at[d], out_pop.at[d], out_sem)

    for d in order:
        vector = LATTICE[d]
        if d == order[4]:
            columns = jnp.transpose(
                jnp.concatenate([ends[...], jnp.zeros((112, 128), jnp.float32)], axis=0)
            )
        for x in range(CX):
            for half in range(2):
                cells = pl.ds(CY * x + 8 * half, 8)
                walls = {
                    (0, 1): low_wall[0] if x == 0 else None,
                    (0, -1): high_wall[0] if x == CX - 1 else None,
                    (1, 1): low_wall[1] & (sub == 0) if half == 0 else None,
                    (1, -1): high_wall[1] & (sub == 7) if half == 1 else None,
                    (2, 1): low_wall[2] & (lane == 0),
                    (2, -1): high_wall[2] & (lane == 127),
                }
                start = STRIDE * (x + 1 - vector[0]) + PAD + 8 * half - vector[1]
                value = rel[PLACE[d], pl.ds(start, 8), :]
                if vector[2] != 0:
                    side = 0 if vector[2] == 1 else 1
                    column = 8 * side + Z_MOVERS[side].index(d)
                    value = jnp.where(
                        lane == (0 if side == 0 else 127),
                        columns[CY * x + 8 * half : CY * x + 8 * half + 8, column : column + 1],
                        pltpu.roll(value, vector[2] % 128, 1),
                    )
                blocked = None
                for axis in range(3):
                    wall = walls.get((axis, vector[axis]))
                    if wall is not None:
                        blocked = wall if blocked is None else blocked | wall
                if blocked is not None:
                    back = rel[PLACE[OPPOSITE[d]], pl.ds(STRIDE * (x + 1) + PAD + 8 * half, 8), :]
                    value = jnp.where(blocked, back, value)
                out_v[d, cells, :] = value
        put(d).start()
    pltpu.make_async_copy(out_v, out_pop, out_sem).wait()
    keep_records.wait()


def body(sizes, pop, frac, inter, touch, part, cont, dcode, dslot):
    f32, i32 = jnp.float32, jnp.int32
    cells = CX * CY
    part, cont = (jnp.transpose(a, (0, 1, 3, 2, 4)) for a in (part, cont))
    args = (
        pop.reshape(19, cells, CZ),
        frac.reshape(cells, CZ),
        inter.reshape(cells, CZ),
        touch,
        part,
        cont,
        dcode,
        dslot,
    )
    vmem = pltpu.VMEM
    sems = pltpu.SemaphoreType.DMA
    in_vmem = pl.BlockSpec(memory_space=vmem)
    in_any = pl.BlockSpec(memory_space=pl.ANY)
    relaxed, columns, records = pl.pallas_call(
        lambda *refs: kernel(sizes, *refs),
        out_shape=(
            vmem((19, STRIDE * (CX + 2), CZ), f32),
            vmem((16, 128), f32),
            vmem((1, 1, 6, 1, SLOTS), f32),
        ),
        in_specs=[in_any] * 8,
        out_specs=(in_vmem,) * 3,
        scratch_shapes=[
            vmem((19, cells, CZ), f32),
            vmem((cells, CZ), f32),
            vmem((cells, CZ), i32),
            vmem((1, TOUCHES), i32),
            vmem((CANDIDATES, SLOTS), i32),
            vmem((1, SLOTS), i32),
            vmem((1, SLOTS), i32),
            vmem((27, 8, 128), f32),
            vmem((6, cells, CZ), f32),
            vmem((8 * cells, CZ), f32),
            vmem((14, 8, 128), i32),
            vmem((8, 8, 128), i32),
            vmem((28, 4, 128), f32),
            vmem((27, 4, 128), f32),
            vmem((2, 3, 8, 128), f32),
            vmem((2, 5, CY, CZ), f32),
            vmem((2, 5, CY, CZ), f32),
            vmem((2, 5, CX, CZ), f32),
            vmem((2, 5, CX, CZ), f32),
            vmem((2, 2, CX, CZ), f32),
            vmem((cells, 128), f32),
            vmem((2, 8, 128), f32),
            vmem((2, 8, 128), f32),
            vmem((2, 4, 8, 128), f32),
            vmem((8, 128), f32),
            vmem((7, 8, 128), f32),
            vmem((7, 8, 128), f32),
            sems((4,)),
            sems((2,)),
            sems((2,)),
            sems,
            sems,
            sems,
        ],
        compiler_params=pltpu.CompilerParams(collective_id=0, has_side_effects=True),
    )(*args)
    populations, records = pl.pallas_call(
        lambda *refs: stream_kernel(sizes, *refs),
        out_shape=(
            jax.ShapeDtypeStruct((19, cells, CZ), f32),
            jax.ShapeDtypeStruct((1, 1, 6, 1, SLOTS), f32),
        ),
        in_specs=[in_vmem] * 3,
        out_specs=(in_any,) * 2,
        scratch_shapes=[vmem((19, cells, CZ), f32), sems, sems],
    )(*(pltpu.with_memory_space_constraint(a, vmem) for a in (relaxed, columns, records)))
    return populations.reshape(19, CX, CY, CZ), jnp.transpose(records, (0, 1, 3, 2, 4))


def solution(mesh):
    sizes = tuple(mesh.shape[axis] for axis in AXES)
    cells, blocks = P(*AXES), P(*AXES, None)
    records = P(*AXES, None, None)
    fields = P(None, *AXES)
    return jax.shard_map(
        lambda *args: body(sizes, *args),
        mesh=mesh,
        in_specs=(fields, cells, cells, blocks, records, records, blocks, blocks),
        out_specs=(fields, records),
        check_vma=False,
    )
```

```python
import jax
import jax.numpy as jnp
from jax import lax
from jax.experimental import pallas as pl
from jax.experimental.pallas import tpu as pltpu
from jax.sharding import PartitionSpec as P

LATTICE = [
    (0, 0, 0),
    (1, 0, 0),
    (-1, 0, 0),
    (0, 1, 0),
    (0, -1, 0),
    (0, 0, 1),
    (0, 0, -1),
    (1, 1, 0),
    (-1, -1, 0),
    (1, -1, 0),
    (-1, 1, 0),
    (1, 0, 1),
    (-1, 0, -1),
    (1, 0, -1),
    (-1, 0, 1),
    (0, 1, 1),
    (0, -1, -1),
    (0, 1, -1),
    (0, -1, 1),
]
OPPOSITE = [0, 2, 1, 4, 3, 6, 5, 8, 7, 10, 9, 12, 11, 14, 13, 16, 15, 18, 17]
WEIGHTS = [1.0 / 3.0] + [1.0 / 18.0] * 6 + [1.0 / 36.0] * 12
PAIRS = [(i, i + 1) for i in range(1, 19, 2)]
RELAX_TIME = 0.8
SPEED_UNIT = 0.05
FORCE_SCALE = 0.1
CONTACT_GAIN = 1.0
GRAVITY_STEP = 0.1
R = 8.0
CX, CY, CZ, SLOTS, TOUCHES, CANDIDATES = 8, 16, 128, 128, 256, 12
SPANS = (CX / R, CY / R, CZ / R)
AXES = ("gx", "gy", "gz")
MESH = pl.DeviceIdType.MESH

X_UP, X_DOWN = [1, 7, 9, 11, 13], [2, 8, 10, 12, 14]
Y_MOVERS = [[3, 7, 10, 15, 17], [4, 9, 8, 18, 16]]
Z_MOVERS = [[5, 11, 14, 15, 18], [6, 13, 12, 17, 16]]
PLACE = {d: n for n, d in enumerate(X_UP + X_DOWN + [0, 3, 4, 5, 6, 15, 16, 17, 18])}
MOVE_CODES = [4, 10, 12, 13, 14, 16, 22]
PAD = 8
STRIDE = CY + 2 * PAD


def offset_of(code):
    return (code // 9 - 1, code // 3 % 3 - 1, code % 3 - 1)


def projected(velocity, d):
    along = None
    for n in range(3):
        if LATTICE[d][n] == 1:
            along = velocity[n] if along is None else along + velocity[n]
        elif LATTICE[d][n] == -1:
            along = -velocity[n] if along is None else along - velocity[n]
    return along


def lane_gather(table, index):
    return jnp.take_along_axis(table, index, axis=1, mode="promise_in_bounds")


def dot_lanes(a, b):
    return lax.dot_general(a, b, (((1,), (1,)), ((), ())), preferred_element_type=jnp.float32)


def kernel(
    sizes,
    pop,
    frac,
    inter,
    touch,
    part,
    cont,
    dcode,
    dslot,
    rel_out,
    col_out,
    out_part,
    f_v,
    frac_v,
    int_v,
    touch_v,
    cont_v,
    dcode_v,
    dslot_v,
    nb,
    mac,
    split,
    inv_v,
    inv2_v,
    cs,
    cr,
    zc,
    xs,
    xr,
    ys,
    yr,
    ye,
    zm,
    zs,
    zr,
    ze,
    rec,
    ds,
    dr,
    in_sem,
    a_recv,
    b_recv,
    c_recv,
    d_recv,
    sent,
):
    rel = rel_out
    here = [lax.axis_index(axis) for axis in AXES]

    def device(offset):
        return tuple(
            here[n] if offset[n] == 0 else lax.rem(here[n] + offset[n] + sizes[n], sizes[n])
            for n in range(3)
        )

    def exists(offset):
        ok = None
        for n in range(3):
            if offset[n] != 0:
                test = here[n] > 0 if offset[n] < 0 else here[n] < sizes[n] - 1
                ok = test if ok is None else ok & test
        return ok

    others = [code for code in range(27) if code != 13]
    others.sort(key=lambda code: -sum(abs(step) for step in offset_of(code)))
    ok = {code: exists(offset_of(code)) for code in others}
    def start_all(make):
        for code in others:
            pl.when(ok[code])(lambda code=code: make(code).start())

    count = [
        (here[n] > 0).astype(jnp.int32) + (here[n] < sizes[n] - 1).astype(jnp.int32)
        for n in range(3)
    ]

    neighbours = (count[0] + 1) * (count[1] + 1) * (count[2] + 1) - 1

    def wait_rows(sem, rows):
        pltpu.make_async_copy(split.at[pl.ds(0, rows)], split.at[pl.ds(0, rows)], sem).wait()

    def wait_all(sem, rows):
        for n in sorted({a * b * c - 1 for a in (2, 3) for b in (2, 3) for c in (2, 3)}):
            pl.when(neighbours == n)(lambda n=n: wait_rows(sem, rows * n))

    def wait_sides(sem, rows_of):
        for a in (1, 2):
            for b in (1, 2):
                for c in (1, 2):
                    here_now = (count[0] == a) & (count[1] == b) & (count[2] == c)
                    pl.when(here_now)(lambda a=a, b=b, c=c: wait_rows(sem, rows_of(a, b, c)))

    barrier = pltpu.get_barrier_semaphore()
    for code in others:

        @pl.when(ok[code])
        def _(code=code):
            pl.semaphore_signal(
                barrier, inc=1, device_id=device(offset_of(code)), device_id_type=MESH
            )

    own_load = pltpu.make_async_copy(part.at[0, 0, :, 0], nb.at[13, pl.ds(0, 6)], in_sem.at[0])
    own_load.start()
    for source, target in (
        (touch.at[0, 0], touch_v),
        (dcode.at[0, 0], dcode_v),
        (dslot.at[0, 0], dslot_v),
        (cont.at[0, 0, :, 0], cont_v),
        (frac, frac_v),
        (inter, int_v),
    ):
        pltpu.make_async_copy(source, target, in_sem.at[1]).start()
    pop_load = pltpu.make_async_copy(pop, f_v, in_sem.at[2])
    pop_load.start()

    lane = lax.broadcasted_iota(jnp.int32, (8, 128), 1)
    sub = lax.broadcasted_iota(jnp.int32, (8, 128), 0)

    def send_a(code):
        return pltpu.make_async_remote_copy(
            src_ref=nb.at[13],
            dst_ref=nb.at[26 - code],
            send_sem=sent,
            recv_sem=a_recv.at[int(0 not in offset_of(code))],
            device_id=device(offset_of(code)),
            device_id_type=MESH,
        )

    def send_c(code):
        return pltpu.make_async_remote_copy(
            src_ref=cs.at[code],
            dst_ref=cr.at[26 - code],
            send_sem=sent,
            recv_sem=c_recv,
            device_id=device(offset_of(code)),
            device_id_type=MESH,
        )

    def partial_sums():
        wait_rows(in_sem.at[1], 4 + CANDIDATES + 2 * CX * CY)
        entry = touch_v[0:1, :]
        wide = lax.broadcasted_iota(jnp.int32, (112, TOUCHES), 1)
        row = lax.broadcasted_iota(jnp.int32, (112, TOUCHES), 0)
        named = jnp.where((entry >> 7) == (row >> 2), wide + 1, 0).astype(jnp.float32)
        slot_row = lax.broadcasted_iota(jnp.int32, (SLOTS, TOUCHES), 0)
        placed = jnp.where((entry & 127) == slot_row, 1.0, 0.0)
        inverse = dot_lanes(named.astype(jnp.bfloat16), placed.astype(jnp.bfloat16))
        inv_v[...] = (inverse.astype(jnp.int32) - 1).reshape(14, 8, 128)
        code_row = jnp.broadcast_to(dcode_v[0:1, :], (8, 128))
        moved = jnp.concatenate(
            [jnp.where(code_row == code, lane + 1, 0).astype(jnp.float32) for code in MOVE_CODES]
            + [jnp.zeros((8, 128), jnp.float32)],
            axis=0,
        )
        tall = lax.broadcasted_iota(jnp.int32, (SLOTS, SLOTS), 0)
        landing = jnp.where(dslot_v[0:1, :] == tall, 1.0, 0.0)
        inverse2 = dot_lanes(moved.astype(jnp.bfloat16), landing.astype(jnp.bfloat16))
        inv2_v[...] = (inverse2.astype(jnp.int32) - 1).reshape(8, 8, 128)

        pop_load.wait()

        def moments(x, carry):
            for half in range(2):
                start = pl.multiple_of(CY * x + 8 * half, 8)
                rows = pl.ds(start, 8)
                f = [f_v[d, rows, :] for d in range(19)]
                rho = f[0]
                momentum = [None, None, None]
                for d in range(1, 19):
                    rho = rho + f[d]
                for n in range(3):
                    for d in range(1, 19):
                        if LATTICE[d][n] == 1:
                            momentum[n] = f[d] if momentum[n] is None else momentum[n] + f[d]
                    for d in range(1, 19):
                        if LATTICE[d][n] == -1:
                            momentum[n] = momentum[n] - f[d]
                eps = frac_v[rows, :]
                weight = jnp.where(
                    int_v[rows, :] < TOUCHES,
                    eps * (RELAX_TIME - 0.5) / (1.0 - eps + (RELAX_TIME - 0.5)),
                    0.0,
                )
                scale = 1.0 / rho
                mac[0, rows, :] = rho
                mac[1, rows, :] = weight
                for n in range(3):
                    mac[2 + n, rows, :] = momentum[n] * scale
                for n, term in enumerate(momentum + [rho]):
                    term = term * weight
                    if n == 3:
                        mac[5, rows, :] = term
                    high = term.astype(jnp.bfloat16).astype(jnp.float32)
                    split[pl.ds(8 * start + n, 8, stride=8), :] = high
                    split[pl.ds(8 * start + 4 + n, 8, stride=8), :] = term - high
            return carry

        lax.fori_loop(0, CX, moments, 0, unroll=2)

        low_row = lax.broadcasted_iota(jnp.int32, (32, 128), 0)

        def add_slab(x, total):
            left, right = [], []
            for y in range(CY):
                slots = int_v[pl.ds(CY * x + y, 1), :]
                tile = split[pl.ds(pl.multiple_of(8 * (CY * x + y), 8), 8), :]
                upper = jnp.broadcast_to(slots >> 5, (8, 128))
                picked = [jnp.where(upper == a, tile, 0.0) for a in range(8)]
                left.append(jnp.concatenate(picked, axis=0).astype(jnp.bfloat16))
                lower = jnp.broadcast_to(slots & 31, (32, 128))
                right.append(jnp.where(lower == low_row, 1.0, 0.0).astype(jnp.bfloat16))
            return total + dot_lanes(
                jnp.concatenate(left, axis=1), jnp.concatenate(right, axis=1)
            )

        total = lax.fori_loop(0, CX, add_slab, jnp.zeros((64, 32), jnp.float32), unroll=4)
        tables = []
        for h in range(2):
            table = jnp.concatenate(
                [total[8 * a : 8 * a + 8, :] for a in range(4 * h, 4 * h + 4)], axis=1
            )
            tables.append(table + pltpu.roll(table, 4, 0))

        for q in range(14):
            source = inv_v[q]
            index = source & 127
            picked = jnp.where(
                source < 128, lane_gather(tables[0], index), lane_gather(tables[1], index)
            )
            picked = jnp.where(source >= 0, picked, 0.0)
            cs[2 * q] = picked[0:4, :]
            cs[2 * q + 1] = picked[4:8, :]


    early = (here[2] == 1) | (here[1] == 4)
    pl.when(early)(partial_sums)

    own_load.wait()
    pl.semaphore_wait(barrier, neighbours)
    start_all(send_a)
    pl.when(jnp.logical_not(early))(partial_sums)

    start_all(send_c)

    def cell_rows(x, half):
        cells = pl.ds(pl.multiple_of(CY * x + 8 * half, 8), 8)
        return cells, pl.ds(pl.multiple_of(STRIDE * (x + 1) + PAD + 8 * half, 8), 8)

    def relax(x, carry):
        for half in range(2):
            rows, dest = cell_rows(x, half)
            rho = mac[0, rows, :]
            weight = mac[1, rows, :]
            u = [mac[2 + n, rows, :] for n in range(3)]
            alpha = (1.0 - weight) * (1.0 / RELAX_TIME)
            keep = 1.0 - alpha - weight
            even = (alpha - weight) * rho
            odd = 3.0 * (alpha + weight) * rho
            base = even * (1.0 - 1.5 * (u[0] * u[0] + u[1] * u[1] + u[2] * u[2]))
            even = 4.5 * even
            rel[PLACE[0], dest, :] = (1.0 - alpha) * f_v[0, rows, :] + WEIGHTS[0] * base
            for i, j in PAIRS:
                along = projected(u, i)
                symmetric = WEIGHTS[i] * (base + even * along * along)
                skew = WEIGHTS[i] * (odd * along)
                fi, fj = f_v[i, rows, :], f_v[j, rows, :]
                rel[PLACE[i], dest, :] = keep * fi + weight * fj + (symmetric + skew)
                rel[PLACE[j], dest, :] = keep * fj + weight * fi + (symmetric - skew)
        return carry

    lax.fori_loop(0, CX, relax, 0, unroll=2)

    def pack_ends(x, carry):
        for half in range(2):
            rows, dest = cell_rows(x, half)
            packed = jnp.zeros((8, 128), jnp.float32)
            for side in range(2):
                edge = 127 if side == 0 else 0
                values = [rel[PLACE[d], dest, :] for d in Z_MOVERS[side]]
                values += [mac[5, rows, :], int_v[rows, :].astype(jnp.float32)]
                for n, value in enumerate(values):
                    packed = jnp.where(lane == 8 * side + n, value[:, edge : edge + 1], packed)
            zm[rows, :] = packed
        return carry

    lax.fori_loop(0, CX, pack_ends, 0, unroll=CX)
    across = jnp.transpose(zm[...])

    def at_target(tile):
        up_y = jnp.where((lane & 15) == 0, pltpu.roll(tile, 128 - 15, 1), pltpu.roll(tile, 1, 1))
        down_y = jnp.where((lane & 15) == 15, pltpu.roll(tile, 15, 1), pltpu.roll(tile, 127, 1))
        moved_z = jnp.where(sub == 1, pltpu.roll(tile, 16, 1), tile)
        moved_z = jnp.where(sub == 2, pltpu.roll(tile, 112, 1), moved_z)
        moved_z = jnp.where(sub == 3, up_y, moved_z)
        return jnp.where(sub == 4, down_y, moved_z)

    for side in range(2):
        zc[side, 0] = at_target(across[8 * side : 8 * side + 8, :])
        for n in range(2):
            line = across[8 * side + 5 + n : 8 * side + 6 + n, :]
            zc[side, 1 + n] = at_target(jnp.broadcast_to(line, (8, 128)))

    touch_code, touch_slot = (
        [jnp.broadcast_to(part_of[:, 128 * h : 128 * h + 128], (8, 128)) for h in range(2)]
        for part_of in (touch_v[0:1, :] >> 7, touch_v[0:1, :] & 127)
    )
    zero = jnp.zeros((8, 128), jnp.float32)
    found = [zero, zero]

    def find_velocity(code):
        tile = nb[code]
        if code != 13:
            tile = jnp.where(ok[code], tile, 0.0)
            nb[code] = tile
        for h in range(2):
            found[h] = jnp.where(
                touch_code[h] == code, lane_gather(tile, touch_slot[h]), found[h]
            )

    corners = [code for code in others if 0 not in offset_of(code)]
    wait_sides(a_recv.at[0], lambda a, b, c: 8 * ((a + 1) * (b + 1) * (c + 1) - 1 - a * b * c))
    find_velocity(13)
    for code in others:
        if code not in corners:
            find_velocity(code)
    wait_sides(a_recv.at[1], lambda a, b, c: 8 * a * b * c)
    for code in corners:
        find_velocity(code)
    speed = [
        [jnp.broadcast_to(SPEED_UNIT * found[h][3 + n : 4 + n, :], (8, 128)) for n in range(3)]
        for h in range(2)
    ]

    def solid_part(slots, mass):
        index = slots & 127
        first = slots < 128
        v = [
            jnp.where(first, lane_gather(speed[0][n], index), lane_gather(speed[1][n], index))
            for n in range(3)
        ]
        base = mass * (1.0 - 1.5 * (v[0] * v[0] + v[1] * v[1] + v[2] * v[2]))
        return v, base, 4.5 * mass, 3.0 * mass

    def solid_term(parts, d):
        v, base, even, odd = parts
        along = projected(v, d)
        return WEIGHTS[d] * (base + along * (even * along + odd))

    def send_b(move):
        source, target, offset = move
        return pltpu.make_async_remote_copy(
            src_ref=source,
            dst_ref=target,
            send_sem=sent,
            recv_sem=b_recv.at[abs(offset[2])],
            device_id=device(offset),
            device_id_type=MESH,
        )

    def code_of(offset):
        return 9 * (offset[0] + 1) + 3 * (offset[1] + 1) + offset[2] + 1

    def start_b(moves):
        for move in moves:
            pl.when(ok[code_of(move[2])])(lambda move=move: send_b(move).start())

    signs = [[jnp.zeros((8, 128), jnp.float32) for n in range(3)] for side in range(2)]
    for side in range(2):
        for n, d in enumerate(Z_MOVERS[side]):
            for axis in range(3):
                if LATTICE[d][axis] != 0:
                    signs[side][axis] = jnp.where(
                        sub == n, float(LATTICE[d][axis]), signs[side][axis]
                    )
    share = jnp.where(sub == 0, 1.0 / 18.0, 1.0 / 36.0)
    for side in range(2):
        v, base, even, odd = solid_part(zc[side, 2].astype(jnp.int32), zc[side, 1])
        along = signs[side][0] * v[0] + signs[side][1] * v[1] + signs[side][2] * v[2]
        zs[side] = zc[side, 0] + share * (base + along * (even * along + odd))
    moves = []
    for n, (step_x, step_y) in ((3, (0, -1)), (2, (0, 1)), (0, (1, 0)), (1, (-1, 0))):
        for side in (1, 0):
            moves.append((zs.at[side], ze.at[side, n], (step_x, step_y, 1 - 2 * side)))
    start_b(moves)
    for side in range(2):
        x = CX - 1 if side == 0 else 0
        for half in range(2):
            rows, dest = cell_rows(x, half)
            parts = solid_part(int_v[rows, :], mac[5, rows, :])
            for n, d in enumerate((X_UP, X_DOWN)[side]):
                value = rel[PLACE[d], dest, :] + solid_term(parts, d)
                xs[side, n, pl.ds(8 * half, 8), :] = value
    for side in range(2):
        y = CY - 1 if side == 0 else 0
        rows = pl.ds(y, CX, stride=CY)
        dest = pl.ds(STRIDE + PAD + y, CX, stride=STRIDE)
        parts = solid_part(int_v[rows, :], mac[5, rows, :])
        for n, d in enumerate(Y_MOVERS[side]):
            value = rel[PLACE[d], dest, :] + solid_term(parts, d)
            if LATTICE[d][0] != 0:
                value = pltpu.roll(value, LATTICE[d][0] % CX, 0)
            ys[side, n] = value
    start_b([(xs.at[side], xr.at[side], (1 - 2 * side, 0, 0)) for side in (1, 0)])
    moves = []
    for side in (1, 0):
        step = 1 - 2 * side
        moves.append((ys.at[side, 1], ye.at[side, 0], (1, step, 0)))
        moves.append((ys.at[side, 2], ye.at[side, 1], (-1, step, 0)))
    for side in (1, 0):
        moves.append((ys.at[side], yr.at[side], (0, 1 - 2 * side, 0)))
    start_b(moves)
    start_b([(zs.at[side], zr.at[side], (0, 0, 1 - 2 * side)) for side in (1, 0)])

    listed = [
        cont_v[0:8, :],
        jnp.concatenate([cont_v[8:12, :], jnp.full((4, 128), 27 * SLOTS, jnp.int32)], axis=0),
    ]
    listed_code = [entries >> 7 for entries in listed]
    listed_slot = [entries & 127 for entries in listed]

    def find_partner(code, partner):
        shifts = (code // 9 - 1, code // 3 % 3 - 1, code % 3 - 1)
        result = []
        for n in range(3):
            line = nb[code, pl.ds(n, 1), :] + shifts[n].astype(jnp.float32) * SPANS[n]
            line = jnp.broadcast_to(line, (8, 128))
            for h in range(2):
                result.append(
                    jnp.where(
                        listed_code[h] == code,
                        lane_gather(line, listed_slot[h]),
                        partner[2 * n + h],
                    )
                )
        return tuple(result)

    partner = lax.fori_loop(0, 27, find_partner, (zero,) * 6, unroll=27)
    force = [None, None, None]
    for h in range(2):
        apart = [nb[13, n : n + 1, :] - partner[2 * n + h] for n in range(3)]
        square = apart[0] * apart[0] + apart[1] * apart[1] + apart[2] * apart[2]
        soften = 1.0 + 0.25 * square
        strength = jnp.where(listed_code[h] < 27, CONTACT_GAIN / (soften * soften), 0.0)
        for n in range(3):
            term = jnp.sum(apart[n] * strength, axis=0, keepdims=True)
            force[n] = term if h == 0 else force[n] + term

    wait_all(c_recv, 4)
    hydro = cs[13]
    for code in others:
        hydro = hydro + jnp.where(ok[code], cr[code], 0.0)
    rec[6:8, :] = jnp.zeros((2, 128), jnp.float32)
    for n in range(3):
        speed_old = nb[13, 3 + n : 4 + n, :]
        pulled = hydro[n : n + 1, :] - (SPEED_UNIT * speed_old) * hydro[3:4, :]
        speed_new = speed_old + FORCE_SCALE * pulled + force[n]
        if n == 2:
            speed_new = speed_new - GRAVITY_STEP
        rec[3 + n : 4 + n, :] = speed_new
        rec[n : n + 1, :] = nb[13, n : n + 1, :] + speed_new * (SPEED_UNIT / R)

    record = rec[...]
    for n, code in enumerate(MOVE_CODES):
        shift = zero
        for axis, step in enumerate(offset_of(code)):
            if step != 0:
                shift = jnp.where(sub == axis, step * SPANS[axis], shift)
        source = inv2_v[n]
        picked = lane_gather(record - shift, source & 127)
        ds[n] = jnp.where(source >= 0, picked, 0.0)
    def send_d(n):
        return pltpu.make_async_remote_copy(
            src_ref=ds.at[n],
            dst_ref=dr.at[6 - n],
            send_sem=sent,
            recv_sem=d_recv,
            device_id=device(offset_of(MOVE_CODES[n])),
            device_id_type=MESH,
        )

    movers = [n for n in range(7) if MOVE_CODES[n] != 13]
    for n in movers:
        pl.when(ok[MOVE_CODES[n]])(lambda n=n: send_d(n).start())

    def solid(x, carry):
        for half in range(2):
            rows, dest = cell_rows(x, half)
            v, base, even, odd = solid_part(int_v[rows, :], mac[5, rows, :])
            rel[PLACE[0], dest, :] = rel[PLACE[0], dest, :] + WEIGHTS[0] * base
            for i, j in PAIRS:
                along = projected(v, i)
                symmetric = WEIGHTS[i] * (base + even * along * along)
                skew = WEIGHTS[i] * (odd * along)
                rel[PLACE[i], dest, :] = rel[PLACE[i], dest, :] + (symmetric + skew)
                rel[PLACE[j], dest, :] = rel[PLACE[j], dest, :] + (symmetric - skew)
        return carry

    lax.fori_loop(0, CX, solid, 0, unroll=CX)

    def near_rows(a, b):
        return 8 * (10 * a + 5 * b + a * b)

    def far_rows(a, b, c):
        return 8 * c * (1 + a + b)

    wait_sides(b_recv.at[0], lambda a, b, c: near_rows(a, b))
    for side in range(2):
        x = -1 if side == 0 else CX
        for n, d in enumerate((X_UP, X_DOWN)[side]):
            rel[PLACE[d], pl.ds(STRIDE * (x + 1) + PAD, CY), :] = xr[side, n]
    for side in range(2):
        y = -1 if side == 0 else CY
        for n, d in enumerate(Y_MOVERS[side]):
            tile = yr[side, n]
            if n == 1:
                tile = jnp.where(sub == 0, ye[side, 0], tile)
            if n == 2:
                tile = jnp.where(sub == CX - 1, ye[side, 1], tile)
            start = STRIDE * (1 - LATTICE[d][0]) + PAD + y
            rel[PLACE[d], pl.ds(start, CX, stride=STRIDE), :] = tile
    wait_sides(d_recv, lambda a, b, c: 8 * (a + b + c))
    arrived = ds[3]
    for n in movers:
        arrived = arrived + jnp.where(ok[MOVE_CODES[n]], dr[n], 0.0)
    out_part[0, 0, :, 0, :] = arrived[0:6, :]

    wait_sides(b_recv.at[1], far_rows)
    for side in range(2):
        tile = zr[side]
        tile = jnp.where((sub == 1) & (lane < CY), ze[side, 0], tile)
        tile = jnp.where((sub == 2) & (lane >= 128 - CY), ze[side, 1], tile)
        tile = jnp.where((sub == 3) & ((lane & 15) == 0), ze[side, 2], tile)
        tile = jnp.where((sub == 4) & ((lane & 15) == 15), ze[side, 3], tile)
        col_out[8 * side : 8 * side + 8, :] = tile
    wait_sides(
        sent,
        lambda a, b, c: 12 * ((a + 1) * (b + 1) * (c + 1) - 1)
        + near_rows(a, b)
        + far_rows(a, b, c)
        + 8 * (a + b + c),
    )


def stream_kernel(sizes, rel, ends, records, out_pop, out_part, out_v, out_sem, part_sem):
    here = [lax.axis_index(axis) for axis in AXES]
    keep_records = pltpu.make_async_copy(records, out_part, part_sem)
    keep_records.start()
    lane = lax.broadcasted_iota(jnp.int32, (8, 128), 1)
    sub = lax.broadcasted_iota(jnp.int32, (8, 128), 0)
    low_wall = [here[n] == 0 for n in range(3)]
    high_wall = [here[n] == sizes[n] - 1 for n in range(3)]
    order = sorted(range(19), key=lambda d: LATTICE[d][2] != 0)

    def put(d):
        return pltpu.make_async_copy(out_v.at[d], out_pop.at[d], out_sem)

    for d in order:
        vector = LATTICE[d]
        if d == order[4]:
            columns = jnp.transpose(
                jnp.concatenate([ends[...], jnp.zeros((112, 128), jnp.float32)], axis=0)
            )
        for x in range(CX):
            for half in range(2):
                cells = pl.ds(CY * x + 8 * half, 8)
                walls = {
                    (0, 1): low_wall[0] if x == 0 else None,
                    (0, -1): high_wall[0] if x == CX - 1 else None,
                    (1, 1): low_wall[1] & (sub == 0) if half == 0 else None,
                    (1, -1): high_wall[1] & (sub == 7) if half == 1 else None,
                    (2, 1): low_wall[2] & (lane == 0),
                    (2, -1): high_wall[2] & (lane == 127),
                }
                start = STRIDE * (x + 1 - vector[0]) + PAD + 8 * half - vector[1]
                value = rel[PLACE[d], pl.ds(start, 8), :]
                if vector[2] != 0:
                    side = 0 if vector[2] == 1 else 1
                    column = 8 * side + Z_MOVERS[side].index(d)
                    value = jnp.where(
                        lane == (0 if side == 0 else 127),
                        columns[CY * x + 8 * half : CY * x + 8 * half + 8, column : column + 1],
                        pltpu.roll(value, vector[2] % 128, 1),
                    )
                blocked = None
                for axis in range(3):
                    wall = walls.get((axis, vector[axis]))
                    if wall is not None:
                        blocked = wall if blocked is None else blocked | wall
                if blocked is not None:
                    back = rel[PLACE[OPPOSITE[d]], pl.ds(STRIDE * (x + 1) + PAD + 8 * half, 8), :]
                    value = jnp.where(blocked, back, value)
                out_v[d, cells, :] = value
        put(d).start()
    pltpu.make_async_copy(out_v, out_pop, out_sem).wait()
    keep_records.wait()


def body(sizes, pop, frac, inter, touch, part, cont, dcode, dslot):
    f32, i32 = jnp.float32, jnp.int32
    cells = CX * CY
    part, cont = (jnp.transpose(a, (0, 1, 3, 2, 4)) for a in (part, cont))
    args = (
        pop.reshape(19, cells, CZ),
        frac.reshape(cells, CZ),
        inter.reshape(cells, CZ),
        touch,
        part,
        cont,
        dcode,
        dslot,
    )
    vmem = pltpu.VMEM
    sems = pltpu.SemaphoreType.DMA
    in_vmem = pl.BlockSpec(memory_space=vmem)
    in_any = pl.BlockSpec(memory_space=pl.ANY)
    relaxed, columns, records = pl.pallas_call(
        lambda *refs: kernel(sizes, *refs),
        out_shape=(
            vmem((19, STRIDE * (CX + 2), CZ), f32),
            vmem((16, 128), f32),
            vmem((1, 1, 6, 1, SLOTS), f32),
        ),
        in_specs=[in_any] * 8,
        out_specs=(in_vmem,) * 3,
        scratch_shapes=[
            vmem((19, cells, CZ), f32),
            vmem((cells, CZ), f32),
            vmem((cells, CZ), i32),
            vmem((1, TOUCHES), i32),
            vmem((CANDIDATES, SLOTS), i32),
            vmem((1, SLOTS), i32),
            vmem((1, SLOTS), i32),
            vmem((27, 8, 128), f32),
            vmem((6, cells, CZ), f32),
            vmem((8 * cells, CZ), f32),
            vmem((14, 8, 128), i32),
            vmem((8, 8, 128), i32),
            vmem((28, 4, 128), f32),
            vmem((27, 4, 128), f32),
            vmem((2, 3, 8, 128), f32),
            vmem((2, 5, CY, CZ), f32),
            vmem((2, 5, CY, CZ), f32),
            vmem((2, 5, CX, CZ), f32),
            vmem((2, 5, CX, CZ), f32),
            vmem((2, 2, CX, CZ), f32),
            vmem((cells, 128), f32),
            vmem((2, 8, 128), f32),
            vmem((2, 8, 128), f32),
            vmem((2, 4, 8, 128), f32),
            vmem((8, 128), f32),
            vmem((7, 8, 128), f32),
            vmem((7, 8, 128), f32),
            sems((3,)),
            sems((2,)),
            sems((2,)),
            sems,
            sems,
            sems,
        ],
        compiler_params=pltpu.CompilerParams(collective_id=0, has_side_effects=True),
    )(*args)
    populations, records = pl.pallas_call(
        lambda *refs: stream_kernel(sizes, *refs),
        out_shape=(
            jax.ShapeDtypeStruct((19, cells, CZ), f32),
            jax.ShapeDtypeStruct((1, 1, 6, 1, SLOTS), f32),
        ),
        in_specs=[in_vmem] * 3,
        out_specs=(in_any,) * 2,
        scratch_shapes=[vmem((19, cells, CZ), f32), sems, sems],
    )(*(pltpu.with_memory_space_constraint(a, vmem) for a in (relaxed, columns, records)))
    return populations.reshape(19, CX, CY, CZ), jnp.transpose(records, (0, 1, 3, 2, 4))


def solution(mesh):
    sizes = tuple(mesh.shape[axis] for axis in AXES)
    cells, blocks = P(*AXES), P(*AXES, None)
    records = P(*AXES, None, None)
    fields = P(None, *AXES)
    return jax.shard_map(
        lambda *args: body(sizes, *args),
        mesh=mesh,
        in_specs=(fields, cells, cells, blocks, records, records, blocks, blocks),
        out_specs=(fields, records),
        check_vma=False,
    )
```
